256 devices in a mesh: row: 16 (over y_hi, x, core), col: 16 (over y_lo, z).
Axes of the slice: x: 4, y: 4 (y_hi: 2, y_lo: 2; y = y_hi * 2 + y_lo), z: 8, core: 2. Of those that a mesh axis runs over, the one named last changes fastest.
Arguments:
- grad_x: float32 [8192, 8192], P('row', 'col'), may hold values from -6 to 6
- grad_y: float32 [8192, 8192], P('row', 'col'), may hold values from -6 to 6
Outputs:
- field: float32 [8192, 8192], P('row', 'col')
The draws below stay inside these ranges and needn't reach their ends.
All inputs are finite; a program needn't handle non-finite values.
Results may differ from the reference program's by a relative error of at most 0.0003.
Values sent between devices are 32-bit elements; how exact they have to be, the bound alone decides.
No kernel may reach another device: no remote copies, remote signals or barrier semaphores. Data moves between devices by JAX's collectives and lax.ppermute only.
A program may use at most 64 MiB of HBM per device.

```python
import math
import jax
import jax.numpy as jnp

NX = 8192
NY = 8192


def block_scale(key, dims, pieces, smallest, high):
    factor_of, own = 1.0, jax.random.fold_in(key, 6)
    for position, parts in pieces:
        steps = jnp.exp(jax.random.uniform(jax.random.fold_in(own, position), (parts,), jnp.float32, smallest / len(pieces), high / len(pieces)))
        factor_of = factor_of * jnp.repeat(steps, dims[position] // parts).reshape([-1 if axis == position else 1 for axis in range(len(dims))])
    return factor_of


def gaussian(rng, extent, scale, limit, pieces=(), kind=jnp.bfloat16):
    array = jax.random.normal(rng, extent, jnp.float32) * scale
    if len(pieces) > 0:
        array = block_scale(rng, extent, pieces, -0.22, 0.18) * array
    return jnp.clip(array, min=-limit, max=limit).astype(kind)


def setup_inputs(seed: int = 0) -> dict:
    splits = jax.random.split(jax.random.key(seed), 3)
    grad_x = gaussian(splits[0], (NX, NY), 1.0, 6.0, ((0, 16), (1, 16)), jnp.float32)
    grad_y = gaussian(splits[1], (NX, NY), 1.0, 6.0, ((0, 16), (1, 16)), jnp.float32)
    return dict(grad_x=grad_x, grad_y=grad_y)


def cosine_forward(values):
    length = values.shape[0]
    spec = jnp.fft.rfft(values, n=2 * length, axis=0)[:length]
    angle = jnp.arange(length, dtype=jnp.float32) * (math.pi / (2 * length))
    return jnp.cos(angle)[:, None] * spec.real + jnp.sin(angle)[:, None] * spec.imag


def cosine_inverse(values):
    length = values.shape[0]
    angle = jnp.arange(length, dtype=jnp.float32) * (math.pi / (2 * length))
    real_part = values * jnp.cos(angle)[:, None]
    imag_part = values * jnp.sin(angle)[:, None]
    zero_row = jnp.zeros((1, values.shape[1]), values.dtype)
    real_part = jnp.concatenate([2.0 * real_part[:1], real_part[1:], zero_row], 0)
    imag_part = jnp.concatenate([2.0 * imag_part[:1], imag_part[1:], zero_row], 0)
    packed = real_part + 1j * imag_part
    return jnp.fft.irfft(packed, n=2 * length, axis=0)[:length] * length


def reference(grad_x, grad_y):
    zero_row = jnp.zeros((1, grad_x.shape[1]), grad_x.dtype)
    zero_col = jnp.zeros((grad_y.shape[0], 1), grad_y.dtype)
    diverge = (grad_x - jnp.concatenate([zero_row, grad_x[:-1]], 0)) + (grad_y - jnp.concatenate([zero_col, grad_y[:, :-1]], 1))
    spectrum = cosine_forward(cosine_forward(diverge).T).T
    total_x, total_y = spectrum.shape
    freq_x = jnp.arange(total_x, dtype=jnp.float32)
    freq_y = jnp.arange(total_y, dtype=jnp.float32)
    eigen = -4.0 * jnp.sin(freq_x * (math.pi / (2 * total_x)))[:, None] ** 2 - 4.0 * jnp.sin(freq_y * (math.pi / (2 * total_y)))[None, :] ** 2
    weight_x = jnp.where(freq_x == 0, 1.0, 2.0) / total_x
    weight_y = jnp.where(freq_y == 0, 1.0, 2.0) / total_y
    anchor = (freq_x == 0)[:, None] & (freq_y == 0)[None, :]
    scaled = jnp.where(anchor, 0.0, spectrum / jnp.where(anchor, 1.0, eigen)) * weight_x[:, None] * weight_y[None, :]
    return cosine_inverse(cosine_inverse(scaled).T).T
```

```python
import math

import jax
import jax.numpy as jnp
import numpy as np
from jax import lax
from jax.experimental import pallas as pl
from jax.experimental.pallas import tpu as pltpu
from jax.sharding import PartitionSpec as P

DIRECT = False
f32 = jnp.float32
bf16 = jnp.bfloat16


def cosine_basis(n):
    k, i = np.arange(n)[:, None], np.arange(n)[None]
    return np.sqrt(np.where(k == 0, 1, 2) / n) * np.cos(np.pi * k * (2 * i + 1) / (2 * n))


def edge_tables(n, members, freq):
    s = 2 * np.sin(freq)
    half = np.arcsinh(s / 2)
    e = np.exp(-2 * n * half)
    safe = np.where(s == 0, 1, s)
    e1 = np.where(s == 0, 0.5, e)
    th = np.tanh(np.arcsinh(safe / 2))
    one = np.where(s == 0, 0, 1)
    lead = one * th * (1 - e1 * e1)
    couple = one * e1 / (th * (1 - e1 * e1))
    return lead, e, couple


def build_tables(n, members):
    total = n * members
    half = n // 2
    q = cosine_basis(n)
    k = np.arange(n)
    s = 2 * np.sin(np.pi * k / (2 * n))
    den = s[:, None] ** 2 + s[None] ** 2
    den[0, 0] = 1
    r = 1 / den
    r[0, 0] = 0
    sp = np.zeros((n, n))
    i = np.arange(n)[None]
    sp = np.sqrt(2 / n) * s[:, None] * np.sin(np.pi * k[:, None] * (i + 1) / n)
    sp[:, n - 1] = 0
    sp[0] = 0
    q0, q1 = q[:, 0], q[:, -1]
    lead, e, couple = edge_tables(n, members, np.pi * k / (2 * n))
    vec = np.zeros((8, n))
    vec[0], vec[1], vec[2], vec[3], vec[4] = q0, q1, lead, e, couple
    m = np.arange(half)
    gvec = np.zeros((members, 8, n))
    for c in range(members):
        kap = np.concatenate([c + 2 * members * m, c + members + 2 * members * m])
        gvec[c, 2], gvec[c, 3], gvec[c, 4] = edge_tables(n, members, np.pi * kap / (2 * total))
    j = 2 * np.arange(n) + 1
    cb = np.concatenate(
        [np.cos(np.pi * m[:, None] * j[None] / n), np.sin(np.pi * m[:, None] * j[None] / n)], 1
    )
    cls = np.arange(2 * members)
    ang = np.pi * cls[:, None] * j[None] / (2 * total)
    acs = np.concatenate([np.cos(ang), np.sin(ang)], 0)
    p = np.arange(members)
    wang = np.pi * cls[:, None] * p[None] / members
    wc, ws = np.cos(wang), np.sin(wang)
    wfwd = np.zeros((members, 8, 2 * members))
    for c in range(members):
        for side in range(2):
            for h in range(2):
                cols = slice(side * members, (side + 1) * members)
                wfwd[c, 2 * side + h, cols] = wc[c + h * members]
                wfwd[c, 4 + 2 * side + h, cols] = ws[c + h * members]
    winv = np.concatenate([wc.T, -ws.T], 1)
    M = members
    t = np.arange(1, M)
    st = np.sqrt(2 / M) * np.sin(np.pi * np.outer(t, t) / M)
    sa, stt, s2 = np.zeros((M, M)), np.zeros((M, M)), np.zeros((M, M))
    sa[: M - 1, : M - 1] = st
    sa[: M - 1, M - 1] = st[:, M - 2]
    stt[: M - 1, 1:] = -st
    s2[: M - 1, : M - 1] = st
    a0 = (q1[1:] ** 2 / s[1:] ** 2).sum()
    b0 = (q0[1:] * q1[1:] / s[1:] ** 2).sum()
    qq = 1 / np.sqrt(n)
    pp = np.arange(M)
    frac = (pp[:, None] + 1) / M
    t1 = frac - (pp[None] <= pp[:, None])
    h15 = np.zeros((M, M))
    h15[:, M - 1] = frac[:, 0]
    hmat = np.concatenate([h15, t1], 1)
    acc = (pp[None] < pp[:, None]).astype(float)
    acc[:, M - 1] = 0
    acc = (acc - acc.mean(0)) / qq
    up = np.zeros((M, M))
    up[:-1, 1:] = np.eye(M - 1)
    keep = np.eye(M)
    keep[M - 1, M - 1] = 0
    ka = acc @ keep
    kt = -acc @ (keep @ up)
    kh = acc @ (keep @ (-(1 + 2 * a0) * np.eye(M) + b0 * up + b0 * up.T))
    mats = np.zeros((6 * M, 128))
    mats[0:M, : 2 * M] = np.concatenate([sa, stt], 1)
    mats[M : 2 * M, :M] = s2
    mats[2 * M : 3 * M, : 2 * M] = hmat
    mats[3 * M : 4 * M, : 3 * M] = np.concatenate([ka, kt, kh], 1)
    mats[4 * M : 5 * M, : 4 * M] = winv
    mats[5 * M : 5 * M + M - 1, :] = np.cos(np.pi * t / M)[:, None]
    wf = np.zeros((M, 8, 128))
    wf[:, :, : 2 * M] = wfwd
    out = dict(q=q, sp=sp, r=r, vec=vec, gvec=gvec, cb=cb, acs=acs, mats=mats, wf=wf)
    return {name: np.asarray(value, np.float32) for name, value in out.items()}


def split(a):
    high = a.astype(bf16)
    return high, (a - high.astype(f32)).astype(bf16)


def mm(a, b, ca, cb):
    return lax.dot_general(a, b, (((ca,), (cb,)), ((), ())), preferred_element_type=f32)


def dot3(a, b, ca=1, cb=0):
    ah, al = a if isinstance(a, tuple) else split(a)
    bh, bl = b if isinstance(b, tuple) else split(b)
    return mm(ah, bh, ca, cb) + (mm(ah, bl, ca, cb) + mm(al, bh, ca, cb))


def doth(a, b, ca=1, cb=0):
    return lax.dot_general(
        a, b, (((ca,), (cb,)), ((), ())), precision=lax.Precision.HIGHEST, preferred_element_type=f32
    )


def rows_of(shape):
    return lax.broadcasted_iota(jnp.int32, shape, 0)


def lanes_of(shape):
    return lax.broadcasted_iota(jnp.int32, shape, 1)


def pick(values, index):
    return jnp.sum(jnp.where(rows_of(values.shape) == index, values, 0.0), 0, keepdims=True)


def below(values):
    return jnp.concatenate([jnp.zeros_like(values[:1]), values[:-1]], 0)


def edge_solve(al, t0, lead, e, couple, source, mats, special):
    M, n = al.shape
    L = min(n, 128)
    last = rows_of((M, n)) == M - 1
    both = jnp.concatenate([jnp.where(last, al * couple, al), t0], 0)
    modes = doth(mats[0:M, : 2 * M], both)
    cosphi = mats[5 * M : 6 * M, :1]
    modes = modes * (lead / (1.0 + e * e - 2.0 * e * cosphi))
    H = jnp.where(last, al, doth(mats[M : 2 * M, :M], modes))
    Hz = doth(mats[2 * M : 3 * M, : 2 * M], jnp.concatenate([al[:, :L], source], 0))
    mean = doth(mats[3 * M : 4 * M, : 3 * M], jnp.concatenate([al[:, :L], t0[:, :L], Hz], 0))
    lane = lanes_of((M, L))
    first = jnp.where((lane == 0) & special, Hz, H[:, :L])
    H = first if n == L else jnp.concatenate([first, H[:, L:]], 1)
    return H, jnp.where(special, mean[:, :1], 0.0)


def to_peers(rows, members):
    one = jnp.concatenate(rows, 0)
    return jnp.broadcast_to(one[None], (members,) + one.shape)


def stage_local(r, c, M, gx, gy, q, sp, rr, vec):
    gx, gy, q, sp, rr, vec = gx[...], gy[...], q[...], sp[...], rr[...], vec[...]
    n = q.shape[0]
    L = min(n, 128)
    qs, ss = split(q), split(sp)
    gys = split(gy)
    m1 = dot3(gx, qs, 1, 1)
    m2 = dot3(gys, ss, 1, 1)
    u = -(dot3(ss, m1) + dot3(qs, m2)) * rr
    slab = (gys[0][:, n - L :], gys[1][:, n - L :])
    gyl = dot3(slab, qs, 0, 1)[L - 1 :]
    us = split(u)
    tk = dot3(vec, us, 1, 1)
    tl = dot3(vec, us, 1, 0)
    alpha = gyl + jnp.where(c < M - 1, tk[1:2], 0.0)
    beta = m1[n - 1 :] + jnp.where(r < M - 1, tl[1:2], 0.0)
    return u, to_peers([alpha, tk[0:1], beta, tl[0:1]], M)


def stage_strip(r, c, M, ag, q, rr, vec, cb, acs, mats, wf):
    al, t0, be, ta0 = (ag[:, a, :] for a in range(4))
    vec, mats = vec[...], mats[...]
    n = al.shape[1]
    q0, q1, lead, e, couple = (vec[a : a + 1] for a in range(5))
    L = min(n, 128)
    zero = jnp.zeros((M, L), f32)
    H, mean = edge_solve(al, t0, lead, e, couple, zero, mats, True)
    Z = doth(jnp.concatenate([H * q0, H * q1], 0), rr[...])
    add0 = q0 * below(Z[:M]) - q1 * Z[:M]
    add1 = q0 * below(Z[M:]) - q1 * Z[M:]
    flat = jnp.where(lanes_of((M, n)) == 0, mean * (1.0 / math.sqrt(n)), 0.0)
    tau0 = ta0 + add0 + flat
    tau1 = be + jnp.where(r < M - 1, add1 + flat, 0.0)
    y = doth(jnp.concatenate([tau0, tau1], 0), q[...])
    g = doth(wf[c][:, : 2 * M], y)
    C, S = g[:4], g[4:]
    ca0, ca1 = acs[pl.ds(c, 1), :], acs[pl.ds(c + M, 1), :]
    sa0, sa1 = acs[pl.ds(c + 2 * M, 1), :], acs[pl.ds(c + 3 * M, 1), :]
    ca = jnp.concatenate([ca0, ca1, ca0, ca1], 0)
    sa = jnp.concatenate([sa0, sa1, sa0, sa1], 0)
    xy = jnp.concatenate([C * ca - S * sa, -(C * sa + S * ca)], 1)
    T = doth(xy, cb[...], 1, 1) * math.sqrt(2.0 / (n * M))
    x0 = jnp.concatenate([T[0:1], T[1:2]], 1)
    x1 = jnp.concatenate([T[2:3], T[3:4]], 1)
    root = jnp.where((lanes_of((1, n)) == 0) & (c == 0), math.sqrt(0.5), 1.0)
    src = jnp.broadcast_to(al[M - 1 :, :1] * (1.0 / math.sqrt(M)), (1, n))
    return (to_peers([x1 * root, x0 * root, src, jnp.zeros((1, n), f32)], M),)


def stage_edges(r, c, M, ag, gvec, mats):
    al, t0 = ag[:, 0, :], ag[:, 1, :]
    n = al.shape[1]
    L = min(n, 128)
    src = ag[:, 2, :][:, :L]
    gv = gvec[c]
    H, mean = edge_solve(al, t0, gv[2:3], gv[3:4], gv[4:5], src, mats[...], c == 0)
    right = pick(H, r)
    left = pick(H, r - 1)
    lift = jnp.broadcast_to(pick(mean, r) * (1.0 / math.sqrt(M)), (1, n))
    return (to_peers([left, right, lift, jnp.zeros((1, n), f32)], M),)


def stage_field(r, c, M, ag3, ag1, u, q, rr, vec, cb, acs, mats):
    q, rr, vec, mats = q[...], rr[...], vec[...], mats[...]
    n = q.shape[0]
    half = n // 2
    L = min(n, 128)
    q0, q1, lead, e, couple = (vec[a : a + 1] for a in range(5))
    hl, hr = ag3[:, 0, :], ag3[:, 1, :]
    T = jnp.concatenate([hl[:, :half], hl[:, half:], hr[:, :half], hr[:, half:]], 0)
    root = jnp.where(
        (lanes_of(T.shape) == 0) & (rows_of(T.shape) % (2 * M) == 0), math.sqrt(0.5), 1.0
    )
    xx = doth(T * (root * math.sqrt(2.0 / (n * M))), cb[...])
    ca, sa = acs[0 : 2 * M, :], acs[2 * M : 4 * M, :]
    h = []
    for side in range(2):
        xc = xx[side * 2 * M : (side + 1) * 2 * M, :n]
        xs = xx[side * 2 * M : (side + 1) * 2 * M, n:]
        rot = jnp.concatenate([ca * xc - sa * xs, sa * xc + ca * xs], 0)
        h.append(doth(mats[4 * M : 5 * M, : 4 * M], rot))
    hx = doth(jnp.concatenate(h, 0), q, 1, 1)
    left, right = hx[:M], hx[M:]
    Y = doth(jnp.concatenate([left * q0, left * q1, right * q0, right * q1], 0), rr)
    t0b = q0 * Y[0:M] - q1 * Y[2 * M : 3 * M]
    t1b = q0 * Y[M : 2 * M] - q1 * Y[3 * M :]
    last = rows_of((M, n)) == M - 1
    al = ag1[:, 0, :] + jnp.where(last, 0.0, t1b)
    t0 = ag1[:, 1, :] + t0b
    src = right[:, :L] - left[:, :L]
    H, mean = edge_solve(al, t0, lead, e, couple, src, mats, True)
    here, before = pick(H, c), pick(H, c - 1)
    lhs = jnp.concatenate([q1, -q0, here, -before], 0)
    rhs = jnp.concatenate([pick(right, c), pick(left, c), q1, q0], 0)
    pad = jnp.zeros((4, n), f32)
    G = doth(jnp.concatenate([lhs, pad], 0), jnp.concatenate([rhs, pad], 0), 0, 0)
    level = pick(mean, c) + ag3[:, 2, :][:1, :1]
    un = u[...] - rr * G
    un = jnp.where((rows_of(un.shape) == 0) & (lanes_of(un.shape) == 0), level, un)
    qs = split(q)
    return (dot3(qs, dot3(un, qs), 0, 0),)


def run_stage(stage, members, outs, *args):
    r, c = lax.axis_index("row"), lax.axis_index("col")
    if DIRECT:
        return stage(r, c, members, *args)

    def kernel(place, *refs):
        results = stage(place[0], place[1], members, *refs[: len(args)])
        for ref, value in zip(refs[len(args) :], results):
            ref[...] = value

    place = jnp.stack([r, c]).astype(jnp.int32)
    vmem = pl.BlockSpec(memory_space=pltpu.VMEM)
    return pl.pallas_call(
        kernel,
        out_shape=[jax.ShapeDtypeStruct(shape, f32) for shape in outs],
        in_specs=[pl.BlockSpec(memory_space=pltpu.SMEM)] + [vmem] * len(args),
        out_specs=[vmem] * len(outs),
        compiler_params=pltpu.CompilerParams(vmem_limit_bytes=56 * 1024 * 1024),
        name=stage.__name__,
    )(place, *args)


def exchange(values, axis):
    return lax.all_to_all(values, axis, split_axis=0, concat_axis=0, tiled=True)


def make_body(members):
    def body(grad_x, grad_y):
        n = grad_x.shape[0]
        t = {k: jnp.asarray(v) for k, v in build_tables(n, members).items()}
        edge = (members, 4, n)
        u, edges = run_stage(
            stage_local, members, [(n, n), edge], grad_x, grad_y, t["q"], t["sp"], t["r"], t["vec"]
        )
        strip = exchange(edges, "col")
        (lines,) = run_stage(
            stage_strip, members, [edge],
            strip, t["q"], t["r"], t["vec"], t["cb"], t["acs"], t["mats"], t["wf"],
        )
        lines = exchange(lines, "row")
        (flux,) = run_stage(stage_edges, members, [edge], lines, t["gvec"], t["mats"])
        flux = exchange(flux, "col")
        (field,) = run_stage(
            stage_field, members, [(n, n)],
            flux, strip, u, t["q"], t["r"], t["vec"], t["cb"], t["acs"], t["mats"],
        )
        return field

    return body


def solution(mesh):
    members = mesh.shape["row"]
    placed = (P("row", "col"), P("row", "col"))
    return jax.shard_map(
        make_body(members), mesh=mesh, in_specs=placed, out_specs=P("row", "col"), check_vma=False
    )
```

```python
import math

import jax
import jax.numpy as jnp
import numpy as np
from jax import lax
from jax.experimental import pallas as pl
from jax.experimental.pallas import tpu as pltpu
from jax.sharding import PartitionSpec as P

DIRECT = False
f32 = jnp.float32
bf16 = jnp.bfloat16


def cosine_basis(n):
    k, i = np.arange(n)[:, None], np.arange(n)[None]
    return np.sqrt(np.where(k == 0, 1, 2) / n) * np.cos(np.pi * k * (2 * i + 1) / (2 * n))


def edge_tables(n, members, freq):
    s = 2 * np.sin(freq)
    half = np.arcsinh(s / 2)
    e = np.exp(-2 * n * half)
    safe = np.where(s == 0, 1, s)
    e1 = np.where(s == 0, 0.5, e)
    th = np.tanh(np.arcsinh(safe / 2))
    one = np.where(s == 0, 0, 1)
    lead = one * th * (1 - e1 * e1)
    couple = one * e1 / (th * (1 - e1 * e1))
    return lead, e, couple


def build_tables(n, members):
    total = n * members
    half = n // 2
    q = cosine_basis(n)
    k = np.arange(n)
    s = 2 * np.sin(np.pi * k / (2 * n))
    den = s[:, None] ** 2 + s[None] ** 2
    den[0, 0] = 1
    r = 1 / den
    r[0, 0] = 0
    sp = np.zeros((n, n))
    i = np.arange(n)[None]
    sp = np.sqrt(2 / n) * s[:, None] * np.sin(np.pi * k[:, None] * (i + 1) / n)
    sp[:, n - 1] = 0
    sp[0] = 0
    q0, q1 = q[:, 0], q[:, -1]
    lead, e, couple = edge_tables(n, members, np.pi * k / (2 * n))
    vec = np.zeros((8, n))
    vec[0], vec[1], vec[2], vec[3], vec[4] = q0, q1, lead, e, couple
    m = np.arange(half)
    cls = np.arange(2 * members)
    kap = cls[:, None] + 2 * members * m[None]
    glob = np.stack(edge_tables(n, members, np.pi * kap / (2 * total)))
    j = 2 * np.arange(n) + 1
    cb = np.concatenate(
        [np.cos(np.pi * m[:, None] * j[None] / n), np.sin(np.pi * m[:, None] * j[None] / n)], 1
    )
    ang = np.pi * cls[:, None] * j[None] / (2 * total)
    acs = np.concatenate([np.cos(ang), np.sin(ang)], 0)
    p = np.arange(members)
    wang = np.pi * cls[:, None] * p[None] / members
    wc, ws = np.cos(wang), np.sin(wang)
    wfwd = np.concatenate([wc, ws], 0)
    winv = np.concatenate([wc.T, -ws.T], 1)
    M = members
    t = np.arange(1, M)
    st = np.sqrt(2 / M) * np.sin(np.pi * np.outer(t, t) / M)
    sa, stt, s2 = np.zeros((M, M)), np.zeros((M, M)), np.zeros((M, M))
    sa[: M - 1, : M - 1] = st
    sa[: M - 1, M - 1] = st[:, M - 2]
    stt[: M - 1, 1:] = -st
    s2[: M - 1, : M - 1] = st
    a0 = (q1[1:] ** 2 / s[1:] ** 2).sum()
    b0 = (q0[1:] * q1[1:] / s[1:] ** 2).sum()
    qq = 1 / np.sqrt(n)
    pp = np.arange(M)
    frac = (pp[:, None] + 1) / M
    t1 = frac - (pp[None] <= pp[:, None])
    h15 = np.zeros((M, M))
    h15[:, M - 1] = frac[:, 0]
    hmat = np.concatenate([h15, t1], 1)
    acc = (pp[None] < pp[:, None]).astype(float)
    acc[:, M - 1] = 0
    acc = (acc - acc.mean(0)) / qq
    up = np.zeros((M, M))
    up[:-1, 1:] = np.eye(M - 1)
    keep = np.eye(M)
    keep[M - 1, M - 1] = 0
    ka = acc @ keep
    kt = -acc @ (keep @ up)
    kh = acc @ (keep @ (-(1 + 2 * a0) * np.eye(M) + b0 * up + b0 * up.T))
    s2x = s2.copy()
    s2x[M - 1, M - 1] = 1
    mats = np.zeros((15 * M, 128))
    mats[0:M, : 2 * M] = np.concatenate([sa, stt], 1)
    mats[M : 2 * M, :M] = s2
    mats[2 * M : 3 * M, : 2 * M] = hmat
    mats[3 * M : 4 * M, : 3 * M] = np.concatenate([ka, kt, kh], 1)
    mats[4 * M : 5 * M, : 4 * M] = winv
    mats[5 * M : 5 * M + M - 1, :] = np.cos(np.pi * t / M)[:, None]
    mats[6 * M : 7 * M, :M] = s2x
    mats[7 * M : 8 * M, :M] = t1.T
    mats[8 * M : 9 * M, :M] = ka.T * qq
    mats[9 * M : 10 * M, :M] = kt.T * qq
    mats[10 * M : 11 * M, :M] = (kh @ t1).T
    mats[11 * M : 15 * M, :M] = wfwd
    out = dict(q=q, sp=sp, r=r, vec=vec, glob=glob, cb=cb, acs=acs, mats=mats)
    return {name: np.asarray(value, np.float32) for name, value in out.items()}


def split(a):
    high = a.astype(bf16)
    return high, (a - high.astype(f32)).astype(bf16)


def mm(a, b, ca, cb):
    return lax.dot_general(a, b, (((ca,), (cb,)), ((), ())), preferred_element_type=f32)


def dot3(a, b, ca=1, cb=0):
    ah, al = a if isinstance(a, tuple) else split(a)
    bh, bl = b if isinstance(b, tuple) else split(b)
    return mm(ah, bh, ca, cb) + (mm(ah, bl, ca, cb) + mm(al, bh, ca, cb))


def doth(a, b, ca=1, cb=0):
    return lax.dot_general(
        a, b, (((ca,), (cb,)), ((), ())), precision=lax.Precision.HIGHEST, preferred_element_type=f32
    )


def rows_of(shape):
    return lax.broadcasted_iota(jnp.int32, shape, 0)


def lanes_of(shape):
    return lax.broadcasted_iota(jnp.int32, shape, 1)


def pick(values, index):
    return jnp.sum(jnp.where(rows_of(values.shape) == index, values, 0.0), 0, keepdims=True)


def below(values):
    return jnp.concatenate([jnp.zeros_like(values[:1]), values[:-1]], 0)


def edge_solve(al, t0, lead, e, couple, source, mats, special):
    M, n = al.shape
    L = min(n, 128)
    last = rows_of((M, n)) == M - 1
    both = jnp.concatenate([jnp.where(last, al * couple, al), t0], 0)
    modes = doth(mats[0:M, : 2 * M], both)
    cosphi = mats[5 * M : 6 * M, :1]
    modes = modes * (lead / (1.0 + e * e - 2.0 * e * cosphi))
    H = jnp.where(last, al, doth(mats[M : 2 * M, :M], modes))
    Hz = doth(mats[2 * M : 3 * M, : 2 * M], jnp.concatenate([al[:, :L], source], 0))
    mean = doth(mats[3 * M : 4 * M, : 3 * M], jnp.concatenate([al[:, :L], t0[:, :L], Hz], 0))
    lane = lanes_of((M, L))
    first = jnp.where((lane == 0) & special, Hz, H[:, :L])
    H = first if n == L else jnp.concatenate([first, H[:, L:]], 1)
    return H, jnp.where(special, mean[:, :1], 0.0)


def to_peers(rows, members):
    one = jnp.concatenate(rows, 0)
    return jnp.broadcast_to(one[None], (members,) + one.shape)


def stage_local(r, c, M, gx, gy, q, sp, rr, vec):
    gx, gy, q, sp, rr, vec = gx[...], gy[...], q[...], sp[...], rr[...], vec[...]
    n = q.shape[0]
    L = min(n, 128)
    qs, ss = split(q), split(sp)
    gys = split(gy)
    m1 = dot3(gx, qs, 1, 1)
    m2 = dot3(gys, ss, 1, 1)
    u = -(dot3(ss, m1) + dot3(qs, m2)) * rr
    slab = (gys[0][:, n - L :], gys[1][:, n - L :])
    gyl = dot3(slab, qs, 0, 1)[L - 1 :]
    us = split(u)
    tk = dot3(vec, us, 1, 1)
    tl = dot3(vec, us, 1, 0)
    alpha = gyl + jnp.where(c < M - 1, tk[1:2], 0.0)
    beta = m1[n - 1 :] + jnp.where(r < M - 1, tl[1:2], 0.0)
    return u, to_peers([alpha, tk[0:1], beta, tl[0:1]], M)


def lane_pick(values, index):
    return jnp.sum(jnp.where(lanes_of(values.shape) == index, values, 0.0), 1, keepdims=True)


def stage_strip(r, c, M, ag, q, rr, vec, glob, cb, acs, mats):
    al, t0, be, ta0 = (ag[:, a, :] for a in range(4))
    vec, mats = vec[...], mats[...]
    n = al.shape[1]
    half = n // 2
    q0, q1, lead, e, couple = (vec[a : a + 1] for a in range(5))
    L = min(n, 128)
    qq = 1.0 / math.sqrt(n)
    zero = jnp.zeros((M, L), f32)
    sa, stt, s2 = mats[:M, :M], mats[:M, M : 2 * M], mats[M : 2 * M, :M]
    cosphi = mats[5 * M : 6 * M, :1]

    H, mean = edge_solve(al, t0, lead, e, couple, zero, mats, True)
    Z = doth(jnp.concatenate([H * q0, H * q1], 0), rr[...])
    add0 = q0 * below(Z[:M]) - q1 * Z[:M]
    add1 = q0 * below(Z[M:]) - q1 * Z[M:]
    flat = jnp.where(lanes_of((M, n)) == 0, mean * qq, 0.0)
    tau0 = ta0 + add0 + flat
    tau1 = be + jnp.where(r < M - 1, add1 + flat, 0.0)

    y = doth(jnp.concatenate([tau1, tau0], 0), q[...])
    wf = mats[11 * M : 15 * M, :M]
    ca, sna = acs[0 : 2 * M, :], acs[2 * M : 4 * M, :]
    turned = []
    for side in range(2):
        g = doth(wf, y[side * M : (side + 1) * M])
        C, S = g[: 2 * M], g[2 * M :]
        turned.append(jnp.concatenate([C * ca - S * sna, -(C * sna + S * ca)], 1))
    T = doth(jnp.concatenate(turned, 0), cb[...], 1, 1)
    shape = (2 * M, half)
    origin = (rows_of(shape) == 0) & (lanes_of(shape) == 0)
    scale = jnp.where(origin, math.sqrt(1.0 / (n * M)), math.sqrt(2.0 / (n * M)))
    T1, T0 = T[: 2 * M] * scale, T[2 * M :] * scale

    own = rows_of((M, L)) == r
    alz = jnp.where(own, T1[:1, :1], 0.0)
    t0z = jnp.where(own, T0[:1, :1], 0.0)
    src = jnp.where(own, al[M - 1 :, :1] * (1.0 / math.sqrt(M)), 0.0)
    Hz = doth(mats[2 * M : 3 * M, : 2 * M], jnp.concatenate([alz, src], 0))
    lift = doth(mats[3 * M : 4 * M, : 3 * M], jnp.concatenate([alz, t0z, Hz], 0))
    g0 = jnp.where(rows_of((M, L)) == M - 1, Hz, doth(s2, Hz))
    ge = glob[1]
    up, down = lane_pick(sa, r), lane_pick(stt, r)
    T1c = jnp.where(r == M - 1, T1 * glob[2], T1)
    top, bottom = glob[0] * T1c, glob[0] * T0
    quad = 1.0 + ge * ge
    modes = []
    for m in range(M - 1):
        value = (up[m : m + 1] * top + down[m : m + 1] * bottom) / (
            quad - ge * (2.0 * cosphi[m : m + 1])
        )
        modes.append(jnp.where(origin, g0[m : m + 1, :1], value) * scale)
    modes.append(jnp.where(r == M - 1, T1, 0.0) * scale)
    XX = dot3(jnp.concatenate(modes, 0), cb[...])
    wi = split(mats[4 * M : 5 * M, : 4 * M])
    lines = []
    for m in range(M):
        xc, xs = XX[2 * M * m : 2 * M * (m + 1), :n], XX[2 * M * m : 2 * M * (m + 1), n:]
        lines.append(dot3(wi, jnp.concatenate([ca * xc - sna * xs, sna * xc + ca * xs], 0)))
    hx = dot3(jnp.concatenate(lines, 0), q[...], 1, 1)
    rs = split(rr[...])
    Y0, Y1 = dot3(hx * q0, rs), dot3(hx * q1, rs)

    D = lead / (1.0 + e * e - 2.0 * e * cosphi)
    inner = rows_of((M, n)) < M - 1
    first = lanes_of((1, n)) == 0
    cols = []
    for cc in (c, c - 1):
        KD = lane_pick(s2, cc) * D
        k1 = jnp.where(inner, doth(sa, KD, 0, 0), 0.0)
        k2 = doth(stt, KD, 0, 0)
        ksrc = lane_pick(mats[7 * M : 8 * M, :M], cc) * (-1.0 / qq)
        cols.append((k1, k2, ksrc))
    ka, kt = lane_pick(mats[8 * M : 9 * M, :M], c), lane_pick(mats[9 * M : 10 * M, :M], c)
    kth = lane_pick(mats[10 * M : 11 * M, :M], c)
    here, side_c, side_b, level = [], [], [], []
    for m in range(M):
        rows = slice(M * m, M * (m + 1))
        hm, y0, y1 = hx[rows], Y0[rows], Y1[rows]
        here.append(pick(hm, c))
        for (k1, k2, ksrc), sides in zip(cols, (side_c, side_b)):
            phi = jnp.sum(k1 * y1 + k2 * y0, 0, keepdims=True)
            z = jnp.sum(ksrc * hm, 0, keepdims=True)
            sides.append(jnp.where(first, z, phi))
        level.append(
            jnp.sum(kth * hm[:, :L] - ka * y1[:, :L] - kt * y0[:, :L], 0, keepdims=True)
        )
    s2x = mats[6 * M : 7 * M, :M]
    mixed = [doth(s2x, jnp.concatenate(v, 0)) for v in (here, side_c, side_b, level)]
    right, fc, fb, lv = mixed
    lv = (lv - below(lv) + lift * (1.0 / math.sqrt(M)))[:, :1]
    share = [
        below(right),
        right,
        q0 * below(fc) - q1 * fc,
        q0 * below(fb) - q1 * fb,
        jnp.broadcast_to(lv, (M, n)),
    ]
    keep = [pick(H, c), pick(H, c - 1), jnp.broadcast_to(pick(mean, c), (1, n))]
    return share, jnp.concatenate(keep + [jnp.zeros((5, n), f32)], 0)


def stage_field(r, c, M, share, keep, u, q, rr, vec):
    keep, vec = keep[...], vec[...]
    n = q.shape[0]
    q0, q1 = vec[0:1], vec[1:2]
    left, right, here, before, level = (
        jnp.sum(share[:, a, :], 0, keepdims=True) for a in range(5)
    )
    here = here + keep[0:1]
    before = before + keep[1:2]
    level = (level + keep[2:3])[:, :1]
    pad = jnp.zeros((4, n), f32)
    lhs = jnp.concatenate([q1, -q0, here, -before, pad], 0)
    rhs = jnp.concatenate([right, left, q1, q0, pad], 0)
    G = doth(lhs, rhs, 0, 0)
    un = u[...] - rr[...] * G
    un = jnp.where((rows_of(un.shape) == 0) & (lanes_of(un.shape) == 0), level, un)
    qs = split(q[...])
    return (dot3(qs, dot3(un, qs), 0, 0),)


def run_stage(stage, members, outs, *args):
    r, c = lax.axis_index("row"), lax.axis_index("col")
    if DIRECT:
        results = stage(r, c, members, *args)
        return [jnp.stack(v, 1) if isinstance(v, list) else v for v in results]

    def kernel(place, *refs):
        results = stage(place[0], place[1], members, *refs[: len(args)])
        for ref, value in zip(refs[len(args) :], results):
            if isinstance(value, list):
                for a, row in enumerate(value):
                    ref[:, a, :] = row
            else:
                ref[...] = value

    place = jnp.stack([r, c]).astype(jnp.int32)
    vmem = pl.BlockSpec(memory_space=pltpu.VMEM)
    return pl.pallas_call(
        kernel,
        out_shape=[jax.ShapeDtypeStruct(shape, f32) for shape in outs],
        in_specs=[pl.BlockSpec(memory_space=pltpu.SMEM)] + [vmem] * len(args),
        out_specs=[vmem] * len(outs),
        compiler_params=pltpu.CompilerParams(vmem_limit_bytes=56 * 1024 * 1024),
        name=stage.__name__,
    )(place, *args)


def exchange(values, axis):
    return lax.all_to_all(values, axis, split_axis=0, concat_axis=0, tiled=True)


def make_body(members):
    def body(grad_x, grad_y):
        n = grad_x.shape[0]
        t = {k: jnp.asarray(v) for k, v in build_tables(n, members).items()}
        edge = (members, 4, n)
        u, edges = run_stage(
            stage_local, members, [(n, n), edge], grad_x, grad_y, t["q"], t["sp"], t["r"], t["vec"]
        )
        strip = exchange(edges, "col")
        share, keep = run_stage(
            stage_strip, members, [(members, 5, n), (8, n)],
            strip, t["q"], t["r"], t["vec"], t["glob"], t["cb"], t["acs"], t["mats"],
        )
        share = exchange(share, "row")
        (field,) = run_stage(
            stage_field, members, [(n, n)], share, keep, u, t["q"], t["r"], t["vec"]
        )
        return field

    return body


def solution(mesh):
    members = mesh.shape["row"]
    placed = (P("row", "col"), P("row", "col"))
    return jax.shard_map(
        make_body(members), mesh=mesh, in_specs=placed, out_specs=P("row", "col"), check_vma=False
    )
```

```python
import math

import jax
import jax.numpy as jnp
import numpy as np
from jax import lax
from jax.experimental import pallas as pl
from jax.experimental.pallas import tpu as pltpu
from jax.sharding import PartitionSpec as P

DIRECT = False
f32 = jnp.float32
bf16 = jnp.bfloat16


def cosine_basis(n):
    k, i = np.arange(n)[:, None], np.arange(n)[None]
    return np.sqrt(np.where(k == 0, 1, 2) / n) * np.cos(np.pi * k * (2 * i + 1) / (2 * n))


def edge_tables(n, members, freq):
    s = 2 * np.sin(freq)
    half = np.arcsinh(s / 2)
    e = np.exp(-2 * n * half)
    safe = np.where(s == 0, 1, s)
    e1 = np.where(s == 0, 0.5, e)
    th = np.tanh(np.arcsinh(safe / 2))
    one = np.where(s == 0, 0, 1)
    lead = one * th * (1 - e1 * e1)
    couple = one * e1 / (th * (1 - e1 * e1))
    return lead, e, couple


def build_tables(n, members):
    total = n * members
    half = n // 2
    k = np.concatenate([np.arange(0, n, 2), np.arange(1, n, 2)])
    q = cosine_basis(n)[k]
    s = 2 * np.sin(np.pi * k / (2 * n))
    q0, q1 = q[:, 0], q[:, -1]
    lead, e, couple = edge_tables(n, members, np.pi * k / (2 * n))
    vec = np.zeros((8, n))
    vec[0], vec[1], vec[2], vec[3], vec[4] = q0, q1, lead, e, couple
    vec[5], vec[6] = s * s, 1
    m = np.arange(half)
    cls = np.arange(2 * members)
    kap = cls[:, None] + 2 * members * m[None]
    glob = np.stack(edge_tables(n, members, np.pi * kap / (2 * total)))
    j = 2 * np.arange(n) + 1
    sb = np.sqrt(2 / n) * np.sin(np.pi * m[:, None] * j[None] / n)
    ang = np.pi * cls[:, None] * j[None] / (2 * total)
    acs = np.concatenate([np.cos(ang), np.sin(ang)], 0)
    p = np.arange(members)
    wang = np.pi * cls[:, None] * p[None] / members
    wc, ws = np.cos(wang), np.sin(wang)
    wfwd = np.concatenate([wc, ws], 0)
    winv = np.concatenate([wc.T, -ws.T], 1)
    M = members
    t = np.arange(1, M)
    st = np.sqrt(2 / M) * np.sin(np.pi * np.outer(t, t) / M)
    sa, stt, s2 = np.zeros((M, M)), np.zeros((M, M)), np.zeros((M, M))
    sa[: M - 1, : M - 1] = st
    sa[: M - 1, M - 1] = st[:, M - 2]
    stt[: M - 1, 1:] = -st
    s2[: M - 1, : M - 1] = st
    a0 = (q1[1:] ** 2 / s[1:] ** 2).sum()
    b0 = (q0[1:] * q1[1:] / s[1:] ** 2).sum()
    qq = 1 / np.sqrt(n)
    pp = np.arange(M)
    frac = (pp[:, None] + 1) / M
    t1 = frac - (pp[None] <= pp[:, None])
    h15 = np.zeros((M, M))
    h15[:, M - 1] = frac[:, 0]
    hmat = np.concatenate([h15, t1], 1)
    acc = (pp[None] < pp[:, None]).astype(float)
    acc[:, M - 1] = 0
    acc = (acc - acc.mean(0)) / qq
    up = np.zeros((M, M))
    up[:-1, 1:] = np.eye(M - 1)
    keep = np.eye(M)
    keep[M - 1, M - 1] = 0
    ka = acc @ keep
    kt = -acc @ (keep @ up)
    kh = acc @ (keep @ (-(1 + 2 * a0) * np.eye(M) + b0 * up + b0 * up.T))
    s2x = s2.copy()
    s2x[M - 1, M - 1] = 1
    mats = np.zeros((15 * M, 128))
    mats[0:M, : 2 * M] = np.concatenate([sa, stt], 1)
    mats[M : 2 * M, :M] = s2
    mats[2 * M : 3 * M, : 2 * M] = hmat
    mats[3 * M : 4 * M, : 3 * M] = np.concatenate([ka, kt, kh], 1)
    mats[4 * M : 5 * M, : 4 * M] = winv
    mats[5 * M : 5 * M + M - 1, :] = np.cos(np.pi * t / M)[:, None]
    mats[6 * M : 7 * M, :M] = s2x
    mats[7 * M : 8 * M, :M] = t1.T
    mats[8 * M : 9 * M, :M] = ka.T * qq
    mats[9 * M : 10 * M, :M] = kt.T * qq
    mats[10 * M : 11 * M, :M] = (kh @ t1).T
    mats[11 * M : 15 * M, :M] = wfwd
    out = dict(q=q, vec=vec, glob=glob, sb=sb, acs=acs, mats=mats)
    return {name: np.asarray(value, np.float32) for name, value in out.items()}


def split(a):
    high = a.astype(bf16)
    return high, (a - high.astype(f32)).astype(bf16)


def mm(a, b, ca, cb):
    return lax.dot_general(a, b, (((ca,), (cb,)), ((), ())), preferred_element_type=f32)


def dot3(a, b, ca=1, cb=0):
    ah, al = a if isinstance(a, tuple) else split(a)
    bh, bl = b if isinstance(b, tuple) else split(b)
    return mm(ah, bh, ca, cb) + (mm(ah, bl, ca, cb) + mm(al, bh, ca, cb))


def doth(a, b, ca=1, cb=0):
    return lax.dot_general(
        a, b, (((ca,), (cb,)), ((), ())), precision=lax.Precision.HIGHEST, preferred_element_type=f32
    )


def rows_of(shape):
    return lax.broadcasted_iota(jnp.int32, shape, 0)


def lanes_of(shape):
    return lax.broadcasted_iota(jnp.int32, shape, 1)


def pick(values, index):
    return jnp.sum(jnp.where(rows_of(values.shape) == index, values, 0.0), 0, keepdims=True)


def below(values):
    return jnp.concatenate([jnp.zeros_like(values[:1]), values[:-1]], 0)


def edge_solve(al, t0, lead, e, couple, source, mats, special):
    M, n = al.shape
    L = min(n, 128)
    last = rows_of((M, n)) == M - 1
    both = jnp.concatenate([jnp.where(last, al * couple, al), t0], 0)
    modes = doth(mats[0:M, : 2 * M], both)
    cosphi = mats[5 * M : 6 * M, :1]
    modes = modes * (lead / (1.0 + e * e - 2.0 * e * cosphi))
    H = jnp.where(last, al, doth(mats[M : 2 * M, :M], modes))
    Hz = doth(mats[2 * M : 3 * M, : 2 * M], jnp.concatenate([al[:, :L], source], 0))
    mean = doth(mats[3 * M : 4 * M, : 3 * M], jnp.concatenate([al[:, :L], t0[:, :L], Hz], 0))
    lane = lanes_of((M, L))
    first = jnp.where((lane == 0) & special, Hz, H[:, :L])
    H = first if n == L else jnp.concatenate([first, H[:, L:]], 1)
    return H, jnp.where(special, mean[:, :1], 0.0)


def to_peers(rows, members):
    one = jnp.concatenate(rows, 0)
    return jnp.broadcast_to(one[None], (members,) + one.shape)


def stage_local(r, c, M, gx, gy, q, vec):
    q, vec = q[...], vec[...]
    n = q.shape[0]
    L = min(n, 128)
    one, two = vec[6:7], vec[5:6]
    pad = jnp.zeros((6, n), f32)
    den = doth(jnp.concatenate([two, one, pad], 0), jnp.concatenate([one, two, pad], 0), 0, 0)
    origin = (rows_of(den.shape) == 0) & (lanes_of(den.shape) == 0)
    rr = jnp.where(origin, 0.0, 1.0 / jnp.where(origin, 1.0, den))
    after = jnp.concatenate([q[:, 1:], q[:, :1]], 1)
    sp = jnp.where(lanes_of(q.shape) == n - 1, 0.0, q - after)
    qs, ss = split(q), split(sp)
    m1 = dot3(gx[...], qs, 1, 1)
    gys = split(gy[...])
    m2 = dot3(gys, ss, 1, 1)
    u = -(dot3(ss, m1) + dot3(qs, m2)) * rr
    slab = (gys[0][:, n - L :], gys[1][:, n - L :])
    gyl = dot3(slab, qs, 0, 1)[L - 1 :]
    us = split(u)
    tk = dot3(vec, us, 1, 1)
    tl = dot3(vec, us, 1, 0)
    alpha = gyl + jnp.where(c < M - 1, tk[1:2], 0.0)
    beta = m1[n - 1 :] + jnp.where(r < M - 1, tl[1:2], 0.0)
    return to_peers([alpha, tk[0:1], beta, tl[0:1]], M), u, q, qs[0], qs[1], rr


def lane_pick(values, index):
    return jnp.sum(jnp.where(lanes_of(values.shape) == index, values, 0.0), 1, keepdims=True)


def stage_strip(r, c, M, ag, q, qh, ql, rr, vec, glob, sb, acs, mats):
    al, t0, be, ta0 = (ag[:, a, :] for a in range(4))
    vec, mats = vec[...], mats[...]
    n = al.shape[1]
    half = n // 2
    q0, q1, lead, e, couple = (vec[a : a + 1] for a in range(5))
    L = min(n, 128)
    qq = 1.0 / math.sqrt(n)
    zero = jnp.zeros((M, L), f32)
    sa, stt, s2 = mats[:M, :M], mats[:M, M : 2 * M], mats[M : 2 * M, :M]
    cosphi = mats[5 * M : 6 * M, :1]

    H, mean = edge_solve(al, t0, lead, e, couple, zero, mats, True)
    Z = doth(jnp.concatenate([H * q0, H * q1], 0), rr[...])
    add0 = q0 * below(Z[:M]) - q1 * Z[:M]
    add1 = q0 * below(Z[M:]) - q1 * Z[M:]
    flat = jnp.where(lanes_of((M, n)) == 0, mean * qq, 0.0)
    tau0 = ta0 + add0 + flat
    tau1 = be + jnp.where(r < M - 1, add1 + flat, 0.0)

    y = doth(jnp.concatenate([tau1, tau0], 0), q[...])
    wf = mats[11 * M : 15 * M, :M]
    ca, sna = acs[0 : 2 * M, :], acs[2 * M : 4 * M, :]
    turned = []
    for side in range(2):
        g = doth(wf, y[side * M : (side + 1) * M])
        C, S = g[: 2 * M], g[2 * M :]
        turned.append(jnp.concatenate([C * ca - S * sna, -(C * sna + S * ca)], 1))
    turned = jnp.concatenate(turned, 0)
    T = doth(turned[:, :n], q[:half, :], 1, 1) + doth(turned[:, n:], sb[...], 1, 1)
    shape = (2 * M, half)
    zeroth = lanes_of(shape) == 0
    origin = (rows_of(shape) == 0) & zeroth
    root = 1.0 / math.sqrt(M)
    scale = jnp.where(zeroth & (rows_of(shape) > 0), root * math.sqrt(2.0), root)
    T1, T0 = T[: 2 * M] * scale, T[2 * M :] * scale

    own = rows_of((M, L)) == r
    alz = jnp.where(own, T1[:1, :1], 0.0)
    t0z = jnp.where(own, T0[:1, :1], 0.0)
    src = jnp.where(own, al[M - 1 :, :1] * (1.0 / math.sqrt(M)), 0.0)
    Hz = doth(mats[2 * M : 3 * M, : 2 * M], jnp.concatenate([alz, src], 0))
    lift = doth(mats[3 * M : 4 * M, : 3 * M], jnp.concatenate([alz, t0z, Hz], 0))
    g0 = jnp.where(rows_of((M, L)) == M - 1, Hz, doth(s2, Hz))
    ge = glob[1]
    up, down = lane_pick(sa, r), lane_pick(stt, r)
    T1c = jnp.where(r == M - 1, T1 * glob[2], T1)
    top, bottom = glob[0] * T1c, glob[0] * T0
    quad = 1.0 + ge * ge
    modes = []
    for m in range(M - 1):
        value = (up[m : m + 1] * top + down[m : m + 1] * bottom) / (
            quad - ge * (2.0 * cosphi[m : m + 1])
        )
        modes.append(jnp.where(origin, g0[m : m + 1, :1], value) * scale)
    modes.append(jnp.where(r == M - 1, T1, 0.0) * scale)
    modes = split(jnp.concatenate(modes, 0))
    XC = dot3(modes, (qh[:half, :], ql[:half, :]))
    XS = dot3(modes, sb[...])
    wi = split(mats[4 * M : 5 * M, : 4 * M])
    lines = []
    for m in range(M):
        xc, xs = XC[2 * M * m : 2 * M * (m + 1)], XS[2 * M * m : 2 * M * (m + 1)]
        lines.append(dot3(wi, jnp.concatenate([ca * xc - sna * xs, sna * xc + ca * xs], 0)))
    hx = dot3(jnp.concatenate(lines, 0), (qh[...], ql[...]), 1, 1)
    rs = split(rr[...])
    Y0, Y1 = dot3(hx * q0, rs), dot3(hx * q1, rs)

    D = lead / (1.0 + e * e - 2.0 * e * cosphi)
    inner = rows_of((M, n)) < M - 1
    first = lanes_of((1, n)) == 0
    cols = []
    for cc in (c, c - 1):
        KD = lane_pick(s2, cc) * D
        k1 = jnp.where(inner, doth(sa, KD, 0, 0), 0.0)
        k2 = doth(stt, KD, 0, 0)
        ksrc = lane_pick(mats[7 * M : 8 * M, :M], cc) * (-1.0 / qq)
        cols.append((k1, k2, ksrc))
    ka, kt = lane_pick(mats[8 * M : 9 * M, :M], c), lane_pick(mats[9 * M : 10 * M, :M], c)
    kth = lane_pick(mats[10 * M : 11 * M, :M], c)
    here, side_c, side_b, level = [], [], [], []
    for m in range(M):
        rows = slice(M * m, M * (m + 1))
        hm, y0, y1 = hx[rows], Y0[rows], Y1[rows]
        here.append(pick(hm, c))
        for (k1, k2, ksrc), sides in zip(cols, (side_c, side_b)):
            phi = jnp.sum(k1 * y1 + k2 * y0, 0, keepdims=True)
            z = jnp.sum(ksrc * hm, 0, keepdims=True)
            sides.append(jnp.where(first, z, phi))
        level.append(
            jnp.sum(kth * hm[:, :L] - ka * y1[:, :L] - kt * y0[:, :L], 0, keepdims=True)
        )
    s2x = mats[6 * M : 7 * M, :M]
    mixed = [doth(s2x, jnp.concatenate(v, 0)) for v in (here, side_c, side_b, level)]
    right, fc, fb, lv = mixed
    lv = (lv - below(lv) + lift * (1.0 / math.sqrt(M)))[:, :1]
    share = [
        below(right),
        right,
        q0 * below(fc) - q1 * fc,
        q0 * below(fb) - q1 * fb,
        jnp.broadcast_to(lv, (M, n)),
    ]
    keep = [pick(H, c), pick(H, c - 1), jnp.broadcast_to(pick(mean, c), (1, n))]
    return share, jnp.concatenate(keep + [jnp.zeros((5, n), f32)], 0)


def stage_field(r, c, M, share, keep, u, qh, ql, rr, vec):
    keep, vec = keep[...], vec[...]
    n = vec.shape[1]
    q0, q1 = vec[0:1], vec[1:2]
    left, right, here, before, level = (
        jnp.sum(share[:, a, :], 0, keepdims=True) for a in range(5)
    )
    here = here + keep[0:1]
    before = before + keep[1:2]
    level = (level + keep[2:3])[:, :1]
    pad = jnp.zeros((4, n), f32)
    lhs = jnp.concatenate([q1, -q0, here, -before, pad], 0)
    rhs = jnp.concatenate([right, left, q1, q0, pad], 0)
    G = doth(lhs, rhs, 0, 0)
    un = u[...] - rr[...] * G
    un = jnp.where((rows_of(un.shape) == 0) & (lanes_of(un.shape) == 0), level, un)
    qs = (qh[...], ql[...])
    return (dot3(qs, dot3(un, qs), 0, 0),)


def run_stage(stage, members, outs, *args):
    if DIRECT:
        results = stage(lax.axis_index("row"), lax.axis_index("col"), members, *args)
        return [jnp.stack(v, 1) if isinstance(v, list) else v for v in results]

    def kernel(*refs):
        r, c = lax.axis_index("row"), lax.axis_index("col")
        results = stage(r, c, members, *refs[: len(args)])
        for ref, value in zip(refs[len(args) :], results):
            if isinstance(value, list):
                for a, row in enumerate(value):
                    ref[:, a, :] = row
            else:
                ref[...] = value

    vmem = pl.BlockSpec(memory_space=pltpu.VMEM)
    return pl.pallas_call(
        kernel,
        out_shape=outs,
        in_specs=[vmem] * len(args),
        out_specs=[vmem] * len(outs),
        compiler_params=pltpu.CompilerParams(vmem_limit_bytes=40 * 1024 * 1024),
        name=stage.__name__,
    )(*args)


def exchange(values, axis):
    return lax.all_to_all(values, axis, split_axis=0, concat_axis=0, tiled=True)


def make_body(members):
    def body(grad_x, grad_y):
        n = grad_x.shape[0]
        t = {k: jnp.asarray(v) for k, v in build_tables(n, members).items()}
        sent, near = jax.ShapeDtypeStruct, pltpu.VMEM
        edges, u, q, qh, ql, rr = run_stage(
            stage_local,
            members,
            [sent((members, 4, n), f32), near((n, n), f32), near((n, n), f32)]
            + [near((n, n), bf16), near((n, n), bf16), near((n, n), f32)],
            grad_x, grad_y, t["q"], t["vec"],
        )
        strip = exchange(edges, "col")
        share, keep = run_stage(
            stage_strip, members, [sent((members, 5, n), f32), near((8, n), f32)],
            strip, q, qh, ql, rr, t["vec"], t["glob"], t["sb"], t["acs"], t["mats"],
        )
        share = exchange(share, "row")
        (field,) = run_stage(
            stage_field, members, [sent((n, n), f32)], share, keep, u, qh, ql, rr, t["vec"]
        )
        return field

    return body


def solution(mesh):
    members = mesh.shape["row"]
    placed = (P("row", "col"), P("row", "col"))
    return jax.shard_map(
        make_body(members), mesh=mesh, in_specs=placed, out_specs=P("row", "col"), check_vma=False
    )
```

```python
import math

import jax
import jax.numpy as jnp
import numpy as np
from jax import lax
from jax.experimental import pallas as pl
from jax.experimental.pallas import tpu as pltpu
from jax.sharding import PartitionSpec as P

VMEM_LIMIT = 32 * 1024 * 1024
DIRECT = False
f32 = jnp.float32
bf16 = jnp.bfloat16


def cosine_basis(n):
    k, i = np.arange(n)[:, None], np.arange(n)[None]
    return np.sqrt(np.where(k == 0, 1, 2) / n) * np.cos(np.pi * k * (2 * i + 1) / (2 * n))


def edge_tables(n, members, freq):
    s = 2 * np.sin(freq)
    half = np.arcsinh(s / 2)
    e = np.exp(-2 * n * half)
    safe = np.where(s == 0, 1, s)
    e1 = np.where(s == 0, 0.5, e)
    th = np.tanh(np.arcsinh(safe / 2))
    one = np.where(s == 0, 0, 1)
    lead = one * th * (1 - e1 * e1)
    couple = one * e1 / (th * (1 - e1 * e1))
    return lead, e, couple


def build_tables(n, members):
    total = n * members
    half = n // 2
    k = np.concatenate([np.arange(0, n, 2), np.arange(1, n, 2)])
    q = cosine_basis(n)[k]
    s = 2 * np.sin(np.pi * k / (2 * n))
    q0, q1 = q[:, 0], q[:, -1]
    lead, e, couple = edge_tables(n, members, np.pi * k / (2 * n))
    vec = np.zeros((8, n))
    vec[0], vec[1], vec[2], vec[3], vec[4] = q0, q1, lead, e, couple
    m = np.arange(half)
    cls = np.arange(2 * members)
    kap = cls[:, None] + 2 * members * m[None]
    glob = np.stack(edge_tables(n, members, np.pi * kap / (2 * total)))
    bend = 1 + glob[1] ** 2 - 2 * glob[1] * np.cos(np.pi * np.arange(1, members) / members)[:, None, None]
    size = np.full((2 * members, half), 1 / np.sqrt(members))
    size[1:, 0] *= np.sqrt(2)
    dens = (glob[0] * size / bend).reshape(-1, half)
    j = 2 * np.arange(n) + 1
    sb = np.sqrt(2 / n) * np.sin(np.pi * m[:, None] * j[None] / n)
    turn = np.concatenate([q[:half].T, sb.T], 0)
    sp = np.sqrt(2 / n) * s[:, None] * np.sin(np.pi * k[:, None] * (np.arange(n)[None] + 1) / n)
    sp[:, n - 1] = 0
    sp[0] = 0
    den = s[:, None] ** 2 + s[None] ** 2
    den[0, 0] = 1
    r = 1 / den
    r[0, 0] = 0
    ang = np.pi * cls[:, None] * j[None] / (2 * total)
    acs = np.concatenate([np.cos(ang), np.sin(ang)], 0)
    p = np.arange(members)
    wang = np.pi * cls[:, None] * p[None] / members
    wc, ws = np.cos(wang), np.sin(wang)
    wfwd = np.concatenate([wc, ws], 0)
    winv = np.concatenate([wc.T, -ws.T], 1)
    M = members
    t = np.arange(1, M)
    st = np.sqrt(2 / M) * np.sin(np.pi * np.outer(t, t) / M)
    sa, stt, s2 = np.zeros((M, M)), np.zeros((M, M)), np.zeros((M, M))
    sa[: M - 1, : M - 1] = st
    sa[: M - 1, M - 1] = st[:, M - 2]
    stt[: M - 1, 1:] = -st
    s2[: M - 1, : M - 1] = st
    a0 = (q1[1:] ** 2 / s[1:] ** 2).sum()
    b0 = (q0[1:] * q1[1:] / s[1:] ** 2).sum()
    qq = 1 / np.sqrt(n)
    pp = np.arange(M)
    frac = (pp[:, None] + 1) / M
    t1 = frac - (pp[None] <= pp[:, None])
    h15 = np.zeros((M, M))
    h15[:, M - 1] = frac[:, 0]
    hmat = np.concatenate([h15, t1], 1)
    acc = (pp[None] < pp[:, None]).astype(float)
    acc[:, M - 1] = 0
    acc = (acc - acc.mean(0)) / qq
    up = np.zeros((M, M))
    up[:-1, 1:] = np.eye(M - 1)
    keep = np.eye(M)
    keep[M - 1, M - 1] = 0
    ka = acc @ keep
    kt = -acc @ (keep @ up)
    kh = acc @ (keep @ (-(1 + 2 * a0) * np.eye(M) + b0 * up + b0 * up.T))
    s2x = s2.copy()
    s2x[M - 1, M - 1] = 1
    mats = np.zeros((15 * M, 128))
    per = min(M, n // (2 * M), 256 // (4 * M))
    wbd = np.kron(np.eye(per), winv)
    mats[0:M, : 2 * M] = np.concatenate([sa, stt], 1)
    mats[M : 2 * M, :M] = s2
    mats[2 * M : 3 * M, : 2 * M] = hmat
    mats[3 * M : 4 * M, : 3 * M] = np.concatenate([ka, kt, kh], 1)
    mats[4 * M : 5 * M, : 4 * M] = winv
    mats[5 * M : 5 * M + M - 1, :] = np.cos(np.pi * t / M)[:, None]
    mats[6 * M : 7 * M, :M] = s2x
    mats[7 * M : 8 * M, :M] = t1.T
    mats[8 * M : 9 * M, :M] = ka.T * qq
    mats[9 * M : 10 * M, :M] = kt.T * qq
    mats[10 * M : 11 * M, :M] = (kh @ t1).T
    mats[11 * M : 15 * M, :M] = wfwd
    out = dict(r=r, vec=vec, couple=glob[2], dens=dens, acs=acs, mats=mats)
    out = {name: np.asarray(value, np.float32) for name, value in out.items()}
    for name, value, pieces in (
        ("q", q, 3), ("s", sp, 2), ("r", r, 3), ("t", turn, 3), ("b", sb, 2), ("w", wbd, 3)
    ):
        for i in range(pieces):
            out[f"{name}{i + 1}"] = np.asarray(value, jnp.bfloat16)
            value = value - out[f"{name}{i + 1}"].astype(np.float64)
    return out


def split(a):
    high = a.astype(bf16)
    return high, (a - high.astype(f32)).astype(bf16)


def mm(a, b, ca, cb):
    return lax.dot_general(a, b, (((ca,), (cb,)), ((), ())), preferred_element_type=f32)


def dot3(a, b, ca=1, cb=0):
    ah, al = a if isinstance(a, tuple) else split(a)
    bh, bl = b if isinstance(b, tuple) else split(b)
    return mm(ah, bh, ca, cb) + (mm(ah, bl, ca, cb) + mm(al, bh, ca, cb))


def split3(a):
    high, rest = a.astype(bf16), None
    rest = a - high.astype(f32)
    mid = rest.astype(bf16)
    return high, mid, (rest - mid.astype(f32)).astype(bf16)


def dot6(a, b, cb=0):
    m = a.shape[0]
    a1, a2, a3 = split3(a)
    b1, b2, b3 = b
    p = mm(jnp.concatenate([a1, a2, a3], 0), b1, 1, cb)
    q = mm(jnp.concatenate([a1, a2], 0), b2, 1, cb)
    small = (p[2 * m :] + q[m:]) + mm(a1, b3, 1, cb)
    return p[:m] + ((p[m : 2 * m] + q[:m]) + small)


def dotl(a, b):
    m = a[0].shape[0]
    b1, b2, b3 = split3(b)
    p = mm(jnp.concatenate(a, 0), b1, 1, 0)
    q = mm(jnp.concatenate(a[:2], 0), b2, 1, 0)
    small = (p[2 * m :] + q[m:]) + mm(a[0], b3, 1, 0)
    return p[:m] + ((p[m : 2 * m] + q[:m]) + small)


def doths(a, qs):
    value = dot3(a, qs, 1, 1)
    exact = jnp.sum(a, 1, keepdims=True) * (1.0 / math.sqrt(a.shape[1]))
    return jnp.where(lanes_of(value.shape) == 0, exact, value)


def doth(a, b, ca=1, cb=0):
    return lax.dot_general(
        a, b, (((ca,), (cb,)), ((), ())), precision=lax.Precision.HIGHEST, preferred_element_type=f32
    )


def rows_of(shape):
    return lax.broadcasted_iota(jnp.int32, shape, 0)


def lanes_of(shape):
    return lax.broadcasted_iota(jnp.int32, shape, 1)


def pick(values, index):
    return jnp.sum(jnp.where(rows_of(values.shape) == index, values, 0.0), 0, keepdims=True)


def below(values):
    return jnp.concatenate([jnp.zeros_like(values[:1]), values[:-1]], 0)


def edge_solve(al, t0, lead, e, couple, source, mats, special):
    M, n = al.shape
    L = min(n, 128)
    last = rows_of((M, n)) == M - 1
    both = jnp.concatenate([jnp.where(last, al * couple, al), t0], 0)
    modes = doth(mats[0:M, : 2 * M], both)
    cosphi = mats[5 * M : 6 * M, :1]
    modes = modes * (lead / (1.0 + e * e - 2.0 * e * cosphi))
    H = jnp.where(last, al, doth(mats[M : 2 * M, :M], modes))
    Hz = doth(mats[2 * M : 3 * M, : 2 * M], jnp.concatenate([al[:, :L], source], 0))
    mean = doth(mats[3 * M : 4 * M, : 3 * M], jnp.concatenate([al[:, :L], t0[:, :L], Hz], 0))
    lane = lanes_of((M, L))
    first = jnp.where((lane == 0) & special, Hz, H[:, :L])
    H = first if n == L else jnp.concatenate([first, H[:, L:]], 1)
    return H, jnp.where(special, mean[:, :1], 0.0)


def to_peers(rows, members):
    one = jnp.concatenate(rows, 0)
    return jnp.broadcast_to(one[None], (members,) + one.shape)


def stage_local(r, c, M, need, vec):
    vec = vec[...]
    n = vec.shape[1]
    L = min(n, 128)
    qs = (need("q1"), need("q2"))
    m1 = dot3(need("x"), qs, 1, 1)
    ss = (need("s1"), need("s2"))
    gys = split(need("y"))
    m2 = dot3(gys, ss, 1, 1)
    slab = (gys[0][:, n - L :], gys[1][:, n - L :])
    gyl = dot3(slab, qs, 0, 1)[L - 1 :]
    f = dot3(ss, m1) + dot3(qs, m2)
    u = -f * need("r")
    us = split(u)
    tk = dot3(vec, us, 1, 1)
    tl = dot3(vec, us, 1, 0)
    alpha = gyl + jnp.where(c < M - 1, tk[1:2], 0.0)
    beta = m1[n - 1 :] + jnp.where(r < M - 1, tl[1:2], 0.0)
    return to_peers([alpha, tk[0:1], beta, tl[0:1]], M), u


FIRST = ("q1", "q2", "x", "s1", "s2", "y", "r")
LATER = ("q3", "r1", "r2", "r3", "t1", "t2", "t3", "b1", "b2", "w1", "w2", "w3")
LATER += ("dens", "couple", "acs", "mats")
KEPT = ("q1", "q2", "r") + LATER


def run_local(members, arrays, vec):
    n = vec.shape[1]
    if DIRECT:
        edges, u = stage_local(
            lax.axis_index("row"), lax.axis_index("col"), members, arrays.__getitem__, vec
        )
        return edges, u, {name: arrays[name] for name in KEPT}

    names = FIRST + LATER

    def kernel(*refs):
        count = len(names)
        sources, vec = refs[:count], refs[count]
        edges, u = refs[count + 1 : count + 3]
        here = dict(zip(KEPT, refs[count + 3 :]))
        here.update(zip((k for k in FIRST if k not in KEPT), refs[count + 3 + len(KEPT) :]))
        sem = refs[-1]
        copies = {
            name: pltpu.make_async_copy(source, here[name], sem.at[i])
            for i, (name, source) in enumerate(zip(names, sources))
        }
        for name in FIRST:
            copies[name].start()

        def need(name):
            copies[name].wait()
            if name == "y":
                for later in LATER:
                    copies[later].start()
            return here[name][...]

        edges[...], u[...] = stage_local(
            lax.axis_index("row"), lax.axis_index("col"), members, need, vec
        )
        for name in LATER:
            copies[name].wait()

    far, vmem, near = pl.BlockSpec(memory_space=pltpu.HBM), pl.BlockSpec(memory_space=pltpu.VMEM), pltpu.VMEM
    shape = {name: near(arrays[name].shape, arrays[name].dtype) for name in names}
    edges, u, *tables = pl.pallas_call(
        kernel,
        out_shape=[jax.ShapeDtypeStruct((members, 4, n), f32), near((n, n), f32)]
        + [shape[name] for name in KEPT],
        in_specs=[far] * len(names) + [vmem],
        out_specs=[vmem] * (2 + len(KEPT)),
        scratch_shapes=[shape[name] for name in FIRST if name not in KEPT]
        + [pltpu.SemaphoreType.DMA((len(names),))],
        compiler_params=pltpu.CompilerParams(vmem_limit_bytes=VMEM_LIMIT),
        name="stage_local",
    )(*(pltpu.with_memory_space_constraint(arrays[name], pltpu.HBM) for name in names), vec)
    return edges, u, dict(zip(KEPT, tables))


def lane_pick(values, index):
    return jnp.sum(jnp.where(lanes_of(values.shape) == index, values, 0.0), 1, keepdims=True)


def stage_strip(
    r, c, M, ag, q1, q2, q3, r1, r2, r3, t1, t2, t3, b1, b2, w1, w2, w3, dens, gcouple, vec, acs, mats
):
    al, t0, be, ta0 = (ag[:, a, :] for a in range(4))
    vec, mats = vec[...], mats[...]
    n = al.shape[1]
    half = n // 2
    v0, v1, lead, e, couple = (vec[a : a + 1] for a in range(5))
    L = min(n, 128)
    qq = 1.0 / math.sqrt(n)
    zero = jnp.zeros((M, L), f32)
    sa, stt, s2 = mats[:M, :M], mats[:M, M : 2 * M], mats[M : 2 * M, :M]
    cosphi = mats[5 * M : 6 * M, :1]

    H, mean = edge_solve(al, t0, lead, e, couple, zero, mats, True)
    rs = (r1[...], r2[...])
    Z = dot6(jnp.concatenate([H * v0, H * v1], 0), rs + (r3[...],))
    add0 = v0 * below(Z[:M]) - v1 * Z[:M]
    add1 = v0 * below(Z[M:]) - v1 * Z[M:]
    flat = jnp.where(lanes_of((M, n)) == 0, mean * qq, 0.0)
    tau0 = ta0 + add0 + flat
    tau1 = be + jnp.where(r < M - 1, add1 + flat, 0.0)

    qs = (q1[...], q2[...])
    y = dot6(jnp.concatenate([tau1, tau0], 0), qs + (q3[...],))
    wf = mats[11 * M : 15 * M, :M]
    ca, sna = acs[0 : 2 * M, :], acs[2 * M : 4 * M, :]
    turned = []
    for side in range(2):
        g = doth(wf, y[side * M : (side + 1) * M])
        C, S = g[: 2 * M], g[2 * M :]
        turned.append(jnp.concatenate([C * ca - S * sna, -(C * sna + S * ca)], 1))
    T = dot6(jnp.concatenate(turned, 0), (t1[...], t2[...], t3[...]))
    shape = (2 * M, half)
    zeroth = lanes_of(shape) == 0
    origin = (rows_of(shape) == 0) & zeroth
    root = 1.0 / math.sqrt(M)
    scale = jnp.where(zeroth & (rows_of(shape) > 0), root * math.sqrt(2.0), root)
    T1, T0 = T[: 2 * M] * scale, T[2 * M :] * scale

    own = rows_of((M, L)) == r
    alz = jnp.where(own, T1[:1, :1], 0.0)
    t0z = jnp.where(own, T0[:1, :1], 0.0)
    src = jnp.where(own, al[M - 1 :, :1] * (1.0 / math.sqrt(M)), 0.0)
    Hz = doth(mats[2 * M : 3 * M, : 2 * M], jnp.concatenate([alz, src], 0))
    lift = doth(mats[3 * M : 4 * M, : 3 * M], jnp.concatenate([alz, t0z, Hz], 0))
    g0 = jnp.where(rows_of((M, L)) == M - 1, Hz, doth(s2, Hz))
    up, down = lane_pick(sa, r), lane_pick(stt, r)
    T1c = jnp.where(r == M - 1, T1 * gcouple[...], T1)
    modes = []
    for m in range(M - 1):
        value = (up[m : m + 1] * T1c + down[m : m + 1] * T0) * dens[2 * M * m : 2 * M * (m + 1), :]
        modes.append(jnp.where(origin, g0[m : m + 1, :1] * root, value))
    modes.append(jnp.where(r == M - 1, T1, 0.0) * scale)
    modes = split(jnp.concatenate(modes, 0))
    XC = dot3(modes, (qs[0][:half], qs[1][:half]))
    XS = dot3(modes, (b1[...], b2[...]))
    ws = (w1[...], w2[...], w3[...])
    group = w1.shape[1] // (4 * M)
    lines = []
    for first in range(0, M, group):
        rots = []
        for m in range(first, first + group):
            xc, xs = XC[2 * M * m : 2 * M * (m + 1)], XS[2 * M * m : 2 * M * (m + 1)]
            rots += [ca * xc - sna * xs, sna * xc + ca * xs]
        lines.append(dotl(ws, jnp.concatenate(rots, 0)))
    hx = doths(jnp.concatenate(lines, 0), qs)
    Y0, Y1 = dot3(hx * v0, rs), dot3(hx * v1, rs)

    D = lead / (1.0 + e * e - 2.0 * e * cosphi)
    inner = rows_of((M, n)) < M - 1
    first = lanes_of((1, n)) == 0
    cols = []
    for cc in (c, c - 1):
        KD = lane_pick(s2, cc) * D
        k1 = jnp.where(inner, doth(sa, KD, 0, 0), 0.0)
        k2 = doth(stt, KD, 0, 0)
        ksrc = lane_pick(mats[7 * M : 8 * M, :M], cc) * (-1.0 / qq)
        cols.append((k1, k2, ksrc))
    ka, kt = lane_pick(mats[8 * M : 9 * M, :M], c), lane_pick(mats[9 * M : 10 * M, :M], c)
    kth = lane_pick(mats[10 * M : 11 * M, :M], c)
    here, side_c, side_b, level = [], [], [], []
    for m in range(M):
        rows = slice(M * m, M * (m + 1))
        hm, y0, y1 = hx[rows], Y0[rows], Y1[rows]
        here.append(pick(hm, c))
        for (k1, k2, ksrc), sides in zip(cols, (side_c, side_b)):
            phi = jnp.sum(k1 * y1 + k2 * y0, 0, keepdims=True)
            z = jnp.sum(ksrc * hm, 0, keepdims=True)
            sides.append(jnp.where(first, z, phi))
        level.append(
            jnp.sum(kth * hm[:, :L] - ka * y1[:, :L] - kt * y0[:, :L], 0, keepdims=True)
        )
    s2x = mats[6 * M : 7 * M, :M]
    mixed = [doth(s2x, jnp.concatenate(v, 0)) for v in (here, side_c, side_b, level)]
    right, fc, fb, lv = mixed
    lv = (lv - below(lv) + lift * (1.0 / math.sqrt(M)))[:, :1]
    share = [
        below(right),
        right,
        v0 * below(fc) - v1 * fc,
        v0 * below(fb) - v1 * fb,
        lv,
    ]
    keep = [pick(H, c), pick(H, c - 1), jnp.broadcast_to(pick(mean, c), (1, n))]
    return share, jnp.concatenate(keep + [jnp.zeros((5, n), f32)], 0)


def stage_field(r, c, M, share, keep, u, qh, ql, rr, vec):
    keep, vec = keep[...], vec[...]
    n = vec.shape[1]
    q0, q1 = vec[0:1], vec[1:2]
    left, right, here, before, level = (
        jnp.sum(share[:, a, :n] if a < 4 else share[:, 0, n:], 0, keepdims=True) for a in range(5)
    )
    here = here + keep[0:1]
    before = before + keep[1:2]
    level = level[:, :1] + keep[2:3, :1]
    pad = jnp.zeros((4, n), f32)
    lhs = jnp.concatenate([q1, -q0, here, -before, pad], 0)
    rhs = jnp.concatenate([right, left, q1, q0, pad], 0)
    G = doth(lhs, rhs, 0, 0)
    un = u[...] - rr[...] * G
    un = jnp.where((rows_of(un.shape) == 0) & (lanes_of(un.shape) == 0), level, un)
    qs = (qh[...], ql[...])
    return (dot3(qs, dot3(un, qs), 0, 0),)


def packed(rows):
    tail = jnp.broadcast_to(rows[4][:, :, None], rows[4].shape[:1] + (4, 128))
    return jnp.concatenate([jnp.stack(rows[:4], 1), tail], 2)


def run_stage(stage, members, outs, *args):
    if DIRECT:
        results = stage(lax.axis_index("row"), lax.axis_index("col"), members, *args)
        return [packed(v) if isinstance(v, list) else v for v in results]

    def kernel(*refs):
        r, c = lax.axis_index("row"), lax.axis_index("col")
        n = args[0].shape[-1]
        results = stage(r, c, members, *refs[: len(args)])
        for ref, value in zip(refs[len(args) :], results):
            if isinstance(value, list):
                for a, row in enumerate(value[:4]):
                    ref[:, a, :n] = row
                ref[:, :, n:] = jnp.broadcast_to(value[4][:, :, None], (members, 4, 128))
            else:
                ref[...] = value

    vmem = pl.BlockSpec(memory_space=pltpu.VMEM)
    return pl.pallas_call(
        kernel,
        out_shape=outs,
        in_specs=[vmem] * len(args),
        out_specs=[vmem] * len(outs),
        compiler_params=pltpu.CompilerParams(vmem_limit_bytes=VMEM_LIMIT),
        name=stage.__name__,
    )(*args)


def exchange(values, axis):
    return lax.all_to_all(values, axis, split_axis=0, concat_axis=0, tiled=True)


def make_body(members):
    def body(grad_x, grad_y):
        n = grad_x.shape[0]
        t = {k: jnp.asarray(v) for k, v in build_tables(n, members).items()}
        sent, near = jax.ShapeDtypeStruct, pltpu.VMEM
        edges, u, kept = run_local(members, {**t, "x": grad_x, "y": grad_y}, t["vec"])
        strip = exchange(edges, "col")
        names = LATER[:-2] + ("vec",) + LATER[-2:]
        kept["vec"] = t["vec"]
        share, keep = run_stage(
            stage_strip, members, [sent((members, 4, n + 128), f32), near((8, n), f32)],
            strip, kept["q1"], kept["q2"], *(kept[name] for name in names),
        )
        share = exchange(share, "row")
        (field,) = run_stage(
            stage_field, members, [sent((n, n), f32)],
            share, keep, u, kept["q1"], kept["q2"], kept["r"], t["vec"],
        )
        return field

    return body


def solution(mesh):
    members = mesh.shape["row"]
    placed = (P("row", "col"), P("row", "col"))
    return jax.shard_map(
        make_body(members), mesh=mesh, in_specs=placed, out_specs=P("row", "col"), check_vma=False
    )
```

```python
import math

import jax
import jax.numpy as jnp
import numpy as np
from jax import lax
from jax.experimental import pallas as pl
from jax.experimental.pallas import tpu as pltpu
from jax.sharding import PartitionSpec as P

VMEM_LIMIT = 32 * 1024 * 1024
DIRECT = False
f32 = jnp.float32
bf16 = jnp.bfloat16


def cosine_basis(n):
    k, i = np.arange(n)[:, None], np.arange(n)[None]
    return np.sqrt(np.where(k == 0, 1, 2) / n) * np.cos(np.pi * k * (2 * i + 1) / (2 * n))


def edge_tables(n, members, freq):
    s = 2 * np.sin(freq)
    half = np.arcsinh(s / 2)
    e = np.exp(-2 * n * half)
    safe = np.where(s == 0, 1, s)
    e1 = np.where(s == 0, 0.5, e)
    th = np.tanh(np.arcsinh(safe / 2))
    one = np.where(s == 0, 0, 1)
    lead = one * th * (1 - e1 * e1)
    couple = one * e1 / (th * (1 - e1 * e1))
    return lead, e, couple


def pieces_of(value, count):
    found = []
    for _ in range(count):
        found.append(np.asarray(value, jnp.bfloat16))
        value = value - found[-1].astype(np.float64)
    return found


def stack_pieces(value):
    a1, a2, a3 = pieces_of(value, 3)
    return np.concatenate([a1, a1, a2, a2, a1, a3], 1)


def build_tables(n, members):
    total = n * members
    half = n // 2
    k = np.concatenate([np.arange(0, n, 2), np.arange(1, n, 2)])
    q = cosine_basis(n)[k]
    s = 2 * np.sin(np.pi * k / (2 * n))
    q0, q1 = q[:, 0], q[:, -1]
    lead, e, couple = edge_tables(n, members, np.pi * k / (2 * n))
    vec = np.zeros((8, n))
    vec[0], vec[1], vec[2], vec[3], vec[4] = q0, q1, lead, e, couple
    m = np.arange(half)
    cls = np.arange(2 * members)
    kap = cls[:, None] + 2 * members * m[None]
    glob = np.stack(edge_tables(n, members, np.pi * kap / (2 * total)))
    bend = 1 + glob[1] ** 2 - 2 * glob[1] * np.cos(np.pi * np.arange(1, members) / members)[:, None, None]
    size = np.full((2 * members, half), 1 / np.sqrt(members))
    size[1:, 0] *= np.sqrt(2)
    dens = (glob[0] * size / bend).reshape(-1, half)
    j = 2 * np.arange(n) + 1
    sb = np.sqrt(2 / n) * np.sin(np.pi * m[:, None] * j[None] / n)
    turn = np.concatenate([q[:half].T, sb.T], 0)
    sp = np.sqrt(2 / n) * s[:, None] * np.sin(np.pi * k[:, None] * (np.arange(n)[None] + 1) / n)
    sp[:, n - 1] = 0
    sp[0] = 0
    den = s[:, None] ** 2 + s[None] ** 2
    den[0, 0] = 1
    r = 1 / den
    r[0, 0] = 0
    ang = np.pi * cls[:, None] * j[None] / (2 * total)
    acs = np.concatenate([np.cos(ang), np.sin(ang)], 0)
    p = np.arange(members)
    wang = np.pi * cls[:, None] * p[None] / members
    wc, ws = np.cos(wang), np.sin(wang)
    wfwd = np.concatenate([wc, ws], 0)
    winv = np.concatenate([wc.T, -ws.T], 1)
    M = members
    t = np.arange(1, M)
    st = np.sqrt(2 / M) * np.sin(np.pi * np.outer(t, t) / M)
    sa, stt, s2 = np.zeros((M, M)), np.zeros((M, M)), np.zeros((M, M))
    sa[: M - 1, : M - 1] = st
    sa[: M - 1, M - 1] = st[:, M - 2]
    stt[: M - 1, 1:] = -st
    s2[: M - 1, : M - 1] = st
    a0 = (q1[1:] ** 2 / s[1:] ** 2).sum()
    b0 = (q0[1:] * q1[1:] / s[1:] ** 2).sum()
    qq = 1 / np.sqrt(n)
    pp = np.arange(M)
    frac = (pp[:, None] + 1) / M
    t1 = frac - (pp[None] <= pp[:, None])
    h15 = np.zeros((M, M))
    h15[:, M - 1] = frac[:, 0]
    hmat = np.concatenate([h15, t1], 1)
    acc = (pp[None] < pp[:, None]).astype(float)
    acc[:, M - 1] = 0
    acc = (acc - acc.mean(0)) / qq
    up = np.zeros((M, M))
    up[:-1, 1:] = np.eye(M - 1)
    keep = np.eye(M)
    keep[M - 1, M - 1] = 0
    ka = acc @ keep
    kt = -acc @ (keep @ up)
    kh = acc @ (keep @ (-(1 + 2 * a0) * np.eye(M) + b0 * up + b0 * up.T))
    s2x = s2.copy()
    s2x[M - 1, M - 1] = 1
    per = min(M, n // (2 * M), 256 // (4 * M))
    wbd = np.kron(np.eye(per), winv)
    minv = np.zeros((M, M, n))
    lean = lead / (1 + e * e - 2 * e * np.cos(np.pi * t / M)[:, None])
    minv[: M - 1, : M - 1] = np.einsum("pm,mk,mq->pqk", st, lean, st)
    mats = np.zeros((8 * M, 128))
    mats[0:M, : 2 * M] = np.concatenate([sa, stt], 1)
    mats[M : 2 * M, :M] = t1.T
    mats[2 * M : 3 * M, :M] = ka.T * qq
    mats[3 * M : 4 * M, :M] = kt.T * qq
    mats[4 * M : 5 * M, :M] = (kh @ t1).T
    kmats = np.zeros((8 * M, 384), jnp.bfloat16)
    row = 0
    for small in (hmat, np.concatenate([ka, kt, kh], 1), s2, s2x, wfwd):
        stacked = stack_pieces(small)
        kmats[row : row + small.shape[0], : stacked.shape[1]] = stacked
        row += small.shape[0]
    out = dict(r=r, vec=vec, couple=glob[2], dens=dens, acs=acs, mats=mats, minv=minv)
    out = {name: np.asarray(value, np.float32) for name, value in out.items()}
    out["kmats"] = kmats
    for name, value, count in (
        ("q", q, 3), ("s", sp, 2), ("r", r, 3), ("t", turn, 3), ("b", sb, 2), ("w", wbd, 3)
    ):
        for i, piece in enumerate(pieces_of(value, count)):
            out[f"{name}{i + 1}"] = piece
    return out


def split(a):
    high = a.astype(bf16)
    return high, (a - high.astype(f32)).astype(bf16)


def mm(a, b, ca, cb):
    return lax.dot_general(a, b, (((ca,), (cb,)), ((), ())), preferred_element_type=f32)


def dot3(a, b, ca=1, cb=0):
    ah, al = a if isinstance(a, tuple) else split(a)
    bh, bl = b if isinstance(b, tuple) else split(b)
    return mm(ah, bh, ca, cb) + (mm(ah, bl, ca, cb) + mm(al, bh, ca, cb))


def split3(a):
    high, rest = a.astype(bf16), None
    rest = a - high.astype(f32)
    mid = rest.astype(bf16)
    return high, mid, (rest - mid.astype(f32)).astype(bf16)


def dot6(a, b, cb=0):
    m = a.shape[0]
    a1, a2, a3 = split3(a)
    b1, b2, b3 = b
    p = mm(jnp.concatenate([a1, a2, a3], 0), b1, 1, cb)
    q = mm(jnp.concatenate([a1, a2], 0), b2, 1, cb)
    small = (p[2 * m :] + q[m:]) + mm(a1, b3, 1, cb)
    return p[:m] + ((p[m : 2 * m] + q[:m]) + small)


def dotl(a, b):
    m = a[0].shape[0]
    b1, b2, b3 = split3(b)
    p = mm(jnp.concatenate(a, 0), b1, 1, 0)
    q = mm(jnp.concatenate(a[:2], 0), b2, 1, 0)
    small = (p[2 * m :] + q[m:]) + mm(a[0], b3, 1, 0)
    return p[:m] + ((p[m : 2 * m] + q[:m]) + small)


def doths(a, qs):
    value = dot3(a, qs, 1, 1)
    exact = jnp.sum(a, 1, keepdims=True) * (1.0 / math.sqrt(a.shape[1]))
    return jnp.where(lanes_of(value.shape) == 0, exact, value)


def doth(a, b, ca=1, cb=0):
    return lax.dot_general(
        a, b, (((ca,), (cb,)), ((), ())), precision=lax.Precision.HIGHEST, preferred_element_type=f32
    )


def rows_of(shape):
    return lax.broadcasted_iota(jnp.int32, shape, 0)


def lanes_of(shape):
    return lax.broadcasted_iota(jnp.int32, shape, 1)


def pick(values, index):
    return jnp.sum(jnp.where(rows_of(values.shape) == index, values, 0.0), 0, keepdims=True)


def below(values):
    return jnp.concatenate([jnp.zeros_like(values[:1]), values[:-1]], 0)


def stacked(b):
    b1, b2, b3 = (piece.astype(f32) for piece in split3(b))
    return jnp.concatenate([b1, b2, b1, b2, b3, b1], 0).astype(bf16)


def dotk(a, b):
    return mm(a[:, : 6 * b.shape[0]], stacked(b), 1, 0)


def edge_solve(al, t0, couple, source, minv, kmats, special):
    M, n = al.shape
    L = min(n, 128)
    last = rows_of((M, n)) == M - 1
    w = al - jnp.concatenate([t0[1:], t0[:1]], 0)
    H = jnp.where(last, al, 0.0)
    tail = couple * al[M - 1 :]
    for p in range(M - 1):
        wp = w[p : p + 1] + tail if p == M - 2 else w[p : p + 1]
        H = H + minv[p] * wp
    Hz = dotk(kmats[0:M, :], jnp.concatenate([al[:, :L], source], 0))
    mean = dotk(kmats[M : 2 * M, :], jnp.concatenate([al[:, :L], t0[:, :L], Hz], 0))
    lane = lanes_of((M, L))
    first = jnp.where((lane == 0) & special, Hz, H[:, :L])
    H = first if n == L else jnp.concatenate([first, H[:, L:]], 1)
    return H, jnp.where(special, mean[:, :1], 0.0)


def to_peers(rows, members):
    one = jnp.concatenate(rows, 0)
    return jnp.broadcast_to(one[None], (members,) + one.shape)


def stage_local(r, c, M, need):
    vec = need("vec")
    n = vec.shape[1]
    L = min(n, 128)
    qs = (need("q1"), need("q2"))
    m1 = dot3(need("x"), qs, 1, 1)
    ss = (need("s1"), need("s2"))
    gys = split(need("y"))
    m2 = dot3(gys, ss, 1, 1)
    slab = (gys[0][:, n - L :], gys[1][:, n - L :])
    gyl = dot3(slab, qs, 0, 1)[L - 1 :]
    f = dot3(ss, m1) + dot3(qs, m2)
    u = -f * need("r")
    us = split(u)
    tk = dot3(vec, us, 1, 1)
    tl = dot3(vec, us, 1, 0)
    alpha = gyl + jnp.where(c < M - 1, tk[1:2], 0.0)
    beta = m1[n - 1 :] + jnp.where(r < M - 1, tl[1:2], 0.0)
    return to_peers([alpha, tk[0:1], beta, tl[0:1]], M), u


WAVES = {None: ("vec", "q1", "x", "q2"), "x": ("s1", "s2", "y", "r")}
WAVES["y"] = ("q3", "r1", "r2", "r3", "t1", "t2", "t3", "b1", "b2", "w1", "w2", "w3")
WAVES["y"] += ("dens", "couple", "minv", "acs", "mats", "kmats")
NAMES = WAVES[None] + WAVES["x"] + WAVES["y"]
KEPT = ("vec", "q1", "q2", "r") + WAVES["y"]


def run_local(members, arrays):
    n = arrays["vec"].shape[1]
    if DIRECT:
        edges, u = stage_local(
            lax.axis_index("row"), lax.axis_index("col"), members, arrays.__getitem__
        )
        return edges, u, {name: arrays[name] for name in KEPT}

    def kernel(*refs):
        count = len(NAMES)
        edges, u = refs[count : count + 2]
        here = dict(zip(KEPT, refs[count + 2 :]))
        here.update(zip((k for k in NAMES if k not in KEPT), refs[count + 2 + len(KEPT) :]))
        sem = refs[-1]
        copies = {
            name: pltpu.make_async_copy(source, here[name], sem.at[i])
            for i, (name, source) in enumerate(zip(NAMES, refs))
        }

        def release(wave):
            for name in WAVES.get(wave, ()):
                copies[name].start()

        def need(name):
            copies[name].wait()
            release(name)
            return here[name][...]

        release(None)
        edges[...], u[...] = stage_local(
            lax.axis_index("row"), lax.axis_index("col"), members, need
        )
        for name in WAVES["y"]:
            copies[name].wait()

    far, vmem, near = pl.BlockSpec(memory_space=pltpu.HBM), pl.BlockSpec(memory_space=pltpu.VMEM), pltpu.VMEM
    shape = {name: near(arrays[name].shape, arrays[name].dtype) for name in NAMES}
    edges, u, *tables = pl.pallas_call(
        kernel,
        out_shape=[jax.ShapeDtypeStruct((members, 4, n), f32), near((n, n), f32)]
        + [shape[name] for name in KEPT],
        in_specs=[far] * len(NAMES),
        out_specs=[vmem] * (2 + len(KEPT)),
        scratch_shapes=[shape[name] for name in NAMES if name not in KEPT]
        + [pltpu.SemaphoreType.DMA((len(NAMES),))],
        compiler_params=pltpu.CompilerParams(vmem_limit_bytes=VMEM_LIMIT),
        name="stage_local",
    )(*(pltpu.with_memory_space_constraint(arrays[name], pltpu.HBM) for name in NAMES))
    return edges, u, dict(zip(KEPT, tables))


def lane_pick(values, index):
    return jnp.sum(jnp.where(lanes_of(values.shape) == index, values, 0.0), 1, keepdims=True)


def stage_strip(
    r, c, M, ag, vec, q1, q2, q3, r1, r2, r3, t1, t2, t3, b1, b2, w1, w2, w3,
    dens, gcouple, minv, acs, mats, kmats,
):
    al, t0, be, ta0 = (ag[:, a, :] for a in range(4))
    vec, mats = vec[...], mats[...]
    n = al.shape[1]
    half = n // 2
    v0, v1, couple = vec[0:1], vec[1:2], vec[4:5]
    L = min(n, 128)
    qq = 1.0 / math.sqrt(n)
    zero = jnp.zeros((M, L), f32)
    sa, stt = mats[:M, :M], mats[:M, M : 2 * M]

    H, mean = edge_solve(al, t0, couple, zero, minv, kmats, True)
    rs = (r1[...], r2[...])
    Z = dot6(jnp.concatenate([H * v0, H * v1], 0), rs + (r3[...],))
    add0 = v0 * below(Z[:M]) - v1 * Z[:M]
    add1 = v0 * below(Z[M:]) - v1 * Z[M:]
    flat = jnp.where(lanes_of((M, n)) == 0, mean * qq, 0.0)
    tau0 = ta0 + add0 + flat
    tau1 = be + jnp.where(r < M - 1, add1 + flat, 0.0)

    qs = (q1[...], q2[...])
    y = dot6(jnp.concatenate([tau1, tau0], 0), qs + (q3[...],))
    ca, sna = acs[0 : 2 * M, :], acs[2 * M : 4 * M, :]
    g = dotk(kmats[4 * M : 8 * M, :], jnp.concatenate([y[:M], y[M:]], 1))
    turned = []
    for side in range(2):
        C, S = (g[k * 2 * M : (k + 1) * 2 * M, side * n : (side + 1) * n] for k in range(2))
        turned.append(jnp.concatenate([C * ca - S * sna, -(C * sna + S * ca)], 1))
    T = dot6(jnp.concatenate(turned, 0), (t1[...], t2[...], t3[...]))
    shape = (2 * M, half)
    zeroth = lanes_of(shape) == 0
    origin = (rows_of(shape) == 0) & zeroth
    root = 1.0 / math.sqrt(M)
    scale = jnp.where(zeroth & (rows_of(shape) > 0), root * math.sqrt(2.0), root)
    T1, T0 = T[: 2 * M] * scale, T[2 * M :] * scale

    own = rows_of((M, L)) == r
    alz = jnp.where(own, T1[:1, :1], 0.0)
    t0z = jnp.where(own, T0[:1, :1], 0.0)
    src = jnp.where(own, al[M - 1 :, :1] * (1.0 / math.sqrt(M)), 0.0)
    Hz = dotk(kmats[0:M, :], jnp.concatenate([alz, src], 0))
    lift = dotk(kmats[M : 2 * M, :], jnp.concatenate([alz, t0z, Hz], 0))
    g0 = jnp.where(rows_of((M, L)) == M - 1, Hz, dotk(kmats[2 * M : 3 * M, :], Hz))
    up, down = lane_pick(sa, r), lane_pick(stt, r)
    T1c = jnp.where(r == M - 1, T1 * gcouple[...], T1)
    modes = []
    for m in range(M - 1):
        value = (up[m : m + 1] * T1c + down[m : m + 1] * T0) * dens[2 * M * m : 2 * M * (m + 1), :]
        modes.append(jnp.where(origin, g0[m : m + 1, :1] * root, value))
    modes.append(jnp.where(r == M - 1, T1, 0.0) * scale)
    modes = split(jnp.concatenate(modes, 0))
    XC = dot3(modes, (qs[0][:half], qs[1][:half]))
    XS = dot3(modes, (b1[...], b2[...]))
    ws = (w1[...], w2[...], w3[...])
    group = w1.shape[1] // (4 * M)
    lines = []
    for first in range(0, M, group):
        rots = []
        for m in range(first, first + group):
            xc, xs = XC[2 * M * m : 2 * M * (m + 1)], XS[2 * M * m : 2 * M * (m + 1)]
            rots += [ca * xc - sna * xs, sna * xc + ca * xs]
        lines.append(dotl(ws, jnp.concatenate(rots, 0)))
    hx = doths(jnp.concatenate(lines, 0), qs)
    Y0, Y1 = dot3(hx * v0, rs), dot3(hx * v1, rs)

    first = lanes_of((1, n)) == 0
    cols = []
    for k1, cc in ((minv[c], c), (minv[jnp.maximum(c - 1, 0)], c - 1)):
        k1 = jnp.where(cc < 0, 0.0, k1)
        cols.append((k1, -below(k1), lane_pick(mats[M : 2 * M, :M], cc) * (-1.0 / qq)))
    ka, kt = lane_pick(mats[2 * M : 3 * M, :M], c), lane_pick(mats[3 * M : 4 * M, :M], c)
    kth = lane_pick(mats[4 * M : 5 * M, :M], c)
    here, side_c, side_b, level = [], [], [], []
    for m in range(M):
        rows = slice(M * m, M * (m + 1))
        hm, y0, y1 = hx[rows], Y0[rows], Y1[rows]
        here.append(pick(hm, c))
        for (k1, k2, ksrc), sides in zip(cols, (side_c, side_b)):
            phi = jnp.sum(k1 * y1 + k2 * y0, 0, keepdims=True)
            z = jnp.sum(ksrc * hm, 0, keepdims=True)
            sides.append(jnp.where(first, z, phi))
        level.append(
            jnp.sum(kth * hm[:, :L] - ka * y1[:, :L] - kt * y0[:, :L], 0, keepdims=True)
        )
    rows = [jnp.concatenate(v, 0) for v in (here, side_c, side_b, level)]
    mixed = dotk(kmats[3 * M : 4 * M, :], jnp.concatenate(rows, 1))
    mixed = [mixed[:, a * n : (a + 1) * n] for a in range(4)]
    right, fc, fb, lv = mixed
    lv = (lv - below(lv) + lift * (1.0 / math.sqrt(M)))[:, :1]
    share = [
        below(right),
        right,
        v0 * below(fc) - v1 * fc,
        v0 * below(fb) - v1 * fb,
        lv,
    ]
    keep = [pick(H, c), pick(H, c - 1), jnp.broadcast_to(pick(mean, c), (1, n))]
    return share, jnp.concatenate(keep + [jnp.zeros((5, n), f32)], 0)


def stage_field(r, c, M, share, keep, u, qh, ql, rr, vec):
    keep, vec = keep[...], vec[...]
    n = vec.shape[1]
    q0, q1 = vec[0:1], vec[1:2]
    left, right, here, before, level = (
        jnp.sum(share[:, a, :n] if a < 4 else share[:, 0, n:], 0, keepdims=True) for a in range(5)
    )
    here = here + keep[0:1]
    before = before + keep[1:2]
    level = level[:, :1] + keep[2:3, :1]
    pad = jnp.zeros((4, n), f32)
    a1, a2, a3 = (
        piece.astype(f32) for piece in split3(jnp.concatenate([q1, -q0, here, -before, pad], 0))
    )
    lhs = jnp.concatenate([a1, a1, a2, a2, a1, a3], 0).astype(bf16)
    G = mm(lhs, stacked(jnp.concatenate([right, left, q1, q0, pad], 0)), 0, 0)
    un = u[...] - rr[...] * G
    un = jnp.where((rows_of(un.shape) == 0) & (lanes_of(un.shape) == 0), level, un)
    qs = (qh[...], ql[...])
    half = split(dot3(un, qs))
    step = n // 4
    for part in range(4):
        cols = slice(part * step, (part + 1) * step)
        yield dot3((qs[0][:, cols], qs[1][:, cols]), half, 0, 0)


def run_field(members, *args):
    n = args[-1].shape[1]
    place = lambda: (lax.axis_index("row"), lax.axis_index("col"))
    if DIRECT:
        return jnp.concatenate(list(stage_field(*place(), members, *args)), 0)

    def kernel(*refs):
        field, rows, sem = refs[len(args) :]
        copies = []
        for part, value in enumerate(stage_field(*place(), members, *refs[: len(args)])):
            step = value.shape[0]
            span = slice(part * step, (part + 1) * step)
            rows[span, :] = value
            copies.append(pltpu.make_async_copy(rows.at[span], field.at[span], sem.at[part]))
            copies[-1].start()
        for copy in copies:
            copy.wait()

    vmem = pl.BlockSpec(memory_space=pltpu.VMEM)
    return pl.pallas_call(
        kernel,
        out_shape=jax.ShapeDtypeStruct((n, n), f32),
        in_specs=[vmem] * len(args),
        out_specs=pl.BlockSpec(memory_space=pltpu.HBM),
        scratch_shapes=[pltpu.VMEM((n, n), f32), pltpu.SemaphoreType.DMA((4,))],
        compiler_params=pltpu.CompilerParams(vmem_limit_bytes=VMEM_LIMIT),
        name="stage_field",
    )(*args)


def packed(rows):
    tail = jnp.broadcast_to(rows[4][:, :, None], rows[4].shape[:1] + (4, 128))
    return jnp.concatenate([jnp.stack(rows[:4], 1), tail], 2)


def run_stage(stage, members, outs, *args):
    if DIRECT:
        results = stage(lax.axis_index("row"), lax.axis_index("col"), members, *args)
        return [packed(v) if isinstance(v, list) else v for v in results]

    def kernel(*refs):
        r, c = lax.axis_index("row"), lax.axis_index("col")
        n = args[0].shape[-1]
        results = stage(r, c, members, *refs[: len(args)])
        for ref, value in zip(refs[len(args) :], results):
            if isinstance(value, list):
                for a, row in enumerate(value[:4]):
                    ref[:, a, :n] = row
                ref[:, :, n:] = jnp.broadcast_to(value[4][:, :, None], (members, 4, 128))
            else:
                ref[...] = value

    vmem = pl.BlockSpec(memory_space=pltpu.VMEM)
    return pl.pallas_call(
        kernel,
        out_shape=outs,
        in_specs=[vmem] * len(args),
        out_specs=[vmem] * len(outs),
        compiler_params=pltpu.CompilerParams(vmem_limit_bytes=VMEM_LIMIT),
        name=stage.__name__,
    )(*args)


def exchange(values, axis):
    return lax.all_to_all(values, axis, split_axis=0, concat_axis=0, tiled=True)


def make_body(members):
    def body(grad_x, grad_y):
        n = grad_x.shape[0]
        t = {k: jnp.asarray(v) for k, v in build_tables(n, members).items()}
        sent, near = jax.ShapeDtypeStruct, pltpu.VMEM
        edges, u, kept = run_local(members, {**t, "x": grad_x, "y": grad_y})
        strip = exchange(edges, "col")
        share, keep = run_stage(
            stage_strip, members, [sent((members, 4, n + 128), f32), near((8, n), f32)],
            strip, kept["vec"], kept["q1"], kept["q2"], *(kept[name] for name in WAVES["y"]),
        )
        share = exchange(share, "row")
        return run_field(
            members, share, keep, u, kept["q1"], kept["q2"], kept["r"], kept["vec"]
        )

    return body


def solution(mesh):
    members = mesh.shape["row"]
    placed = (P("row", "col"), P("row", "col"))
    return jax.shard_map(
        make_body(members), mesh=mesh, in_specs=placed, out_specs=P("row", "col"), check_vma=False
    )
```

```python
import math

import jax
import jax.numpy as jnp
import numpy as np
from jax import lax
from jax.experimental import pallas as pl
from jax.experimental.pallas import tpu as pltpu
from jax.sharding import PartitionSpec as P

VMEM_LIMIT = 32 * 1024 * 1024
DIRECT = False
f32 = jnp.float32
bf16 = jnp.bfloat16


def cosine_basis(n):
    k, i = np.arange(n)[:, None], np.arange(n)[None]
    return np.sqrt(np.where(k == 0, 1, 2) / n) * np.cos(np.pi * k * (2 * i + 1) / (2 * n))


def edge_tables(n, members, freq):
    s = 2 * np.sin(freq)
    half = np.arcsinh(s / 2)
    e = np.exp(-2 * n * half)
    safe = np.where(s == 0, 1, s)
    e1 = np.where(s == 0, 0.5, e)
    th = np.tanh(np.arcsinh(safe / 2))
    one = np.where(s == 0, 0, 1)
    lead = one * th * (1 - e1 * e1)
    couple = one * e1 / (th * (1 - e1 * e1))
    return lead, e, couple


def pieces_of(value, count):
    found = []
    for _ in range(count):
        found.append(np.asarray(value, jnp.bfloat16))
        value = value - found[-1].astype(np.float64)
    return found


def stack_pieces(value):
    a1, a2, a3 = pieces_of(value, 3)
    return np.concatenate([a1, a1, a2, a2, a1, a3], 1)


def build_tables(n, members):
    total = n * members
    half = n // 2
    k = np.concatenate([np.arange(0, n, 2), np.arange(1, n, 2)])
    q = cosine_basis(n)[k]
    s = 2 * np.sin(np.pi * k / (2 * n))
    q0, q1 = q[:, 0], q[:, -1]
    lead, e, couple = edge_tables(n, members, np.pi * k / (2 * n))
    vec = np.zeros((8, n))
    vec[0], vec[1], vec[2], vec[3], vec[4] = q0, q1, lead, e, couple
    m = np.arange(half)
    cls = np.arange(2 * members)
    kap = cls[:, None] + 2 * members * m[None]
    glob = np.stack(edge_tables(n, members, np.pi * kap / (2 * total)))
    bend = 1 + glob[1] ** 2 - 2 * glob[1] * np.cos(np.pi * np.arange(1, members) / members)[:, None, None]
    size = np.full((2 * members, half), 1 / np.sqrt(members))
    size[1:, 0] *= np.sqrt(2)
    dens = (glob[0] * size / bend).reshape(-1, half)
    j = 2 * np.arange(n) + 1
    sb = np.sqrt(2 / n) * np.sin(np.pi * m[:, None] * j[None] / n)
    turn = np.concatenate([q[:half].T, sb.T], 0)
    sp = np.sqrt(2 / n) * s[:, None] * np.sin(np.pi * k[:, None] * (np.arange(n)[None] + 1) / n)
    sp[:, n - 1] = 0
    sp[0] = 0
    den = s[:, None] ** 2 + s[None] ** 2
    den[0, 0] = 1
    r = 1 / den
    r[0, 0] = 0
    ang = np.pi * cls[:, None] * j[None] / (2 * total)
    acs = np.concatenate([np.cos(ang), np.sin(ang)], 0)
    p = np.arange(members)
    wang = np.pi * cls[:, None] * p[None] / members
    wc, ws = np.cos(wang), np.sin(wang)
    wfwd = np.concatenate([wc, ws], 0)
    winv = np.concatenate([wc.T, -ws.T], 1)
    M = members
    t = np.arange(1, M)
    st = np.sqrt(2 / M) * np.sin(np.pi * np.outer(t, t) / M)
    sa, stt, s2 = np.zeros((M, M)), np.zeros((M, M)), np.zeros((M, M))
    sa[: M - 1, : M - 1] = st
    sa[: M - 1, M - 1] = st[:, M - 2]
    stt[: M - 1, 1:] = -st
    s2[: M - 1, : M - 1] = st
    a0 = (q1[1:] ** 2 / s[1:] ** 2).sum()
    b0 = (q0[1:] * q1[1:] / s[1:] ** 2).sum()
    qq = 1 / np.sqrt(n)
    pp = np.arange(M)
    frac = (pp[:, None] + 1) / M
    t1 = frac - (pp[None] <= pp[:, None])
    h15 = np.zeros((M, M))
    h15[:, M - 1] = frac[:, 0]
    hmat = np.concatenate([h15, t1], 1)
    acc = (pp[None] < pp[:, None]).astype(float)
    acc[:, M - 1] = 0
    acc = (acc - acc.mean(0)) / qq
    up = np.zeros((M, M))
    up[:-1, 1:] = np.eye(M - 1)
    keep = np.eye(M)
    keep[M - 1, M - 1] = 0
    ka = acc @ keep
    kt = -acc @ (keep @ up)
    kh = acc @ (keep @ (-(1 + 2 * a0) * np.eye(M) + b0 * up + b0 * up.T))
    s2x = s2.copy()
    s2x[M - 1, M - 1] = 1
    per = min(M, n // (2 * M), 256 // (4 * M))
    wbd = np.kron(np.eye(per), winv)
    minv = np.zeros((M, M, n))
    lean = lead / (1 + e * e - 2 * e * np.cos(np.pi * t / M)[:, None])
    minv[: M - 1, : M - 1] = np.einsum("pm,mk,mq->pqk", st, lean, st)
    mats = np.zeros((8 * M, 128))
    mats[0:M, : 2 * M] = np.concatenate([sa, stt], 1)
    mats[M : 2 * M, :M] = t1.T
    mats[2 * M : 3 * M, :M] = ka.T * qq
    mats[3 * M : 4 * M, :M] = kt.T * qq
    mats[4 * M : 5 * M, :M] = (kh @ t1).T
    kmats = np.zeros((8 * M, 384), jnp.bfloat16)
    row = 0
    for small in (hmat, np.concatenate([ka, kt, kh], 1), s2, s2x, wfwd):
        stacked = stack_pieces(small)
        kmats[row : row + small.shape[0], : stacked.shape[1]] = stacked
        row += small.shape[0]
    q1, q2, q3 = pieces_of(q, 3)
    s1, s2 = pieces_of(sp, 2)
    v1, v2 = pieces_of(vec, 2)
    out = dict(
        vec=vec, r=r, col=np.repeat(q0[:, None], min(n, 128), 1), mats=mats,
        thin=np.concatenate([dens, glob[2]], 0),
        long=np.concatenate([minv.reshape(-1, n), acs], 0),
    )
    out = {name: np.asarray(value, np.float32) for name, value in out.items()}
    out.update(
        q1=q1, q2=q2, s1=s1, s2=s2, v=np.concatenate([v1, v2], 0), kmats=kmats,
        w=np.concatenate(pieces_of(wbd, 3), 0), turn=np.concatenate(pieces_of(turn, 3), 0),
        wide=np.concatenate([q3] + pieces_of(r, 3) + pieces_of(sb, 2), 0),
    )
    return out


def split(a):
    high = a.astype(bf16)
    return high, (a - high.astype(f32)).astype(bf16)


def mm(a, b, ca, cb):
    return lax.dot_general(a, b, (((ca,), (cb,)), ((), ())), preferred_element_type=f32)


def dot3(a, b, ca=1, cb=0):
    ah, al = a if isinstance(a, tuple) else split(a)
    bh, bl = b if isinstance(b, tuple) else split(b)
    return mm(ah, bh, ca, cb) + (mm(ah, bl, ca, cb) + mm(al, bh, ca, cb))


def split3(a):
    high, rest = a.astype(bf16), None
    rest = a - high.astype(f32)
    mid = rest.astype(bf16)
    return high, mid, (rest - mid.astype(f32)).astype(bf16)


def dot6(a, b, cb=0):
    m = a.shape[0]
    a1, a2, a3 = split3(a)
    b1, b2, b3 = b
    p = mm(jnp.concatenate([a1, a2, a3], 0), b1, 1, cb)
    q = mm(jnp.concatenate([a1, a2], 0), b2, 1, cb)
    small = (p[2 * m :] + q[m:]) + mm(a1, b3, 1, cb)
    return p[:m] + ((p[m : 2 * m] + q[:m]) + small)


def dotl(a, b):
    m = a[0].shape[0]
    b1, b2, b3 = split3(b)
    p = mm(jnp.concatenate(a, 0), b1, 1, 0)
    q = mm(jnp.concatenate(a[:2], 0), b2, 1, 0)
    small = (p[2 * m :] + q[m:]) + mm(a[0], b3, 1, 0)
    return p[:m] + ((p[m : 2 * m] + q[:m]) + small)


def doths(a, qs):
    value = dot3(a, qs, 1, 1)
    exact = jnp.sum(a, 1, keepdims=True) * (1.0 / math.sqrt(a.shape[1]))
    return jnp.where(lanes_of(value.shape) == 0, exact, value)


def doth(a, b, ca=1, cb=0):
    return lax.dot_general(
        a, b, (((ca,), (cb,)), ((), ())), precision=lax.Precision.HIGHEST, preferred_element_type=f32
    )


def rows_of(shape):
    return lax.broadcasted_iota(jnp.int32, shape, 0)


def lanes_of(shape):
    return lax.broadcasted_iota(jnp.int32, shape, 1)


def pick(values, index):
    return jnp.sum(jnp.where(rows_of(values.shape) == index, values, 0.0), 0, keepdims=True)


def below(values):
    return jnp.concatenate([jnp.zeros_like(values[:1]), values[:-1]], 0)


def stacked(b):
    b1, b2, b3 = (piece.astype(f32) for piece in split3(b))
    return jnp.concatenate([b1, b2, b1, b2, b3, b1], 0).astype(bf16)


def dotk(a, b):
    return mm(a[:, : 6 * b.shape[0]], stacked(b), 1, 0)


def edge_solve(al, t0, couple, source, minv, kmats, special):
    M, n = al.shape
    L = min(n, 128)
    last = rows_of((M, n)) == M - 1
    w = al - jnp.concatenate([t0[1:], t0[:1]], 0)
    H = jnp.where(last, al, 0.0)
    tail = couple * al[M - 1 :]
    for p in range(M - 1):
        wp = w[p : p + 1] + tail if p == M - 2 else w[p : p + 1]
        H = H + minv[M * p : M * (p + 1), :] * wp
    Hz = dotk(kmats[0:M, :], jnp.concatenate([al[:, :L], source], 0))
    mean = dotk(kmats[M : 2 * M, :], jnp.concatenate([al[:, :L], t0[:, :L], Hz], 0))
    lane = lanes_of((M, L))
    first = jnp.where((lane == 0) & special, Hz, H[:, :L])
    H = first if n == L else jnp.concatenate([first, H[:, L:]], 1)
    return H, jnp.where(special, mean[:, :1], 0.0)


def to_peers(rows, members):
    one = jnp.concatenate(rows, 0)
    return jnp.broadcast_to(one[None], (members,) + one.shape)


def stage_local(r, c, M, need):
    q1 = need("q1")
    n = q1.shape[0]
    half = n // 2
    L = min(n, 128)
    pieces, sums = [], []
    for name in ("x0", "x1"):
        pieces.append(split(need(name)))
        sums.append(mm(pieces[-1][0], q1, 1, 1))
    q2 = need("q2")
    m1 = jnp.concatenate(
        [p + (mm(xh, q2, 1, 1) + mm(xl, q1, 1, 1)) for p, (xh, xl) in zip(sums, pieces)], 0
    )
    qs = (q1, q2)
    n2 = dot3(qs, need("y"))
    ss = (need("s1"), need("s2"))
    f = dot3(ss, m1) + dot3(n2, ss, 1, 1)
    gyl = n2[:, n - L :].T[L - 1 :]
    u = -f * need("r")
    uh, ul = split(u)
    v = need("v")
    p = mm(v, uh, 1, 1)
    tk = p[:8] + (p[8:] + mm(v, ul, 1, 1)[:8])
    col = need("col")
    groups = []
    for rows in (slice(0, half), slice(half, n)):
        groups.append(
            jnp.concatenate(
                [
                    jnp.sum(u[rows, a : a + L] * col[rows], 0, keepdims=True)
                    for a in range(0, n, L)
                ],
                1,
            )
        )
    low, high = groups[0] + groups[1], groups[0] - groups[1]
    alpha = gyl + jnp.where(c < M - 1, tk[1:2], 0.0)
    beta = m1[n - 1 :] + jnp.where(r < M - 1, high, 0.0)
    return to_peers([alpha, tk[0:1], beta, low], M), u


WAVES = {None: ("q1", "x0", "x1", "q2"), "x0": ("y", "s1", "s2"), "y": ("r", "v", "col")}
WAVES["s2"] = ("vec", "wide", "turn", "w", "thin", "long", "mats", "kmats")
NAMES = WAVES[None] + WAVES["x0"] + WAVES["y"] + WAVES["s2"]
KEPT = ("q1", "q2", "r") + WAVES["s2"]


def run_local(members, arrays):
    n = arrays["q1"].shape[1]
    arrays["x0"], arrays["x1"] = arrays["x"][: n // 2], arrays["x"][n // 2 :]
    shapes = {name: (arrays[name].shape, arrays[name].dtype) for name in NAMES}
    if DIRECT:
        edges, u = stage_local(
            lax.axis_index("row"), lax.axis_index("col"), members, arrays.__getitem__
        )
        return edges, u, {name: arrays[name] for name in KEPT}

    def kernel(*refs):
        count = len(NAMES)
        edges, u = refs[count : count + 2]
        here = dict(zip(KEPT, refs[count + 2 :]))
        here.update(zip((k for k in NAMES if k not in KEPT), refs[count + 2 + len(KEPT) :]))
        sem = refs[-1]
        def part_of(name, source):
            pick_half = {"x0": pl.ds(0, n // 2), "x1": pl.ds(n // 2, n // 2)}
            return source.at[pick_half[name]] if name in pick_half else source

        copies = {
            name: pltpu.make_async_copy(part_of(name, source), here[name], sem.at[i])
            for i, (name, source) in enumerate(zip(NAMES, refs))
        }

        def release(wave):
            for name in WAVES.get(wave, ()):
                copies[name].start()

        def need(name):
            copies[name].wait()
            release(name)
            return here[name][...]

        release(None)
        edges[...], u[...] = stage_local(
            lax.axis_index("row"), lax.axis_index("col"), members, need
        )
        for name in WAVES["s2"]:
            copies[name].wait()

    operands = [name if name not in ("x0", "x1") else "x" for name in NAMES]
    far, vmem, near = pl.BlockSpec(memory_space=pltpu.HBM), pl.BlockSpec(memory_space=pltpu.VMEM), pltpu.VMEM
    shape = {name: near(*shapes[name]) for name in NAMES}
    edges, u, *tables = pl.pallas_call(
        kernel,
        out_shape=[jax.ShapeDtypeStruct((members, 4, n), f32), near((n, n), f32)]
        + [shape[name] for name in KEPT],
        in_specs=[far] * len(NAMES),
        out_specs=[vmem] * (2 + len(KEPT)),
        scratch_shapes=[shape[name] for name in NAMES if name not in KEPT]
        + [pltpu.SemaphoreType.DMA((len(NAMES),))],
        compiler_params=pltpu.CompilerParams(vmem_limit_bytes=VMEM_LIMIT),
        name="stage_local",
    )(*(pltpu.with_memory_space_constraint(arrays[name], pltpu.HBM) for name in operands))
    return edges, u, dict(zip(KEPT, tables))


def lane_pick(values, index):
    return jnp.sum(jnp.where(lanes_of(values.shape) == index, values, 0.0), 1, keepdims=True)


def stage_strip(r, c, M, ag, q1, q2, vec, wide, turn, w, thin, long, mats, kmats):
    n = q1.shape[0]
    half = n // 2
    r1, r2, r3 = (wide[a * n : (a + 1) * n, :] for a in range(1, 4))
    b1, b2 = wide[4 * n : 4 * n + half, :], wide[4 * n + half : 5 * n, :]
    acs = long[M * M : M * M + 4 * M, :]
    al, t0, be, ta0 = (ag[:, a, :] for a in range(4))
    vec, mats = vec[...], mats[...]
    v0, v1, couple = vec[0:1], vec[1:2], vec[4:5]
    L = min(n, 128)
    qq = 1.0 / math.sqrt(n)
    zero = jnp.zeros((M, L), f32)
    sa, stt = mats[:M, :M], mats[:M, M : 2 * M]

    H, mean = edge_solve(al, t0, couple, zero, long, kmats, True)
    rs = (r1, r2)
    Z = dot6(jnp.concatenate([H * v0, H * v1], 0), rs + (r3,))
    add0 = v0 * below(Z[:M]) - v1 * Z[:M]
    add1 = v0 * below(Z[M:]) - v1 * Z[M:]
    flat = jnp.where(lanes_of((M, n)) == 0, mean * qq, 0.0)
    tau0 = ta0 + add0 + flat
    tau1 = be + jnp.where(r < M - 1, add1 + flat, 0.0)

    qs = (q1[...], q2[...])
    y = dot6(jnp.concatenate([tau1, tau0], 0), qs + (wide[:n, :],))
    ca, sna = acs[0 : 2 * M, :], acs[2 * M : 4 * M, :]
    g = dotk(kmats[4 * M : 8 * M, :], jnp.concatenate([y[:M], y[M:]], 1))
    turned = []
    for side in range(2):
        C, S = (g[k * 2 * M : (k + 1) * 2 * M, side * n : (side + 1) * n] for k in range(2))
        turned.append(jnp.concatenate([C * ca - S * sna, -(C * sna + S * ca)], 1))
    T = dot6(jnp.concatenate(turned, 0), tuple(turn[2 * n * a : 2 * n * (a + 1), :] for a in range(3)))
    shape = (2 * M, half)
    zeroth = lanes_of(shape) == 0
    origin = (rows_of(shape) == 0) & zeroth
    root = 1.0 / math.sqrt(M)
    scale = jnp.where(zeroth & (rows_of(shape) > 0), root * math.sqrt(2.0), root)
    T1, T0 = T[: 2 * M] * scale, T[2 * M :] * scale

    own = rows_of((M, L)) == r
    alz = jnp.where(own, T1[:1, :1], 0.0)
    t0z = jnp.where(own, T0[:1, :1], 0.0)
    src = jnp.where(own, al[M - 1 :, :1] * (1.0 / math.sqrt(M)), 0.0)
    Hz = dotk(kmats[0:M, :], jnp.concatenate([alz, src], 0))
    lift = dotk(kmats[M : 2 * M, :], jnp.concatenate([alz, t0z, Hz], 0))
    g0 = jnp.where(rows_of((M, L)) == M - 1, Hz, dotk(kmats[2 * M : 3 * M, :], Hz))
    up, down = lane_pick(sa, r), lane_pick(stt, r)
    T1c = jnp.where(r == M - 1, T1 * thin[2 * M * (M - 1) :, :], T1)
    modes = []
    for m in range(M - 1):
        value = (up[m : m + 1] * T1c + down[m : m + 1] * T0) * thin[2 * M * m : 2 * M * (m + 1), :]
        modes.append(jnp.where(origin, g0[m : m + 1, :1] * root, value))
    modes.append(jnp.where(r == M - 1, T1, 0.0) * scale)
    modes = split(jnp.concatenate(modes, 0))
    XC = dot3(modes, (qs[0][:half], qs[1][:half]))
    XS = dot3(modes, (b1, b2))
    third = w.shape[0] // 3
    ws = tuple(w[third * a : third * (a + 1), :] for a in range(3))
    group = w.shape[1] // (4 * M)
    lines = []
    for first in range(0, M, group):
        rots = []
        for m in range(first, first + group):
            xc, xs = XC[2 * M * m : 2 * M * (m + 1)], XS[2 * M * m : 2 * M * (m + 1)]
            rots += [ca * xc - sna * xs, sna * xc + ca * xs]
        lines.append(dotl(ws, jnp.concatenate(rots, 0)))
    hx = doths(jnp.concatenate(lines, 0), qs)
    Y0, Y1 = dot3(hx * v0, rs), dot3(hx * v1, rs)

    first = lanes_of((1, n)) == 0
    cols = []
    for cc in (c, c - 1):
        k1 = long[pl.ds(pl.multiple_of(jnp.maximum(cc, 0) * M, M), M), :]
        k1 = jnp.where(cc < 0, 0.0, k1)
        cols.append((k1, -below(k1), lane_pick(mats[M : 2 * M, :M], cc) * (-1.0 / qq)))
    ka, kt = lane_pick(mats[2 * M : 3 * M, :M], c), lane_pick(mats[3 * M : 4 * M, :M], c)
    kth = lane_pick(mats[4 * M : 5 * M, :M], c)
    here, side_c, side_b, level = [], [], [], []
    for m in range(M):
        rows = slice(M * m, M * (m + 1))
        hm, y0, y1 = hx[rows], Y0[rows], Y1[rows]
        here.append(pick(hm, c))
        for (k1, k2, ksrc), sides in zip(cols, (side_c, side_b)):
            phi = jnp.sum(k1 * y1 + k2 * y0, 0, keepdims=True)
            z = jnp.sum(ksrc * hm, 0, keepdims=True)
            sides.append(jnp.where(first, z, phi))
        level.append(
            jnp.sum(kth * hm[:, :L] - ka * y1[:, :L] - kt * y0[:, :L], 0, keepdims=True)
        )
    rows = [jnp.concatenate(v, 0) for v in (here, side_c, side_b, level)]
    mixed = dotk(kmats[3 * M : 4 * M, :], jnp.concatenate(rows, 1))
    mixed = [mixed[:, a * n : (a + 1) * n] for a in range(4)]
    right, fc, fb, lv = mixed
    lv = (lv - below(lv) + lift * (1.0 / math.sqrt(M)))[:, :1]
    share = [
        below(right),
        right,
        v0 * below(fc) - v1 * fc,
        v0 * below(fb) - v1 * fb,
        lv,
    ]
    keep = [pick(H, c), pick(H, c - 1), jnp.broadcast_to(pick(mean, c), (1, n))]
    return share, jnp.concatenate(keep + [jnp.zeros((5, n), f32)], 0)


def stage_field(r, c, M, share, keep, u, qh, ql, rr, vec):
    keep, vec = keep[...], vec[...]
    n = vec.shape[1]
    q0, q1 = vec[0:1], vec[1:2]
    left, right, here, before, level = (
        jnp.sum(share[:, a, :n] if a < 4 else share[:, 0, n:], 0, keepdims=True) for a in range(5)
    )
    here = here + keep[0:1]
    before = before + keep[1:2]
    level = level[:, :1] + keep[2:3, :1]
    pad = jnp.zeros((4, n), f32)
    a1, a2, a3 = (
        piece.astype(f32) for piece in split3(jnp.concatenate([q1, -q0, here, -before, pad], 0))
    )
    lhs = jnp.concatenate([a1, a1, a2, a2, a1, a3], 0).astype(bf16)
    G = mm(lhs, stacked(jnp.concatenate([right, left, q1, q0, pad], 0)), 0, 0)
    un = u[...] - rr[...] * G
    un = jnp.where((rows_of(un.shape) == 0) & (lanes_of(un.shape) == 0), level, un)
    qs = (qh[...], ql[...])
    half = split(dot3(un, qs))
    step = n // 4
    for part in range(4):
        cols = slice(part * step, (part + 1) * step)
        yield dot3((qs[0][:, cols], qs[1][:, cols]), half, 0, 0)


def run_field(members, *args):
    n = args[-1].shape[1]
    place = lambda: (lax.axis_index("row"), lax.axis_index("col"))
    if DIRECT:
        return jnp.concatenate(list(stage_field(*place(), members, *args)), 0)

    def kernel(*refs):
        field, rows, sem = refs[len(args) :]
        copies = []
        for part, value in enumerate(stage_field(*place(), members, *refs[: len(args)])):
            step = value.shape[0]
            span = slice(part * step, (part + 1) * step)
            rows[span, :] = value
            copies.append(pltpu.make_async_copy(rows.at[span], field.at[span], sem.at[part]))
            copies[-1].start()
        for copy in copies:
            copy.wait()

    vmem = pl.BlockSpec(memory_space=pltpu.VMEM)
    return pl.pallas_call(
        kernel,
        out_shape=jax.ShapeDtypeStruct((n, n), f32),
        in_specs=[vmem] * len(args),
        out_specs=pl.BlockSpec(memory_space=pltpu.HBM),
        scratch_shapes=[pltpu.VMEM((n, n), f32), pltpu.SemaphoreType.DMA((4,))],
        compiler_params=pltpu.CompilerParams(vmem_limit_bytes=VMEM_LIMIT),
        name="stage_field",
    )(*args)


def packed(rows):
    tail = jnp.broadcast_to(rows[4][:, :, None], rows[4].shape[:1] + (4, 128))
    return jnp.concatenate([jnp.stack(rows[:4], 1), tail], 2)


def run_stage(stage, members, outs, *args):
    if DIRECT:
        results = stage(lax.axis_index("row"), lax.axis_index("col"), members, *args)
        return [packed(v) if isinstance(v, list) else v for v in results]

    def kernel(*refs):
        r, c = lax.axis_index("row"), lax.axis_index("col")
        n = args[0].shape[-1]
        results = stage(r, c, members, *refs[: len(args)])
        for ref, value in zip(refs[len(args) :], results):
            if isinstance(value, list):
                for a, row in enumerate(value[:4]):
                    ref[:, a, :n] = row
                ref[:, :, n:] = jnp.broadcast_to(value[4][:, :, None], (members, 4, 128))
            else:
                ref[...] = value

    vmem = pl.BlockSpec(memory_space=pltpu.VMEM)
    return pl.pallas_call(
        kernel,
        out_shape=outs,
        in_specs=[vmem] * len(args),
        out_specs=[vmem] * len(outs),
        compiler_params=pltpu.CompilerParams(vmem_limit_bytes=VMEM_LIMIT),
        name=stage.__name__,
    )(*args)


def exchange(values, axis):
    return lax.all_to_all(values, axis, split_axis=0, concat_axis=0, tiled=True)


def make_body(members):
    def body(grad_x, grad_y):
        n = grad_x.shape[0]
        t = {k: jnp.asarray(v) for k, v in build_tables(n, members).items()}
        sent, near = jax.ShapeDtypeStruct, pltpu.VMEM
        edges, u, kept = run_local(members, {**t, "x": grad_x, "y": grad_y})
        strip = exchange(edges, "col")
        share, keep = run_stage(
            stage_strip, members, [sent((members, 4, n + 128), f32), near((8, n), f32)],
            strip, kept["q1"], kept["q2"], *(kept[name] for name in WAVES["s2"]),
        )
        share = exchange(share, "row")
        return run_field(
            members, share, keep, u, kept["q1"], kept["q2"], kept["r"], kept["vec"]
        )

    return body


def solution(mesh):
    members = mesh.shape["row"]
    placed = (P("row", "col"), P("row", "col"))
    return jax.shard_map(
        make_body(members), mesh=mesh, in_specs=placed, out_specs=P("row", "col"), check_vma=False
    )
```

```python
import math

import jax
import jax.numpy as jnp
import numpy as np
from jax import lax
from jax.experimental import pallas as pl
from jax.experimental.pallas import tpu as pltpu
from jax.sharding import PartitionSpec as P

VMEM_LIMIT = 32 * 1024 * 1024
DIRECT = False
f32 = jnp.float32
bf16 = jnp.bfloat16


def cosine_basis(n):
    k, i = np.arange(n)[:, None], np.arange(n)[None]
    return np.sqrt(np.where(k == 0, 1, 2) / n) * np.cos(np.pi * k * (2 * i + 1) / (2 * n))


def edge_tables(n, members, freq):
    s = 2 * np.sin(freq)
    half = np.arcsinh(s / 2)
    e = np.exp(-2 * n * half)
    safe = np.where(s == 0, 1, s)
    e1 = np.where(s == 0, 0.5, e)
    th = np.tanh(np.arcsinh(safe / 2))
    one = np.where(s == 0, 0, 1)
    lead = one * th * (1 - e1 * e1)
    couple = one * e1 / (th * (1 - e1 * e1))
    return lead, e, couple


def pieces_of(value, count):
    found = []
    for _ in range(count):
        found.append(np.asarray(value, jnp.bfloat16))
        value = value - found[-1].astype(np.float64)
    return found


def stack_pieces(value):
    a1, a2, a3 = pieces_of(value, 3)
    return np.concatenate([a1, a1, a2, a2, a1, a3], 1)


def build_tables(n, members):
    total = n * members
    half = n // 2
    k = np.concatenate([np.arange(0, n, 2), np.arange(1, n, 2)])
    q = cosine_basis(n)[k]
    s = 2 * np.sin(np.pi * k / (2 * n))
    q0, q1 = q[:, 0], q[:, -1]
    lead, e, couple = edge_tables(n, members, np.pi * k / (2 * n))
    vec = np.zeros((8, n))
    vec[0], vec[1], vec[2], vec[3], vec[4] = q0, q1, lead, e, couple
    m = np.arange(half)
    cls = np.arange(2 * members)
    kap = cls[:, None] + 2 * members * m[None]
    glob = np.stack(edge_tables(n, members, np.pi * kap / (2 * total)))
    bend = 1 + glob[1] ** 2 - 2 * glob[1] * np.cos(np.pi * np.arange(1, members) / members)[:, None, None]
    size = np.full((2 * members, half), 1 / np.sqrt(members))
    size[1:, 0] *= np.sqrt(2)
    dens = (glob[0] * size / bend).reshape(-1, half)
    j = 2 * np.arange(n) + 1
    sb = np.sqrt(2 / n) * np.sin(np.pi * m[:, None] * j[None] / n)
    turn = np.concatenate([q[:half].T, sb.T], 0)
    sp = np.sqrt(2 / n) * s[:, None] * np.sin(np.pi * k[:, None] * (np.arange(n)[None] + 1) / n)
    sp[:, n - 1] = 0
    sp[0] = 0
    den = s[:, None] ** 2 + s[None] ** 2
    den[0, 0] = 1
    r = 1 / den
    r[0, 0] = 0
    ang = np.pi * cls[:, None] * j[None] / (2 * total)
    acs = np.concatenate([np.cos(ang), np.sin(ang)], 0)
    p = np.arange(members)
    wang = np.pi * cls[:, None] * p[None] / members
    wc, ws = np.cos(wang), np.sin(wang)
    wfwd = np.concatenate([wc, ws], 0)
    winv = np.concatenate([wc.T, -ws.T], 1)
    M = members
    t = np.arange(1, M)
    st = np.sqrt(2 / M) * np.sin(np.pi * np.outer(t, t) / M)
    sa, stt, s2 = np.zeros((M, M)), np.zeros((M, M)), np.zeros((M, M))
    sa[: M - 1, : M - 1] = st
    sa[: M - 1, M - 1] = st[:, M - 2]
    stt[: M - 1, 1:] = -st
    s2[: M - 1, : M - 1] = st
    a0 = (q1[1:] ** 2 / s[1:] ** 2).sum()
    b0 = (q0[1:] * q1[1:] / s[1:] ** 2).sum()
    qq = 1 / np.sqrt(n)
    pp = np.arange(M)
    frac = (pp[:, None] + 1) / M
    t1 = frac - (pp[None] <= pp[:, None])
    h15 = np.zeros((M, M))
    h15[:, M - 1] = frac[:, 0]
    hmat = np.concatenate([h15, t1], 1)
    acc = (pp[None] < pp[:, None]).astype(float)
    acc[:, M - 1] = 0
    acc = (acc - acc.mean(0)) / qq
    up = np.zeros((M, M))
    up[:-1, 1:] = np.eye(M - 1)
    keep = np.eye(M)
    keep[M - 1, M - 1] = 0
    ka = acc @ keep
    kt = -acc @ (keep @ up)
    kh = acc @ (keep @ (-(1 + 2 * a0) * np.eye(M) + b0 * up + b0 * up.T))
    s2x = s2.copy()
    s2x[M - 1, M - 1] = 1
    per = min(M, n // (2 * M), 256 // (4 * M))
    wbd = np.kron(np.eye(per), winv)
    minv = np.zeros((M, M, n))
    lean = lead / (1 + e * e - 2 * e * np.cos(np.pi * t / M)[:, None])
    minv[: M - 1, : M - 1] = np.einsum("pm,mk,mq->pqk", st, lean, st)
    mats = np.zeros((8 * M, 128))
    mats[0:M, : 2 * M] = np.concatenate([sa, stt], 1)
    mats[M : 2 * M, :M] = t1.T
    mats[2 * M : 3 * M, :M] = ka.T * qq
    mats[3 * M : 4 * M, :M] = kt.T * qq
    mats[4 * M : 5 * M, :M] = (kh @ t1).T
    kmats = np.zeros((8 * M, 384), jnp.bfloat16)
    row = 0
    for small in (hmat, np.concatenate([ka, kt, kh], 1), s2, s2x, wfwd):
        stacked = stack_pieces(small)
        kmats[row : row + small.shape[0], : stacked.shape[1]] = stacked
        row += small.shape[0]
    q1, q2, q3 = pieces_of(q, 3)
    s1, s2 = pieces_of(sp, 2)
    v1, v2 = pieces_of(vec, 2)
    out = dict(
        vec=vec, r=r, col=np.repeat(q0[:, None], min(n, 128), 1), mats=mats,
        thin=np.concatenate([dens, glob[2]], 0),
        long=np.concatenate([minv.reshape(-1, n), acs], 0),
    )
    out = {name: np.asarray(value, np.float32) for name, value in out.items()}
    out.update(
        q1=q1, q2=q2, s1=s1, s2=s2, v=np.concatenate([v1, v2], 0), kmats=kmats,
        w=np.concatenate(pieces_of(wbd, 3), 0), turn=np.concatenate(pieces_of(turn, 3), 0),
        wide=np.concatenate([q3] + pieces_of(r, 3) + pieces_of(sb, 2), 0),
    )
    return out


def split(a):
    high = a.astype(bf16)
    return high, (a - high.astype(f32)).astype(bf16)


def mm(a, b, ca, cb):
    return lax.dot_general(a, b, (((ca,), (cb,)), ((), ())), preferred_element_type=f32)


def dot3s(a, b, ca=1, cb=0):
    ah, al = a if isinstance(a, tuple) else split(a)
    bh, bl = b if isinstance(b, tuple) else split(b)
    return mm(ah, bh, ca, cb) + (mm(ah, bl, ca, cb) + mm(al, bh, ca, cb))


def dot3(a, b, ca=1, cb=0):
    ah, al = a if isinstance(a, tuple) else split(a)
    bh, bl = b if isinstance(b, tuple) else split(b)
    return mm(jnp.concatenate([ah, ah, al], ca), jnp.concatenate([bh, bl, bh], cb), ca, cb)


def split3(a):
    high, rest = a.astype(bf16), None
    rest = a - high.astype(f32)
    mid = rest.astype(bf16)
    return high, mid, (rest - mid.astype(f32)).astype(bf16)


def dot6(a, b, cb=0):
    m = a.shape[0]
    a1, a2, a3 = split3(a)
    b1, b2, b3 = b
    p = mm(jnp.concatenate([a1, a2, a3], 0), b1, 1, cb)
    q = mm(jnp.concatenate([a1, a2], 0), b2, 1, cb)
    small = (p[2 * m :] + q[m:]) + mm(a1, b3, 1, cb)
    return p[:m] + ((p[m : 2 * m] + q[:m]) + small)


def dotl(a, b):
    m = a[0].shape[0]
    b1, b2, b3 = split3(b)
    p = mm(jnp.concatenate(a, 0), b1, 1, 0)
    q = mm(jnp.concatenate(a[:2], 0), b2, 1, 0)
    small = (p[2 * m :] + q[m:]) + mm(a[0], b3, 1, 0)
    return p[:m] + ((p[m : 2 * m] + q[:m]) + small)


def doths(a, qs):
    value = dot3(a, qs, 1, 1)
    exact = jnp.sum(a, 1, keepdims=True) * (1.0 / math.sqrt(a.shape[1]))
    return jnp.where(lanes_of(value.shape) == 0, exact, value)


def doth(a, b, ca=1, cb=0):
    return lax.dot_general(
        a, b, (((ca,), (cb,)), ((), ())), precision=lax.Precision.HIGHEST, preferred_element_type=f32
    )


def rows_of(shape):
    return lax.broadcasted_iota(jnp.int32, shape, 0)


def lanes_of(shape):
    return lax.broadcasted_iota(jnp.int32, shape, 1)


def pick(values, index):
    return jnp.sum(jnp.where(rows_of(values.shape) == index, values, 0.0), 0, keepdims=True)


def below(values):
    return jnp.concatenate([jnp.zeros_like(values[:1]), values[:-1]], 0)


def stacked(b):
    b1, b2, b3 = (piece.astype(f32) for piece in split3(b))
    return jnp.concatenate([b1, b2, b1, b2, b3, b1], 0).astype(bf16)


def dotk(a, b):
    return mm(a[:, : 6 * b.shape[0]], stacked(b), 1, 0)


def edge_solve(al, t0, couple, source, minv, kmats, special):
    M, n = al.shape
    L = min(n, 128)
    last = rows_of((M, n)) == M - 1
    w = al - jnp.concatenate([t0[1:], t0[:1]], 0)
    H = jnp.where(last, al, 0.0)
    tail = couple * al[M - 1 :]
    for p in range(M - 1):
        wp = w[p : p + 1] + tail if p == M - 2 else w[p : p + 1]
        H = H + minv[M * p : M * (p + 1), :] * wp
    Hz = dotk(kmats[0:M, :], jnp.concatenate([al[:, :L], source], 0))
    mean = dotk(kmats[M : 2 * M, :], jnp.concatenate([al[:, :L], t0[:, :L], Hz], 0))
    lane = lanes_of((M, L))
    first = jnp.where((lane == 0) & special, Hz, H[:, :L])
    H = first if n == L else jnp.concatenate([first, H[:, L:]], 1)
    return H, jnp.where(special, mean[:, :1], 0.0)


def to_peers(rows, members):
    one = jnp.concatenate(rows, 0)
    return jnp.broadcast_to(one[None], (members,) + one.shape)


def stage_local(r, c, M, wait, get):
    wait("q1", "x0", "x1", "q2")
    m1 = dot3(
        jnp.concatenate([get("x0"), get("x1")], 0), (get("q1"), get("q2")), 1, 1
    )
    wait("y", "s1", "s2", "r", "v", "col")
    n = m1.shape[0]
    half = n // 2
    L = min(n, 128)
    n2 = dot3((get("q1"), get("q2")), get("y"))
    ss = (get("s1"), get("s2"))
    f = dot3(ss, m1) + dot3(n2, ss, 1, 1)
    gyl = n2[:, n - L :].T[L - 1 :]
    u = -f * get("r")
    uh, ul = split(u)
    v = get("v")
    p = mm(v, uh, 1, 1)
    tk = p[:8] + (p[8:] + mm(v, ul, 1, 1)[:8])
    col = get("col")
    groups = []
    for rows in (slice(0, half), slice(half, n)):
        groups.append(
            jnp.concatenate(
                [
                    jnp.sum(u[rows, a : a + L] * col[rows], 0, keepdims=True)
                    for a in range(0, n, L)
                ],
                1,
            )
        )
    low, high = groups[0] + groups[1], groups[0] - groups[1]
    alpha = gyl + jnp.where(c < M - 1, tk[1:2], 0.0)
    beta = m1[n - 1 :] + jnp.where(r < M - 1, high, 0.0)
    return to_peers([alpha, tk[0:1], beta, low], M), u


WAVES = {None: ("q1", "x0", "x1", "q2"), "x0": ("y", "s1", "s2", "r", "v", "col")}
WAVES["s2"] = ("vec", "wide", "turn", "w", "thin", "long", "mats", "kmats")
NAMES = WAVES[None] + WAVES["x0"] + WAVES["s2"]
KEPT = ("q1", "q2", "r") + WAVES["s2"]


def run_local(members, arrays):
    n = arrays["q1"].shape[1]
    arrays["x0"], arrays["x1"] = arrays["x"][: n // 2], arrays["x"][n // 2 :]
    shapes = {name: (arrays[name].shape, arrays[name].dtype) for name in NAMES}
    if DIRECT:
        edges, u = stage_local(
            lax.axis_index("row"), lax.axis_index("col"), members, lambda *names: None,
            arrays.__getitem__,
        )
        return edges, u, {name: arrays[name] for name in KEPT}

    def kernel(*refs):
        count = len(NAMES)
        edges, u = refs[count : count + 2]
        here = dict(zip(KEPT, refs[count + 2 :]))
        here.update(zip((k for k in NAMES if k not in KEPT), refs[count + 2 + len(KEPT) :]))
        sem = refs[-1]
        def part_of(name, source):
            pick_half = {"x0": pl.ds(0, n // 2), "x1": pl.ds(n // 2, n // 2)}
            return source.at[pick_half[name]] if name in pick_half else source

        copies = {
            name: pltpu.make_async_copy(part_of(name, source), here[name], sem.at[i])
            for i, (name, source) in enumerate(zip(NAMES, refs))
        }

        def release(wave):
            for name in WAVES.get(wave, ()):
                copies[name].start()

        def wait(*names):
            for name in names:
                copies[name].wait()
                release(name)

        def get(name):
            return here[name][...]

        release(None)
        edges[...], u[...] = stage_local(
            lax.axis_index("row"), lax.axis_index("col"), members, wait, get
        )
        wait(*WAVES["s2"])

    operands = [name if name not in ("x0", "x1") else "x" for name in NAMES]
    far, vmem, near = pl.BlockSpec(memory_space=pltpu.HBM), pl.BlockSpec(memory_space=pltpu.VMEM), pltpu.VMEM
    shape = {name: near(*shapes[name]) for name in NAMES}
    edges, u, *tables = pl.pallas_call(
        kernel,
        out_shape=[jax.ShapeDtypeStruct((members, 4, n), f32), near((n, n), f32)]
        + [shape[name] for name in KEPT],
        in_specs=[far] * len(NAMES),
        out_specs=[vmem] * (2 + len(KEPT)),
        scratch_shapes=[shape[name] for name in NAMES if name not in KEPT]
        + [pltpu.SemaphoreType.DMA((len(NAMES),))],
        compiler_params=pltpu.CompilerParams(vmem_limit_bytes=VMEM_LIMIT),
        name="stage_local",
    )(*(pltpu.with_memory_space_constraint(arrays[name], pltpu.HBM) for name in operands))
    return edges, u, dict(zip(KEPT, tables))


def lane_pick(values, index):
    return jnp.sum(jnp.where(lanes_of(values.shape) == index, values, 0.0), 1, keepdims=True)


def stage_strip(r, c, M, ag, q1, q2, vec, wide, turn, w, thin, long, mats, kmats):
    n = q1.shape[0]
    half = n // 2
    r1, r2, r3 = (wide[a * n : (a + 1) * n, :] for a in range(1, 4))
    b1, b2 = wide[4 * n : 4 * n + half, :], wide[4 * n + half : 5 * n, :]
    acs = long[M * M : M * M + 4 * M, :]
    al, t0, be, ta0 = (ag[:, a, :] for a in range(4))
    vec, mats = vec[...], mats[...]
    v0, v1, couple = vec[0:1], vec[1:2], vec[4:5]
    L = min(n, 128)
    qq = 1.0 / math.sqrt(n)
    zero = jnp.zeros((M, L), f32)
    sa, stt = mats[:M, :M], mats[:M, M : 2 * M]

    H, mean = edge_solve(al, t0, couple, zero, long, kmats, True)
    rs = (r1, r2)
    Z = dot6(jnp.concatenate([H * v0, H * v1], 0), rs + (r3,))
    add0 = v0 * below(Z[:M]) - v1 * Z[:M]
    add1 = v0 * below(Z[M:]) - v1 * Z[M:]
    flat = jnp.where(lanes_of((M, n)) == 0, mean * qq, 0.0)
    tau0 = ta0 + add0 + flat
    tau1 = be + jnp.where(r < M - 1, add1 + flat, 0.0)

    qs = (q1[...], q2[...])
    y = dot6(jnp.concatenate([tau1, tau0], 0), qs + (wide[:n, :],))
    ca, sna = acs[0 : 2 * M, :], acs[2 * M : 4 * M, :]
    g = dotk(kmats[4 * M : 8 * M, :], jnp.concatenate([y[:M], y[M:]], 1))
    turned = []
    for side in range(2):
        C, S = (g[k * 2 * M : (k + 1) * 2 * M, side * n : (side + 1) * n] for k in range(2))
        turned.append(jnp.concatenate([C * ca - S * sna, -(C * sna + S * ca)], 1))
    T = dot6(jnp.concatenate(turned, 0), tuple(turn[2 * n * a : 2 * n * (a + 1), :] for a in range(3)))
    shape = (2 * M, half)
    zeroth = lanes_of(shape) == 0
    origin = (rows_of(shape) == 0) & zeroth
    root = 1.0 / math.sqrt(M)
    scale = jnp.where(zeroth & (rows_of(shape) > 0), root * math.sqrt(2.0), root)
    T1, T0 = T[: 2 * M] * scale, T[2 * M :] * scale

    own = rows_of((M, L)) == r
    alz = jnp.where(own, T1[:1, :1], 0.0)
    t0z = jnp.where(own, T0[:1, :1], 0.0)
    src = jnp.where(own, al[M - 1 :, :1] * (1.0 / math.sqrt(M)), 0.0)
    Hz = dotk(kmats[0:M, :], jnp.concatenate([alz, src], 0))
    lift = dotk(kmats[M : 2 * M, :], jnp.concatenate([alz, t0z, Hz], 0))
    g0 = jnp.where(rows_of((M, L)) == M - 1, Hz, dotk(kmats[2 * M : 3 * M, :], Hz))
    up, down = lane_pick(sa, r), lane_pick(stt, r)
    T1c = jnp.where(r == M - 1, T1 * thin[2 * M * (M - 1) :, :], T1)
    modes = []
    for m in range(M - 1):
        value = (up[m : m + 1] * T1c + down[m : m + 1] * T0) * thin[2 * M * m : 2 * M * (m + 1), :]
        modes.append(jnp.where(origin, g0[m : m + 1, :1] * root, value))
    modes.append(jnp.where(r == M - 1, T1, 0.0) * scale)
    modes = split(jnp.concatenate(modes, 0))
    XC = dot3s(modes, (qs[0][:half], qs[1][:half]))
    XS = dot3s(modes, (b1, b2))
    third = w.shape[0] // 3
    ws = tuple(w[third * a : third * (a + 1), :] for a in range(3))
    group = w.shape[1] // (4 * M)
    lines = []
    for first in range(0, M, group):
        rots = []
        for m in range(first, first + group):
            xc, xs = XC[2 * M * m : 2 * M * (m + 1)], XS[2 * M * m : 2 * M * (m + 1)]
            rots += [ca * xc - sna * xs, sna * xc + ca * xs]
        lines.append(dotl(ws, jnp.concatenate(rots, 0)))
    hx = doths(jnp.concatenate(lines, 0), qs)
    Y = dot3(jnp.concatenate([hx * v0, hx * v1], 0), rs)
    Y0, Y1 = Y[: M * M], Y[M * M :]

    first = lanes_of((1, n)) == 0
    cols = []
    for cc in (c, c - 1):
        k1 = long[pl.ds(pl.multiple_of(jnp.maximum(cc, 0) * M, M), M), :]
        k1 = jnp.where(cc < 0, 0.0, k1)
        cols.append((k1, -below(k1), lane_pick(mats[M : 2 * M, :M], cc) * (-1.0 / qq)))
    ka, kt = lane_pick(mats[2 * M : 3 * M, :M], c), lane_pick(mats[3 * M : 4 * M, :M], c)
    kth = lane_pick(mats[4 * M : 5 * M, :M], c)
    here, side_c, side_b, level = [], [], [], []
    for m in range(M):
        rows = slice(M * m, M * (m + 1))
        hm, y0, y1 = hx[rows], Y0[rows], Y1[rows]
        here.append(pick(hm, c))
        for (k1, k2, ksrc), sides in zip(cols, (side_c, side_b)):
            phi = jnp.sum(k1 * y1 + k2 * y0, 0, keepdims=True)
            z = jnp.sum(ksrc * hm, 0, keepdims=True)
            sides.append(jnp.where(first, z, phi))
        level.append(
            jnp.sum(kth * hm[:, :L] - ka * y1[:, :L] - kt * y0[:, :L], 0, keepdims=True)
        )
    rows = [jnp.concatenate(v, 0) for v in (here, side_c, side_b, level)]
    mixed = dotk(kmats[3 * M : 4 * M, :], jnp.concatenate(rows, 1))
    mixed = [mixed[:, a * n : (a + 1) * n] for a in range(4)]
    right, fc, fb, lv = mixed
    lv = (lv - below(lv) + lift * (1.0 / math.sqrt(M)))[:, :1]
    share = [
        below(right),
        right,
        v0 * below(fc) - v1 * fc,
        v0 * below(fb) - v1 * fb,
        lv,
    ]
    keep = [pick(H, c), pick(H, c - 1), jnp.broadcast_to(pick(mean, c), (1, n))]
    return share, jnp.concatenate(keep + [jnp.zeros((5, n), f32)], 0)


def stage_field(r, c, M, share, keep, u, qh, ql, rr, vec):
    keep, vec = keep[...], vec[...]
    n = vec.shape[1]
    q0, q1 = vec[0:1], vec[1:2]
    left, right, here, before, level = (
        jnp.sum(share[:, a, :n] if a < 4 else share[:, 0, n:], 0, keepdims=True) for a in range(5)
    )
    here = here + keep[0:1]
    before = before + keep[1:2]
    level = level[:, :1] + keep[2:3, :1]
    pad = jnp.zeros((4, n), f32)
    a1, a2, a3 = (
        piece.astype(f32) for piece in split3(jnp.concatenate([q1, -q0, here, -before, pad], 0))
    )
    lhs = jnp.concatenate([a1, a1, a2, a2, a1, a3], 0).astype(bf16)
    G = mm(lhs, stacked(jnp.concatenate([right, left, q1, q0, pad], 0)), 0, 0)
    un = u[...] - rr[...] * G
    un = jnp.where((rows_of(un.shape) == 0) & (lanes_of(un.shape) == 0), level, un)
    qs = (qh[...], ql[...])
    half = split(dot3(un, qs))
    step = n // 4
    for part in range(4):
        cols = slice(part * step, (part + 1) * step)
        yield dot3((qs[0][:, cols], qs[1][:, cols]), half, 0, 0)


def run_field(members, *args):
    n = args[-1].shape[1]
    place = lambda: (lax.axis_index("row"), lax.axis_index("col"))
    if DIRECT:
        return jnp.concatenate(list(stage_field(*place(), members, *args)), 0)

    def kernel(*refs):
        field, rows, sem = refs[len(args) :]
        copies = []
        for part, value in enumerate(stage_field(*place(), members, *refs[: len(args)])):
            step = value.shape[0]
            span = slice(part * step, (part + 1) * step)
            rows[span, :] = value
            copies.append(pltpu.make_async_copy(rows.at[span], field.at[span], sem.at[part]))
            copies[-1].start()
        for copy in copies:
            copy.wait()

    vmem = pl.BlockSpec(memory_space=pltpu.VMEM)
    return pl.pallas_call(
        kernel,
        out_shape=jax.ShapeDtypeStruct((n, n), f32),
        in_specs=[vmem] * len(args),
        out_specs=pl.BlockSpec(memory_space=pltpu.HBM),
        scratch_shapes=[pltpu.VMEM((n, n), f32), pltpu.SemaphoreType.DMA((4,))],
        compiler_params=pltpu.CompilerParams(vmem_limit_bytes=VMEM_LIMIT),
        name="stage_field",
    )(*args)


def packed(rows):
    tail = jnp.broadcast_to(rows[4][:, :, None], rows[4].shape[:1] + (4, 128))
    return jnp.concatenate([jnp.stack(rows[:4], 1), tail], 2)


def run_stage(stage, members, outs, *args):
    if DIRECT:
        results = stage(lax.axis_index("row"), lax.axis_index("col"), members, *args)
        return [packed(v) if isinstance(v, list) else v for v in results]

    def kernel(*refs):
        r, c = lax.axis_index("row"), lax.axis_index("col")
        n = args[0].shape[-1]
        results = stage(r, c, members, *refs[: len(args)])
        for ref, value in zip(refs[len(args) :], results):
            if isinstance(value, list):
                for a, row in enumerate(value[:4]):
                    ref[:, a, :n] = row
                ref[:, :, n:] = jnp.broadcast_to(value[4][:, :, None], (members, 4, 128))
            else:
                ref[...] = value

    vmem = pl.BlockSpec(memory_space=pltpu.VMEM)
    return pl.pallas_call(
        kernel,
        out_shape=outs,
        in_specs=[vmem] * len(args),
        out_specs=[vmem] * len(outs),
        compiler_params=pltpu.CompilerParams(vmem_limit_bytes=VMEM_LIMIT),
        name=stage.__name__,
    )(*args)


def exchange(values, axis):
    return lax.all_to_all(values, axis, split_axis=0, concat_axis=0, tiled=True)


def make_body(members):
    def body(grad_x, grad_y):
        n = grad_x.shape[0]
        t = {k: jnp.asarray(v) for k, v in build_tables(n, members).items()}
        sent, near = jax.ShapeDtypeStruct, pltpu.VMEM
        edges, u, kept = run_local(members, {**t, "x": grad_x, "y": grad_y})
        strip = exchange(edges, "col")
        share, keep = run_stage(
            stage_strip, members, [sent((members, 4, n + 128), f32), near((8, n), f32)],
            strip, kept["q1"], kept["q2"], *(kept[name] for name in WAVES["s2"]),
        )
        share = exchange(share, "row")
        return run_field(
            members, share, keep, u, kept["q1"], kept["q2"], kept["r"], kept["vec"]
        )

    return body


def solution(mesh):
    members = mesh.shape["row"]
    placed = (P("row", "col"), P("row", "col"))
    return jax.shard_map(
        make_body(members), mesh=mesh, in_specs=placed, out_specs=P("row", "col"), check_vma=False
    )
```

```python
import math

import jax
import jax.numpy as jnp
import numpy as np
from jax import lax
from jax.experimental import pallas as pl
from jax.experimental.pallas import tpu as pltpu
from jax.sharding import PartitionSpec as P

VMEM_LIMIT = 32 * 1024 * 1024
DIRECT = False
f32 = jnp.float32
bf16 = jnp.bfloat16


def cosine_basis(n):
    k, i = np.arange(n)[:, None], np.arange(n)[None]
    return np.sqrt(np.where(k == 0, 1, 2) / n) * np.cos(np.pi * k * (2 * i + 1) / (2 * n))


def edge_tables(n, members, freq):
    s = 2 * np.sin(freq)
    half = np.arcsinh(s / 2)
    e = np.exp(-2 * n * half)
    safe = np.where(s == 0, 1, s)
    e1 = np.where(s == 0, 0.5, e)
    th = np.tanh(np.arcsinh(safe / 2))
    one = np.where(s == 0, 0, 1)
    lead = one * th * (1 - e1 * e1)
    couple = one * e1 / (th * (1 - e1 * e1))
    return lead, e, couple


def pieces_of(value, count):
    found = []
    for _ in range(count):
        found.append(np.asarray(value, jnp.bfloat16))
        value = value - found[-1].astype(np.float64)
    return found


def stack_pieces(value):
    a1, a2, a3 = pieces_of(value, 3)
    return np.concatenate([a1, a1, a2, a2, a1, a3], 1)


def build_tables(n, members):
    total = n * members
    half = n // 2
    k = np.concatenate([np.arange(0, n, 2), np.arange(1, n, 2)])
    q = cosine_basis(n)[k]
    s = 2 * np.sin(np.pi * k / (2 * n))
    q0, q1 = q[:, 0], q[:, -1]
    lead, e, couple = edge_tables(n, members, np.pi * k / (2 * n))
    vec = np.zeros((8, n))
    vec[0], vec[1], vec[2], vec[3], vec[4] = q0, q1, lead, e, couple
    lane = np.arange(half)
    other = np.where(lane == 0, half, lane)
    d = np.arange(members)
    kap = np.concatenate(
        [
            d[:, None] + 2 * members * lane[None],
            2 * members * other[None] - np.where(d == 0, members, d)[:, None],
        ]
    )
    glob = np.stack(edge_tables(n, members, np.pi * kap / (2 * total)))
    bend = 1 + glob[1] ** 2 - 2 * glob[1] * np.cos(np.pi * np.arange(1, members) / members)[:, None, None]
    size = np.full((2 * members, half), 1 / np.sqrt(members))
    size[1:members, 0] *= np.sqrt(2)
    dens = (glob[0] * size / bend).reshape(-1, half)
    j = 2 * np.arange(n) + 1
    sb = np.sqrt(2 / n) * np.sin(np.pi * other[:, None] * j[None] / n)
    turn = np.concatenate([q[:half].T, sb.T], 0)
    sp = np.sqrt(2 / n) * s[:, None] * np.sin(np.pi * k[:, None] * (np.arange(n)[None] + 1) / n)
    sp[:, n - 1] = 0
    sp[0] = 0
    den = s[:, None] ** 2 + s[None] ** 2
    den[0, 0] = 1
    r = 1 / den
    r[0, 0] = 0
    ang = np.pi * np.arange(members + 1)[:, None] * j[None] / (2 * total)
    ca, sa = np.cos(ang), np.sin(ang)
    swap = np.concatenate([sa[members:], ca[1:members]], 0)
    acs = np.concatenate([ca[:members], sa[:members], swap, np.repeat(ca[members:], members, 0)], 0)
    p = np.arange(members)
    wang = np.pi * np.arange(members + 1)[:, None] * p[None] / members
    wc, ws = np.cos(wang), np.sin(wang)
    wfwd = np.concatenate([wc[:members], wc[members:], ws[1:members]], 0)
    winv = np.concatenate([wc[:members], wc[members:], -ws[1:members]], 0).T
    M = members
    t = np.arange(1, M)
    st = np.sqrt(2 / M) * np.sin(np.pi * np.outer(t, t) / M)
    sa, stt, s2 = np.zeros((M, M)), np.zeros((M, M)), np.zeros((M, M))
    sa[: M - 1, : M - 1] = st
    sa[: M - 1, M - 1] = st[:, M - 2]
    stt[: M - 1, 1:] = -st
    s2[: M - 1, : M - 1] = st
    a0 = (q1[1:] ** 2 / s[1:] ** 2).sum()
    b0 = (q0[1:] * q1[1:] / s[1:] ** 2).sum()
    qq = 1 / np.sqrt(n)
    pp = np.arange(M)
    frac = (pp[:, None] + 1) / M
    t1 = frac - (pp[None] <= pp[:, None])
    h15 = np.zeros((M, M))
    h15[:, M - 1] = frac[:, 0]
    hmat = np.concatenate([h15, t1], 1)
    acc = (pp[None] < pp[:, None]).astype(float)
    acc[:, M - 1] = 0
    acc = (acc - acc.mean(0)) / qq
    up = np.zeros((M, M))
    up[:-1, 1:] = np.eye(M - 1)
    keep = np.eye(M)
    keep[M - 1, M - 1] = 0
    ka = acc @ keep
    kt = -acc @ (keep @ up)
    kh = acc @ (keep @ (-(1 + 2 * a0) * np.eye(M) + b0 * up + b0 * up.T))
    s2x = s2.copy()
    s2x[M - 1, M - 1] = 1
    per = min(M, 256 // (2 * M))
    wbd = np.kron(np.eye(per), winv)
    minv = np.zeros((M, M, n))
    lean = lead / (1 + e * e - 2 * e * np.cos(np.pi * t / M)[:, None])
    minv[: M - 1, : M - 1] = np.einsum("pm,mk,mq->pqk", st, lean, st)
    mats = np.zeros((8 * M, 128))
    mats[0:M, : 2 * M] = np.concatenate([sa, stt], 1)
    mats[M : 2 * M, :M] = t1.T
    mats[2 * M : 3 * M, :M] = ka.T * qq
    mats[3 * M : 4 * M, :M] = kt.T * qq
    mats[4 * M : 5 * M, :M] = (kh @ t1).T
    kmats = np.zeros((8 * M, 384), jnp.bfloat16)
    row = 0
    for small in (hmat, np.concatenate([ka, kt, kh], 1), s2, s2x, wfwd):
        stacked = stack_pieces(small)
        kmats[row : row + small.shape[0], : stacked.shape[1]] = stacked
        row += small.shape[0]
    q1, q2, q3 = pieces_of(q, 3)
    s1, s2 = pieces_of(sp, 2)
    v1, v2 = pieces_of(vec, 2)
    out = dict(
        vec=vec, r=r, col=np.repeat(q0[:, None], min(n, 128), 1), mats=mats,
        thin=np.concatenate([dens, glob[2]], 0),
        long=np.concatenate([minv.reshape(-1, n), acs], 0),
    )
    out = {name: np.asarray(value, np.float32) for name, value in out.items()}
    out.update(
        q1=q1, q2=q2, s1=s1, s2=s2, v=np.concatenate([v1, v2], 0), kmats=kmats,
        w=np.concatenate(pieces_of(wbd, 3), 0), turn=np.concatenate(pieces_of(turn, 3), 0),
        wide=np.concatenate([q3] + pieces_of(r, 3) + pieces_of(sb, 2), 0),
    )
    return out


def split(a):
    high = a.astype(bf16)
    return high, (a - high.astype(f32)).astype(bf16)


def mm(a, b, ca, cb):
    return lax.dot_general(a, b, (((ca,), (cb,)), ((), ())), preferred_element_type=f32)


def dot3s(a, b, ca=1, cb=0):
    ah, al = a if isinstance(a, tuple) else split(a)
    bh, bl = b if isinstance(b, tuple) else split(b)
    return mm(ah, bh, ca, cb) + (mm(ah, bl, ca, cb) + mm(al, bh, ca, cb))


def dot3(a, b, ca=1, cb=0):
    ah, al = a if isinstance(a, tuple) else split(a)
    bh, bl = b if isinstance(b, tuple) else split(b)
    return mm(jnp.concatenate([ah, ah, al], ca), jnp.concatenate([bh, bl, bh], cb), ca, cb)


def split3(a):
    high, rest = a.astype(bf16), None
    rest = a - high.astype(f32)
    mid = rest.astype(bf16)
    return high, mid, (rest - mid.astype(f32)).astype(bf16)


def dot6(a, b, cb=0):
    m = a.shape[0]
    a1, a2, a3 = split3(a)
    b1, b2, b3 = b
    p = mm(jnp.concatenate([a1, a2, a3], 0), b1, 1, cb)
    q = mm(jnp.concatenate([a1, a2], 0), b2, 1, cb)
    small = (p[2 * m :] + q[m:]) + mm(a1, b3, 1, cb)
    return p[:m] + ((p[m : 2 * m] + q[:m]) + small)


def dotl(a, b):
    m = a[0].shape[0]
    b1, b2, b3 = split3(b)
    p = mm(jnp.concatenate(a, 0), b1, 1, 0)
    q = mm(jnp.concatenate(a[:2], 0), b2, 1, 0)
    small = (p[2 * m :] + q[m:]) + mm(a[0], b3, 1, 0)
    return p[:m] + ((p[m : 2 * m] + q[:m]) + small)


def doths(a, qs):
    value = dot3(a, qs, 1, 1)
    exact = jnp.sum(a, 1, keepdims=True) * (1.0 / math.sqrt(a.shape[1]))
    return jnp.where(lanes_of(value.shape) == 0, exact, value)


def doth(a, b, ca=1, cb=0):
    return lax.dot_general(
        a, b, (((ca,), (cb,)), ((), ())), precision=lax.Precision.HIGHEST, preferred_element_type=f32
    )


def rows_of(shape):
    return lax.broadcasted_iota(jnp.int32, shape, 0)


def lanes_of(shape):
    return lax.broadcasted_iota(jnp.int32, shape, 1)


def pick(values, index):
    return jnp.sum(jnp.where(rows_of(values.shape) == index, values, 0.0), 0, keepdims=True)


def below(values):
    return jnp.concatenate([jnp.zeros_like(values[:1]), values[:-1]], 0)


def stacked(b):
    b1, b2, b3 = (piece.astype(f32) for piece in split3(b))
    return jnp.concatenate([b1, b2, b1, b2, b3, b1], 0).astype(bf16)


def dotk(a, b):
    return mm(a[:, : 6 * b.shape[0]], stacked(b), 1, 0)


def edge_solve(al, t0, couple, source, minv, kmats, special):
    M, n = al.shape
    L = min(n, 128)
    last = rows_of((M, n)) == M - 1
    w = al - jnp.concatenate([t0[1:], t0[:1]], 0)
    H = jnp.where(last, al, 0.0)
    tail = couple * al[M - 1 :]
    for p in range(M - 1):
        wp = w[p : p + 1] + tail if p == M - 2 else w[p : p + 1]
        H = H + minv[M * p : M * (p + 1), :] * wp
    Hz = dotk(kmats[0:M, :], jnp.concatenate([al[:, :L], source], 0))
    mean = dotk(kmats[M : 2 * M, :], jnp.concatenate([al[:, :L], t0[:, :L], Hz], 0))
    lane = lanes_of((M, L))
    first = jnp.where((lane == 0) & special, Hz, H[:, :L])
    H = first if n == L else jnp.concatenate([first, H[:, L:]], 1)
    return H, jnp.where(special, mean[:, :1], 0.0)


def to_peers(rows, members):
    one = jnp.concatenate(rows, 0)
    return jnp.broadcast_to(one[None], (members,) + one.shape)


def stage_local(r, c, M, wait, get):
    wait("q1", "x0", "x1", "q2")
    m1 = dot3(
        jnp.concatenate([get("x0"), get("x1")], 0), (get("q1"), get("q2")), 1, 1
    )
    wait("y")
    n = m1.shape[0]
    half = n // 2
    L = min(n, 128)
    n2 = dot3((get("q1"), get("q2")), get("y"))
    wait("s1", "s2", "r", "v", "col")
    ss = (get("s1"), get("s2"))
    f = dot3(ss, m1) + dot3(n2, ss, 1, 1)
    gyl = n2[:, n - L :].T[L - 1 :]
    u = -f * get("r")
    uh, ul = split(u)
    v = get("v")
    p = mm(v, uh, 1, 1)
    tk = p[:8] + (p[8:] + mm(v, ul, 1, 1)[:8])
    col = get("col")
    groups = []
    for rows in (slice(0, half), slice(half, n)):
        groups.append(
            jnp.concatenate(
                [
                    jnp.sum(u[rows, a : a + L] * col[rows], 0, keepdims=True)
                    for a in range(0, n, L)
                ],
                1,
            )
        )
    low, high = groups[0] + groups[1], groups[0] - groups[1]
    alpha = gyl + jnp.where(c < M - 1, tk[1:2], 0.0)
    beta = m1[n - 1 :] + jnp.where(r < M - 1, high, 0.0)
    return to_peers([alpha, tk[0:1], beta, low], M), u


WAVES = {None: ("q1", "x0", "x1", "q2"), "q1": ("y",), "x0": ("s1", "s2"), "x1": ("r", "v", "col")}
WAVES["y"] = ("vec", "wide", "turn", "w", "thin", "long", "mats", "kmats")
NAMES = sum(WAVES.values(), ())
KEPT = ("q1", "q2", "r") + WAVES["y"]


def run_local(members, arrays):
    n = arrays["q1"].shape[1]
    arrays["x0"], arrays["x1"] = arrays["x"][: n // 2], arrays["x"][n // 2 :]
    shapes = {name: (arrays[name].shape, arrays[name].dtype) for name in NAMES}
    if DIRECT:
        edges, u = stage_local(
            lax.axis_index("row"), lax.axis_index("col"), members, lambda *names: None,
            arrays.__getitem__,
        )
        return edges, u, {name: arrays[name] for name in KEPT}

    def kernel(*refs):
        count = len(NAMES)
        edges, u = refs[count : count + 2]
        here = dict(zip(KEPT, refs[count + 2 :]))
        here.update(zip((k for k in NAMES if k not in KEPT), refs[count + 2 + len(KEPT) :]))
        sem = refs[-1]
        def part_of(name, source):
            pick_half = {"x0": pl.ds(0, n // 2), "x1": pl.ds(n // 2, n // 2)}
            return source.at[pick_half[name]] if name in pick_half else source

        copies = {
            name: pltpu.make_async_copy(part_of(name, source), here[name], sem.at[i])
            for i, (name, source) in enumerate(zip(NAMES, refs))
        }

        def release(wave):
            for name in WAVES.get(wave, ()):
                copies[name].start()

        def wait(*names):
            for name in names:
                copies[name].wait()
                release(name)

        def get(name):
            return here[name][...]

        release(None)
        edges[...], u[...] = stage_local(
            lax.axis_index("row"), lax.axis_index("col"), members, wait, get
        )
        wait(*WAVES["y"])

    operands = [name if name not in ("x0", "x1") else "x" for name in NAMES]
    far, vmem, near = pl.BlockSpec(memory_space=pltpu.HBM), pl.BlockSpec(memory_space=pltpu.VMEM), pltpu.VMEM
    shape = {name: near(*shapes[name]) for name in NAMES}
    edges, u, *tables = pl.pallas_call(
        kernel,
        out_shape=[jax.ShapeDtypeStruct((members, 4, n), f32), near((n, n), f32)]
        + [shape[name] for name in KEPT],
        in_specs=[far] * len(NAMES),
        out_specs=[vmem] * (2 + len(KEPT)),
        scratch_shapes=[shape[name] for name in NAMES if name not in KEPT]
        + [pltpu.SemaphoreType.DMA((len(NAMES),))],
        compiler_params=pltpu.CompilerParams(vmem_limit_bytes=VMEM_LIMIT),
        name="stage_local",
    )(*(pltpu.with_memory_space_constraint(arrays[name], pltpu.HBM) for name in operands))
    return edges, u, dict(zip(KEPT, tables))


def lane_pick(values, index):
    return jnp.sum(jnp.where(lanes_of(values.shape) == index, values, 0.0), 1, keepdims=True)


def stage_strip(r, c, M, ag, q1, q2, vec, wide, turn, w, thin, long, mats, kmats):
    n = q1.shape[0]
    half = n // 2
    r1, r2, r3 = (wide[a * n : (a + 1) * n, :] for a in range(1, 4))
    b1, b2 = wide[4 * n : 4 * n + half, :], wide[4 * n + half : 5 * n, :]
    acs = long[M * M : M * M + 4 * M, :]
    al, t0, be, ta0 = (ag[:, a, :] for a in range(4))
    vec, mats = vec[...], mats[...]
    v0, v1, couple = vec[0:1], vec[1:2], vec[4:5]
    L = min(n, 128)
    qq = 1.0 / math.sqrt(n)
    zero = jnp.zeros((M, L), f32)
    sa, stt = mats[:M, :M], mats[:M, M : 2 * M]

    H, mean = edge_solve(al, t0, couple, zero, long, kmats, True)
    rs = (r1, r2)
    Z = dot6(jnp.concatenate([H * v0, H * v1], 0), rs + (r3,))
    add0 = v0 * below(Z[:M]) - v1 * Z[:M]
    add1 = v0 * below(Z[M:]) - v1 * Z[M:]
    flat = jnp.where(lanes_of((M, n)) == 0, mean * qq, 0.0)
    tau0 = ta0 + add0 + flat
    tau1 = be + jnp.where(r < M - 1, add1 + flat, 0.0)

    qs = (q1[...], q2[...])
    y = dot6(jnp.concatenate([tau1, tau0], 0), qs + (wide[:n, :],))
    ca, sna, swap, c16 = (acs[a * M : (a + 1) * M, :] for a in range(4))
    c16 = c16[:1]
    g = dotk(kmats[4 * M : 6 * M, :], jnp.concatenate([y[:M], y[M:]], 1))
    xs, ys, extra = [], [], []
    for side in range(2):
        C, S = (g[k * M : (k + 1) * M, side * n : (side + 1) * n] for k in range(2))
        xs.append(C * ca - S * sna)
        ys.append(C * sna + S * swap)
        extra.append(S[:1] * c16)
    xs += extra + [jnp.zeros((M - 2, n), f32)]
    cosines = tuple(turn[2 * n * a : 2 * n * a + n, :] for a in range(3))
    sines = tuple(turn[2 * n * a + n : 2 * n * (a + 1), :] for a in range(3))
    xcos = dot6(jnp.concatenate(xs, 0), cosines)
    ysin = dot6(jnp.concatenate(ys, 0), sines)
    pair = (M, half)
    left_lane, top_row = lanes_of(pair) == 0, rows_of(pair) == 0
    shape = (2 * M, half)
    origin = (rows_of(shape) == 0) & (lanes_of(shape) == 0)
    root = 1.0 / math.sqrt(M)
    wider = (lanes_of(shape) == 0) & (rows_of(shape) > 0) & (rows_of(shape) < M)
    scale = jnp.where(wider, root * math.sqrt(2.0), root)
    ends = []
    for side in range(2):
        xc, yb = xcos[side * M : (side + 1) * M], ysin[side * M : (side + 1) * M]
        plus = xc - jnp.where(left_lane | top_row, 0.0, yb)
        alone = jnp.where(top_row, xcos[2 * M + side : 2 * M + side + 1], xc)
        minus = jnp.where(left_lane, 0.0, alone) + yb
        ends.append(jnp.concatenate([plus, minus], 0) * scale)
    T1, T0 = ends

    own = rows_of((M, L)) == r
    alz = jnp.where(own, T1[:1, :1], 0.0)
    t0z = jnp.where(own, T0[:1, :1], 0.0)
    src = jnp.where(own, al[M - 1 :, :1] * (1.0 / math.sqrt(M)), 0.0)
    Hz = dotk(kmats[0:M, :], jnp.concatenate([alz, src], 0))
    lift = dotk(kmats[M : 2 * M, :], jnp.concatenate([alz, t0z, Hz], 0))
    g0 = jnp.where(rows_of((M, L)) == M - 1, Hz, dotk(kmats[2 * M : 3 * M, :], Hz))
    up, down = lane_pick(sa, r), lane_pick(stt, r)
    T1c = jnp.where(r == M - 1, T1 * thin[2 * M * (M - 1) :, :], T1)
    modes = []
    for m in range(M - 1):
        value = (up[m : m + 1] * T1c + down[m : m + 1] * T0) * thin[2 * M * m : 2 * M * (m + 1), :]
        modes.append(jnp.where(origin, g0[m : m + 1, :1] * root, value))
    modes.append(jnp.where(r == M - 1, T1, 0.0) * scale)
    sums, gaps, single = [], [], []
    for value in modes:
        gp, gm = value[:M], value[M:]
        sums.append(gp + jnp.where(left_lane | top_row, 0.0, gm))
        gaps.append(jnp.where(top_row, gm, jnp.where(left_lane, 0.0, gp) - gm))
        single.append(jnp.where(left_lane[:1], 0.0, gm[:1]))
    XC = dot3s(split(jnp.concatenate(sums + single, 0)), (qs[0][:half], qs[1][:half]))
    XS = dot3s(split(jnp.concatenate(gaps, 0)), (b1, b2))
    third = w.shape[0] // 3
    ws = tuple(w[third * a : third * (a + 1), :] for a in range(3))
    group = w.shape[1] // (2 * M)
    lines = []
    top_line = rows_of((M, n)) == 0
    for first in range(0, M, group):
        rots = []
        for m in range(first, first + group):
            xc, xs = XC[M * m : M * (m + 1)], XS[M * m : M * (m + 1)]
            alone = jnp.where(top_line, c16 * XC[M * M + m : M * M + m + 1], 0.0)
            rots += [ca * xc - sna * xs, sna * xc + swap * xs + alone]
        lines.append(dotl(ws, jnp.concatenate(rots, 0)))
    hx = doths(jnp.concatenate(lines, 0), qs)
    Y = dot3(jnp.concatenate([hx * v0, hx * v1], 0), rs)
    Y0, Y1 = Y[: M * M], Y[M * M :]

    first = lanes_of((1, n)) == 0
    cols = []
    for cc in (c, c - 1):
        k1 = long[pl.ds(pl.multiple_of(jnp.maximum(cc, 0) * M, M), M), :]
        k1 = jnp.where(cc < 0, 0.0, k1)
        cols.append((k1, -below(k1), lane_pick(mats[M : 2 * M, :M], cc) * (-1.0 / qq)))
    ka, kt = lane_pick(mats[2 * M : 3 * M, :M], c), lane_pick(mats[3 * M : 4 * M, :M], c)
    kth = lane_pick(mats[4 * M : 5 * M, :M], c)
    here, side_c, side_b, level = [], [], [], []
    for m in range(M):
        rows = slice(M * m, M * (m + 1))
        hm, y0, y1 = hx[rows], Y0[rows], Y1[rows]
        here.append(pick(hm, c))
        for (k1, k2, ksrc), sides in zip(cols, (side_c, side_b)):
            phi = jnp.sum(k1 * y1 + k2 * y0, 0, keepdims=True)
            z = jnp.sum(ksrc * hm, 0, keepdims=True)
            sides.append(jnp.where(first, z, phi))
        level.append(
            jnp.sum(kth * hm[:, :L] - ka * y1[:, :L] - kt * y0[:, :L], 0, keepdims=True)
        )
    rows = [jnp.concatenate(v, 0) for v in (here, side_c, side_b, level)]
    mixed = dotk(kmats[3 * M : 4 * M, :], jnp.concatenate(rows, 1))
    mixed = [mixed[:, a * n : (a + 1) * n] for a in range(4)]
    right, fc, fb, lv = mixed
    lv = (lv - below(lv) + lift * (1.0 / math.sqrt(M)))[:, :1]
    share = [
        below(right),
        right,
        v0 * below(fc) - v1 * fc,
        v0 * below(fb) - v1 * fb,
        lv,
    ]
    keep = [pick(H, c), pick(H, c - 1), jnp.broadcast_to(pick(mean, c), (1, n))]
    return share, jnp.concatenate(keep + [jnp.zeros((5, n), f32)], 0)


def stage_field(r, c, M, share, keep, u, qh, ql, rr, vec):
    keep, vec = keep[...], vec[...]
    n = vec.shape[1]
    q0, q1 = vec[0:1], vec[1:2]
    left, right, here, before, level = (
        jnp.sum(share[:, a, :n] if a < 4 else share[:, 0, n:], 0, keepdims=True) for a in range(5)
    )
    here = here + keep[0:1]
    before = before + keep[1:2]
    level = level[:, :1] + keep[2:3, :1]
    pad = jnp.zeros((4, n), f32)
    a1, a2, a3 = (
        piece.astype(f32) for piece in split3(jnp.concatenate([q1, -q0, here, -before, pad], 0))
    )
    lhs = jnp.concatenate([a1, a1, a2, a2, a1, a3], 0).astype(bf16)
    G = mm(lhs, stacked(jnp.concatenate([right, left, q1, q0, pad], 0)), 0, 0)
    un = u[...] - rr[...] * G
    un = jnp.where((rows_of(un.shape) == 0) & (lanes_of(un.shape) == 0), level, un)
    qs = (qh[...], ql[...])
    half = split(dot3(un, qs))
    step = n // 4
    for part in range(4):
        cols = slice(part * step, (part + 1) * step)
        yield dot3((qs[0][:, cols], qs[1][:, cols]), half, 0, 0)


def run_field(members, *args):
    n = args[-1].shape[1]
    place = lambda: (lax.axis_index("row"), lax.axis_index("col"))
    if DIRECT:
        return jnp.concatenate(list(stage_field(*place(), members, *args)), 0)

    def kernel(*refs):
        field, rows, sem = refs[len(args) :]
        copies = []
        for part, value in enumerate(stage_field(*place(), members, *refs[: len(args)])):
            step = value.shape[0]
            span = slice(part * step, (part + 1) * step)
            rows[span, :] = value
            copies.append(pltpu.make_async_copy(rows.at[span], field.at[span], sem.at[part]))
            copies[-1].start()
        for copy in copies:
            copy.wait()

    vmem = pl.BlockSpec(memory_space=pltpu.VMEM)
    return pl.pallas_call(
        kernel,
        out_shape=jax.ShapeDtypeStruct((n, n), f32),
        in_specs=[vmem] * len(args),
        out_specs=pl.BlockSpec(memory_space=pltpu.HBM),
        scratch_shapes=[pltpu.VMEM((n, n), f32), pltpu.SemaphoreType.DMA((4,))],
        compiler_params=pltpu.CompilerParams(vmem_limit_bytes=VMEM_LIMIT),
        name="stage_field",
    )(*args)


def packed(rows):
    tail = jnp.broadcast_to(rows[4][:, :, None], rows[4].shape[:1] + (4, 128))
    return jnp.concatenate([jnp.stack(rows[:4], 1), tail], 2)


def run_stage(stage, members, outs, *args):
    if DIRECT:
        results = stage(lax.axis_index("row"), lax.axis_index("col"), members, *args)
        return [packed(v) if isinstance(v, list) else v for v in results]

    def kernel(*refs):
        r, c = lax.axis_index("row"), lax.axis_index("col")
        n = args[0].shape[-1]
        results = stage(r, c, members, *refs[: len(args)])
        for ref, value in zip(refs[len(args) :], results):
            if isinstance(value, list):
                for a, row in enumerate(value[:4]):
                    ref[:, a, :n] = row
                ref[:, :, n:] = jnp.broadcast_to(value[4][:, :, None], (members, 4, 128))
            else:
                ref[...] = value

    vmem = pl.BlockSpec(memory_space=pltpu.VMEM)
    return pl.pallas_call(
        kernel,
        out_shape=outs,
        in_specs=[vmem] * len(args),
        out_specs=[vmem] * len(outs),
        compiler_params=pltpu.CompilerParams(vmem_limit_bytes=VMEM_LIMIT),
        name=stage.__name__,
    )(*args)


def exchange(values, axis):
    return lax.all_to_all(values, axis, split_axis=0, concat_axis=0, tiled=True)


def make_body(members):
    def body(grad_x, grad_y):
        n = grad_x.shape[0]
        t = {k: jnp.asarray(v) for k, v in build_tables(n, members).items()}
        sent, near = jax.ShapeDtypeStruct, pltpu.VMEM
        edges, u, kept = run_local(members, {**t, "x": grad_x, "y": grad_y})
        strip = exchange(edges, "col")
        share, keep = run_stage(
            stage_strip, members, [sent((members, 4, n + 128), f32), near((8, n), f32)],
            strip, kept["q1"], kept["q2"], *(kept[name] for name in WAVES["y"]),
        )
        share = exchange(share, "row")
        return run_field(
            members, share, keep, u, kept["q1"], kept["q2"], kept["r"], kept["vec"]
        )

    return body


def solution(mesh):
    members = mesh.shape["row"]
    placed = (P("row", "col"), P("row", "col"))
    return jax.shard_map(
        make_body(members), mesh=mesh, in_specs=placed, out_specs=P("row", "col"), check_vma=False
    )
```

```python
import math

import jax
import jax.numpy as jnp
import numpy as np
from jax import lax
from jax.experimental import pallas as pl
from jax.experimental.pallas import tpu as pltpu
from jax.sharding import PartitionSpec as P

VMEM_LIMIT = 32 * 1024 * 1024
DIRECT = False
f32 = jnp.float32
bf16 = jnp.bfloat16


def cosine_basis(n):
    k, i = np.arange(n)[:, None], np.arange(n)[None]
    return np.sqrt(np.where(k == 0, 1, 2) / n) * np.cos(np.pi * k * (2 * i + 1) / (2 * n))


def edge_tables(n, members, freq):
    s = 2 * np.sin(freq)
    half = np.arcsinh(s / 2)
    e = np.exp(-2 * n * half)
    safe = np.where(s == 0, 1, s)
    e1 = np.where(s == 0, 0.5, e)
    th = np.tanh(np.arcsinh(safe / 2))
    one = np.where(s == 0, 0, 1)
    lead = one * th * (1 - e1 * e1)
    couple = one * e1 / (th * (1 - e1 * e1))
    return lead, e, couple


def pieces_of(value, count):
    found = []
    for _ in range(count):
        found.append(np.asarray(value, jnp.bfloat16))
        value = value - found[-1].astype(np.float64)
    return found


def stack_pieces(value):
    a1, a2, a3 = pieces_of(value, 3)
    return np.concatenate([a1, a1, a2, a2, a1, a3], 1)


def build_tables(n, members):
    total = n * members
    half = n // 2
    k = np.concatenate([np.arange(0, n, 2), np.arange(1, n, 2)])
    q = cosine_basis(n)[k]
    s = 2 * np.sin(np.pi * k / (2 * n))
    q0, q1 = q[:, 0], q[:, -1]
    lead, e, couple = edge_tables(n, members, np.pi * k / (2 * n))
    vec = np.zeros((8, n))
    vec[0], vec[1], vec[2], vec[3], vec[4] = q0, q1, lead, e, couple
    lane = np.arange(half)
    other = np.where(lane == 0, half, lane)
    d = np.arange(members)
    kap = np.concatenate(
        [
            d[:, None] + 2 * members * lane[None],
            2 * members * other[None] - np.where(d == 0, members, d)[:, None],
        ]
    )
    glob = np.stack(edge_tables(n, members, np.pi * kap / (2 * total)))
    bend = 1 + glob[1] ** 2 - 2 * glob[1] * np.cos(np.pi * np.arange(1, members) / members)[:, None, None]
    size = np.full((2 * members, half), 1 / np.sqrt(members))
    size[1:members, 0] *= np.sqrt(2)
    dens = (glob[0] * size / bend).reshape(-1, half)
    j = 2 * np.arange(n) + 1
    sb = np.sqrt(2 / n) * np.sin(np.pi * other[:, None] * j[None] / n)
    turn = np.concatenate([q[:half].T, sb.T], 0)
    sp = np.sqrt(2 / n) * s[:, None] * np.sin(np.pi * k[:, None] * (np.arange(n)[None] + 1) / n)
    sp[:, n - 1] = 0
    sp[0] = 0
    den = s[:, None] ** 2 + s[None] ** 2
    den[0, 0] = 1
    r = 1 / den
    r[0, 0] = 0
    ang = np.pi * np.arange(members + 1)[:, None] * j[None] / (2 * total)
    ca, sa = np.cos(ang), np.sin(ang)
    swap = np.concatenate([sa[members:], ca[1:members]], 0)
    acs = np.concatenate([ca[:members], sa[:members], swap, np.repeat(ca[members:], members, 0)], 0)
    p = np.arange(members)
    wang = np.pi * np.arange(members + 1)[:, None] * p[None] / members
    wc, ws = np.cos(wang), np.sin(wang)
    wfwd = np.concatenate([wc[:members], wc[members:], ws[1:members]], 0)
    winv = np.concatenate([wc[:members], wc[members:], -ws[1:members]], 0).T
    M = members
    t = np.arange(1, M)
    st = np.sqrt(2 / M) * np.sin(np.pi * np.outer(t, t) / M)
    sa, stt, s2 = np.zeros((M, M)), np.zeros((M, M)), np.zeros((M, M))
    sa[: M - 1, : M - 1] = st
    sa[: M - 1, M - 1] = st[:, M - 2]
    stt[: M - 1, 1:] = -st
    s2[: M - 1, : M - 1] = st
    a0 = (q1[1:] ** 2 / s[1:] ** 2).sum()
    b0 = (q0[1:] * q1[1:] / s[1:] ** 2).sum()
    qq = 1 / np.sqrt(n)
    pp = np.arange(M)
    frac = (pp[:, None] + 1) / M
    t1 = frac - (pp[None] <= pp[:, None])
    h15 = np.zeros((M, M))
    h15[:, M - 1] = frac[:, 0]
    hmat = np.concatenate([h15, t1], 1)
    acc = (pp[None] < pp[:, None]).astype(float)
    acc[:, M - 1] = 0
    acc = (acc - acc.mean(0)) / qq
    up = np.zeros((M, M))
    up[:-1, 1:] = np.eye(M - 1)
    keep = np.eye(M)
    keep[M - 1, M - 1] = 0
    ka = acc @ keep
    kt = -acc @ (keep @ up)
    kh = acc @ (keep @ (-(1 + 2 * a0) * np.eye(M) + b0 * up + b0 * up.T))
    s2x = s2.copy()
    s2x[M - 1, M - 1] = 1
    per = min(M, 256 // (2 * M))
    wbd = np.kron(np.eye(per), winv)
    minv = np.zeros((M, M, n))
    lean = lead / (1 + e * e - 2 * e * np.cos(np.pi * t / M)[:, None])
    minv[: M - 1, : M - 1] = np.einsum("pm,mk,mq->pqk", st, lean, st)
    mats = np.zeros((8 * M, 128))
    mats[0:M, : 2 * M] = np.concatenate([sa, stt], 1)
    mats[M : 2 * M, :M] = t1.T
    mats[2 * M : 3 * M, :M] = ka.T * qq
    mats[3 * M : 4 * M, :M] = kt.T * qq
    mats[4 * M : 5 * M, :M] = (kh @ t1).T
    step = (pp[:, None] >= pp[None]).astype(float)
    blocks = (ka, kt, s2x @ step, kh @ step, s2x @ frac, kh @ frac, frac)
    for a, block in enumerate(blocks):
        mats[5 * M : 6 * M, a * M : a * M + block.shape[1]] = block
    kmats = np.zeros((8 * M, 384), jnp.bfloat16)
    row = 0
    for small in (hmat, np.concatenate([ka, kt, kh], 1), s2, s2x, wfwd):
        stacked = stack_pieces(small)
        kmats[row : row + small.shape[0], : stacked.shape[1]] = stacked
        row += small.shape[0]
    q1, q2, q3 = pieces_of(q, 3)
    s1, s2 = pieces_of(sp, 2)
    v1, v2 = pieces_of(vec, 2)
    out = dict(
        vec=vec, r=r, col=np.repeat(q0[:, None], min(n, 128), 1), mats=mats,
        thin=np.concatenate([dens, glob[2]], 0),
        long=np.concatenate([minv.reshape(-1, n), acs], 0),
    )
    out = {name: np.asarray(value, np.float32) for name, value in out.items()}
    out.update(
        q1=q1, q2=q2, s1=s1, s2=s2, v=np.concatenate([v1, v2], 0), kmats=kmats,
        w=np.concatenate(pieces_of(wbd, 3), 0), turn=np.concatenate(pieces_of(turn, 3), 0),
        wide=np.concatenate([q3] + pieces_of(r, 3) + pieces_of(sb, 2), 0),
    )
    return out


def split(a):
    high = a.astype(bf16)
    return high, (a - high.astype(f32)).astype(bf16)


def mm(a, b, ca, cb):
    return lax.dot_general(a, b, (((ca,), (cb,)), ((), ())), preferred_element_type=f32)


def dot3s(a, b, ca=1, cb=0):
    ah, al = a if isinstance(a, tuple) else split(a)
    bh, bl = b if isinstance(b, tuple) else split(b)
    return mm(ah, bh, ca, cb) + (mm(ah, bl, ca, cb) + mm(al, bh, ca, cb))


def dot3(a, b, ca=1, cb=0):
    ah, al = a if isinstance(a, tuple) else split(a)
    bh, bl = b if isinstance(b, tuple) else split(b)
    return mm(jnp.concatenate([ah, ah, al], ca), jnp.concatenate([bh, bl, bh], cb), ca, cb)


def split3(a):
    high, rest = a.astype(bf16), None
    rest = a - high.astype(f32)
    mid = rest.astype(bf16)
    return high, mid, (rest - mid.astype(f32)).astype(bf16)


def dot6(a, b, cb=0):
    m = a.shape[0]
    a1, a2, a3 = split3(a)
    b1, b2, b3 = b
    p = mm(jnp.concatenate([a1, a2, a3], 0), b1, 1, cb)
    q = mm(jnp.concatenate([a1, a2], 0), b2, 1, cb)
    small = (p[2 * m :] + q[m:]) + mm(a1, b3, 1, cb)
    return p[:m] + ((p[m : 2 * m] + q[:m]) + small)


def dotl(a, b):
    m = a[0].shape[0]
    b1, b2, b3 = split3(b)
    p = mm(jnp.concatenate(a, 0), b1, 1, 0)
    q = mm(jnp.concatenate(a[:2], 0), b2, 1, 0)
    small = (p[2 * m :] + q[m:]) + mm(a[0], b3, 1, 0)
    return p[:m] + ((p[m : 2 * m] + q[:m]) + small)


def doths(a, qs):
    value = dot3(a, qs, 1, 1)
    exact = jnp.sum(a, 1, keepdims=True) * (1.0 / math.sqrt(a.shape[1]))
    return jnp.where(lanes_of(value.shape) == 0, exact, value)


def doth(a, b, ca=1, cb=0):
    return lax.dot_general(
        a, b, (((ca,), (cb,)), ((), ())), precision=lax.Precision.HIGHEST, preferred_element_type=f32
    )


def rows_of(shape):
    return lax.broadcasted_iota(jnp.int32, shape, 0)


def lanes_of(shape):
    return lax.broadcasted_iota(jnp.int32, shape, 1)


def pick(values, index):
    return jnp.sum(jnp.where(rows_of(values.shape) == index, values, 0.0), 0, keepdims=True)


def below(values):
    return jnp.concatenate([jnp.zeros_like(values[:1]), values[:-1]], 0)


def stacked(b):
    b1, b2, b3 = (piece.astype(f32) for piece in split3(b))
    return jnp.concatenate([b1, b2, b1, b2, b3, b1], 0).astype(bf16)


def dotk(a, b):
    return mm(a[:, : 6 * b.shape[0]], stacked(b), 1, 0)


def edge_solve(al, t0, couple, minv, mats, kmats):
    M, n = al.shape
    L = min(n, 128)
    last = rows_of((M, n)) == M - 1
    w = al - jnp.concatenate([t0[1:], t0[:1]], 0)
    H = jnp.where(last, al, 0.0)
    tail = couple * al[M - 1 :]
    for p in range(M - 1):
        wp = w[p : p + 1] + tail if p == M - 2 else w[p : p + 1]
        H = H + minv[M * p : M * (p + 1), :] * wp
    Hz = mats[5 * M : 6 * M, 6 * M : 6 * M + 1] * al[M - 1 :, :L]
    mean = dotk(kmats[M : 2 * M, :], jnp.concatenate([al[:, :L], t0[:, :L], Hz], 0))
    lane = lanes_of((M, L))
    first = jnp.where(lane == 0, Hz, H[:, :L])
    H = first if n == L else jnp.concatenate([first, H[:, L:]], 1)
    return H, mean[:, :1]


def to_peers(rows, members):
    one = jnp.concatenate(rows, 0)
    return jnp.broadcast_to(one[None], (members,) + one.shape)


def stage_local(r, c, M, wait, get):
    wait("q1", "x0", "x1", "q2")
    m1 = dot3(
        jnp.concatenate([get("x0"), get("x1")], 0), (get("q1"), get("q2")), 1, 1
    )
    wait("y", "s1", "s2", "r", "v", "col")
    n = m1.shape[0]
    half = n // 2
    L = min(n, 128)
    n2 = dot3((get("q1"), get("q2")), get("y"))
    ss = (get("s1"), get("s2"))
    f = dot3(ss, m1) + dot3(n2, ss, 1, 1)
    gyl = n2[:, n - L :].T[L - 1 :]
    u = -f * get("r")
    uh, ul = split(u)
    v = get("v")
    p = mm(v, uh, 1, 1)
    tk = p[:8] + (p[8:] + mm(v, ul, 1, 1)[:8])
    col = get("col")
    groups = []
    for rows in (slice(0, half), slice(half, n)):
        groups.append(
            jnp.concatenate(
                [
                    jnp.sum(u[rows, a : a + L] * col[rows], 0, keepdims=True)
                    for a in range(0, n, L)
                ],
                1,
            )
        )
    low, high = groups[0] + groups[1], groups[0] - groups[1]
    alpha = gyl + jnp.where(c < M - 1, tk[1:2], 0.0)
    beta = m1[n - 1 :] + jnp.where(r < M - 1, high, 0.0)
    return to_peers([alpha, tk[0:1], beta, low], M), u


WAVES = {None: ("q1", "x0", "x1", "q2", "y", "s1", "s2", "r", "v", "col")}
WAVES["y"] = ("vec", "wide", "turn", "w", "thin", "long", "mats", "kmats")
NAMES = sum(WAVES.values(), ())
KEPT = ("q1", "q2", "r") + WAVES["y"]


def run_local(members, arrays):
    n = arrays["q1"].shape[1]
    arrays["x0"], arrays["x1"] = arrays["x"][: n // 2], arrays["x"][n // 2 :]
    shapes = {name: (arrays[name].shape, arrays[name].dtype) for name in NAMES}
    if DIRECT:
        edges, u = stage_local(
            lax.axis_index("row"), lax.axis_index("col"), members, lambda *names: None,
            arrays.__getitem__,
        )
        return edges, u, {name: arrays[name] for name in KEPT}

    def kernel(*refs):
        count = len(NAMES)
        edges, u = refs[count : count + 2]
        here = dict(zip(KEPT, refs[count + 2 :]))
        here.update(zip((k for k in NAMES if k not in KEPT), refs[count + 2 + len(KEPT) :]))
        sem = refs[-1]
        def part_of(name, source):
            pick_half = {"x0": pl.ds(0, n // 2), "x1": pl.ds(n // 2, n // 2)}
            return source.at[pick_half[name]] if name in pick_half else source

        copies = {
            name: pltpu.make_async_copy(part_of(name, source), here[name], sem.at[i])
            for i, (name, source) in enumerate(zip(NAMES, refs))
        }

        def release(wave):
            for name in WAVES.get(wave, ()):
                copies[name].start()

        def wait(*names):
            for name in names:
                copies[name].wait()
                release(name)

        def get(name):
            return here[name][...]

        release(None)
        edges[...], u[...] = stage_local(
            lax.axis_index("row"), lax.axis_index("col"), members, wait, get
        )
        wait(*WAVES["y"])

    operands = [name if name not in ("x0", "x1") else "x" for name in NAMES]
    far, vmem, near = pl.BlockSpec(memory_space=pltpu.HBM), pl.BlockSpec(memory_space=pltpu.VMEM), pltpu.VMEM
    shape = {name: near(*shapes[name]) for name in NAMES}
    edges, u, *tables = pl.pallas_call(
        kernel,
        out_shape=[jax.ShapeDtypeStruct((members, 4, n), f32), near((n, n), f32)]
        + [shape[name] for name in KEPT],
        in_specs=[far] * len(NAMES),
        out_specs=[vmem] * (2 + len(KEPT)),
        scratch_shapes=[shape[name] for name in NAMES if name not in KEPT]
        + [pltpu.SemaphoreType.DMA((len(NAMES),))],
        compiler_params=pltpu.CompilerParams(vmem_limit_bytes=VMEM_LIMIT),
        name="stage_local",
    )(*(pltpu.with_memory_space_constraint(arrays[name], pltpu.HBM) for name in operands))
    return edges, u, dict(zip(KEPT, tables))


def lane_pick(values, index):
    return jnp.sum(jnp.where(lanes_of(values.shape) == index, values, 0.0), 1, keepdims=True)


def stage_strip(r, c, M, ag, q1, q2, vec, wide, turn, w, thin, long, mats, kmats):
    n = q1.shape[0]
    half = n // 2
    r1, r2, r3 = (wide[a * n : (a + 1) * n, :] for a in range(1, 4))
    b1, b2 = wide[4 * n : 4 * n + half, :], wide[4 * n + half : 5 * n, :]
    acs = long[M * M : M * M + 4 * M, :]
    al, t0, be, ta0 = (ag[:, a, :] for a in range(4))
    vec, mats = vec[...], mats[...]
    v0, v1, couple = vec[0:1], vec[1:2], vec[4:5]
    L = min(n, 128)
    qq = 1.0 / math.sqrt(n)
    sa, stt = mats[:M, :M], mats[:M, M : 2 * M]

    H, mean = edge_solve(al, t0, couple, long, mats, kmats)
    rs = (r1, r2)
    Z = dot6(jnp.concatenate([H * v0, H * v1], 0), rs + (r3,))
    add0 = v0 * below(Z[:M]) - v1 * Z[:M]
    add1 = v0 * below(Z[M:]) - v1 * Z[M:]
    flat = jnp.where(lanes_of((M, n)) == 0, mean * qq, 0.0)
    tau0 = ta0 + add0 + flat
    tau1 = be + jnp.where(r < M - 1, add1 + flat, 0.0)

    qs = (q1[...], q2[...])
    y = dot6(jnp.concatenate([tau1, tau0], 0), qs + (wide[:n, :],))
    ca, sna, swap, c16 = (acs[a * M : (a + 1) * M, :] for a in range(4))
    c16 = c16[:1]
    g = dotk(kmats[4 * M : 6 * M, :], jnp.concatenate([y[:M], y[M:]], 1))
    xs, ys, extra = [], [], []
    for side in range(2):
        C, S = (g[k * M : (k + 1) * M, side * n : (side + 1) * n] for k in range(2))
        xs.append(C * ca - S * sna)
        ys.append(C * sna + S * swap)
        extra.append(S[:1] * c16)
    xs += extra + [jnp.zeros((M - 2, n), f32)]
    cosines = tuple(turn[2 * n * a : 2 * n * a + n, :] for a in range(3))
    sines = tuple(turn[2 * n * a + n : 2 * n * (a + 1), :] for a in range(3))
    xcos = dot6(jnp.concatenate(xs, 0), cosines)
    ysin = dot6(jnp.concatenate(ys, 0), sines)
    pair = (M, half)
    left_lane, top_row = lanes_of(pair) == 0, rows_of(pair) == 0
    shape = (2 * M, half)
    origin = (rows_of(shape) == 0) & (lanes_of(shape) == 0)
    root = 1.0 / math.sqrt(M)
    wider = (lanes_of(shape) == 0) & (rows_of(shape) > 0) & (rows_of(shape) < M)
    scale = jnp.where(wider, root * math.sqrt(2.0), root)
    ends = []
    for side in range(2):
        xc, yb = xcos[side * M : (side + 1) * M], ysin[side * M : (side + 1) * M]
        plus = xc - jnp.where(left_lane | top_row, 0.0, yb)
        alone = jnp.where(top_row, xcos[2 * M + side : 2 * M + side + 1], xc)
        minus = jnp.where(left_lane, 0.0, alone) + yb
        ends.append(jnp.concatenate([plus, minus], 0) * scale)
    T1, T0 = ends

    edge = mats[5 * M : 6 * M, :]
    src = al[M - 1 :, :1] * (1.0 / math.sqrt(M))
    a15 = jnp.where(r == M - 1, T1[:1, :1], 0.0)
    kac, ktc, gstep, hstep = (lane_pick(edge[:, a * M : (a + 1) * M], r) for a in range(4))
    gfrac, hfrac = edge[:, 4 * M : 4 * M + 1], edge[:, 5 * M : 5 * M + 1]
    lift = kac * T1[:1, :1] + ktc * T0[:1, :1] + hfrac * (a15 + src) - hstep * src
    g0 = gfrac * (a15 + src) - gstep * src
    up, down = lane_pick(sa, r), lane_pick(stt, r)
    T1c = jnp.where(r == M - 1, T1 * thin[2 * M * (M - 1) :, :], T1)
    modes = []
    for m in range(M - 1):
        value = (up[m : m + 1] * T1c + down[m : m + 1] * T0) * thin[2 * M * m : 2 * M * (m + 1), :]
        modes.append(jnp.where(origin, g0[m : m + 1, :1] * root, value))
    modes.append(jnp.where(r == M - 1, T1, 0.0) * scale)
    sums, gaps, single = [], [], []
    for value in modes:
        gp, gm = value[:M], value[M:]
        sums.append(gp + jnp.where(left_lane | top_row, 0.0, gm))
        gaps.append(jnp.where(top_row, gm, jnp.where(left_lane, 0.0, gp) - gm))
        single.append(jnp.where(left_lane[:1], 0.0, gm[:1]))
    XC = dot3s(split(jnp.concatenate(sums + single, 0)), (qs[0][:half], qs[1][:half]))
    XS = dot3s(split(jnp.concatenate(gaps, 0)), (b1, b2))
    third = w.shape[0] // 3
    ws = tuple(w[third * a : third * (a + 1), :] for a in range(3))
    group = w.shape[1] // (2 * M)
    lines = []
    top_line = rows_of((M, n)) == 0
    for first in range(0, M, group):
        rots = []
        for m in range(first, first + group):
            xc, xs = XC[M * m : M * (m + 1)], XS[M * m : M * (m + 1)]
            alone = jnp.where(top_line, c16 * XC[M * M + m : M * M + m + 1], 0.0)
            rots += [ca * xc - sna * xs, sna * xc + swap * xs + alone]
        lines.append(dotl(ws, jnp.concatenate(rots, 0)))
    hx = doths(jnp.concatenate(lines, 0), qs)
    Y = dot3(jnp.concatenate([hx * v0, hx * v1], 0), rs)
    Y0, Y1 = Y[: M * M], Y[M * M :]

    first = lanes_of((1, n)) == 0
    cols = []
    for cc in (c, c - 1):
        k1 = long[pl.ds(pl.multiple_of(jnp.maximum(cc, 0) * M, M), M), :]
        k1 = jnp.where(cc < 0, 0.0, k1)
        cols.append((k1, -below(k1), lane_pick(mats[M : 2 * M, :M], cc) * (-1.0 / qq)))
    ka, kt = lane_pick(mats[2 * M : 3 * M, :M], c), lane_pick(mats[3 * M : 4 * M, :M], c)
    kth = lane_pick(mats[4 * M : 5 * M, :M], c)
    here, side_c, side_b, level = [], [], [], []
    for m in range(M):
        rows = slice(M * m, M * (m + 1))
        hm, y0, y1 = hx[rows], Y0[rows], Y1[rows]
        here.append(pick(hm, c))
        for (k1, k2, ksrc), sides in zip(cols, (side_c, side_b)):
            phi = jnp.sum(k1 * y1 + k2 * y0, 0, keepdims=True)
            z = jnp.sum(ksrc * hm, 0, keepdims=True)
            sides.append(jnp.where(first, z, phi))
        level.append(
            jnp.sum(kth * hm[:, :L] - ka * y1[:, :L] - kt * y0[:, :L], 0, keepdims=True)
        )
    rows = [jnp.concatenate(v, 0) for v in (here, side_c, side_b, level)]
    mixed = dotk(kmats[3 * M : 4 * M, :], jnp.concatenate(rows, 1))
    mixed = [mixed[:, a * n : (a + 1) * n] for a in range(4)]
    right, fc, fb, lv = mixed
    lv = (lv - below(lv) + lift * (1.0 / math.sqrt(M)))[:, :1]
    share = [
        below(right),
        right,
        v0 * below(fc) - v1 * fc,
        v0 * below(fb) - v1 * fb,
        lv,
    ]
    keep = [pick(H, c), pick(H, c - 1), jnp.broadcast_to(pick(mean, c), (1, n))]
    return share, jnp.concatenate(keep + [jnp.zeros((5, n), f32)], 0)


def stage_field(r, c, M, share, keep, u, qh, ql, rr, vec):
    keep, vec = keep[...], vec[...]
    n = vec.shape[1]
    q0, q1 = vec[0:1], vec[1:2]
    left, right, here, before, level = (
        jnp.sum(share[:, a, :n] if a < 4 else share[:, 0, n:], 0, keepdims=True) for a in range(5)
    )
    here = here + keep[0:1]
    before = before + keep[1:2]
    level = level[:, :1] + keep[2:3, :1]
    pad = jnp.zeros((4, n), f32)
    a1, a2, a3 = (
        piece.astype(f32) for piece in split3(jnp.concatenate([q1, -q0, here, -before, pad], 0))
    )
    lhs = jnp.concatenate([a1, a1, a2, a2, a1, a3], 0).astype(bf16)
    G = mm(lhs, stacked(jnp.concatenate([right, left, q1, q0, pad], 0)), 0, 0)
    un = u[...] - rr[...] * G
    un = jnp.where((rows_of(un.shape) == 0) & (lanes_of(un.shape) == 0), level, un)
    qs = (qh[...], ql[...])
    half = split(dot3(un, qs))
    step = n // 4
    for part in range(4):
        cols = slice(part * step, (part + 1) * step)
        yield dot3((qs[0][:, cols], qs[1][:, cols]), half, 0, 0)


def run_field(members, *args):
    n = args[-1].shape[1]
    place = lambda: (lax.axis_index("row"), lax.axis_index("col"))
    if DIRECT:
        return jnp.concatenate(list(stage_field(*place(), members, *args)), 0)

    def kernel(*refs):
        field, rows, sem = refs[len(args) :]
        copies = []
        for part, value in enumerate(stage_field(*place(), members, *refs[: len(args)])):
            step = value.shape[0]
            span = slice(part * step, (part + 1) * step)
            rows[span, :] = value
            copies.append(pltpu.make_async_copy(rows.at[span], field.at[span], sem.at[part]))
            copies[-1].start()
        for copy in copies:
            copy.wait()

    vmem = pl.BlockSpec(memory_space=pltpu.VMEM)
    return pl.pallas_call(
        kernel,
        out_shape=jax.ShapeDtypeStruct((n, n), f32),
        in_specs=[vmem] * len(args),
        out_specs=pl.BlockSpec(memory_space=pltpu.HBM),
        scratch_shapes=[pltpu.VMEM((n, n), f32), pltpu.SemaphoreType.DMA((4,))],
        compiler_params=pltpu.CompilerParams(vmem_limit_bytes=VMEM_LIMIT),
        name="stage_field",
    )(*args)


def packed(rows):
    tail = jnp.broadcast_to(rows[4][:, :, None], rows[4].shape[:1] + (4, 128))
    return jnp.concatenate([jnp.stack(rows[:4], 1), tail], 2)


def run_stage(stage, members, outs, *args):
    if DIRECT:
        results = stage(lax.axis_index("row"), lax.axis_index("col"), members, *args)
        return [packed(v) if isinstance(v, list) else v for v in results]

    def kernel(*refs):
        r, c = lax.axis_index("row"), lax.axis_index("col")
        n = args[0].shape[-1]
        results = stage(r, c, members, *refs[: len(args)])
        for ref, value in zip(refs[len(args) :], results):
            if isinstance(value, list):
                for a, row in enumerate(value[:4]):
                    ref[:, a, :n] = row
                ref[:, :, n:] = jnp.broadcast_to(value[4][:, :, None], (members, 4, 128))
            else:
                ref[...] = value

    vmem = pl.BlockSpec(memory_space=pltpu.VMEM)
    return pl.pallas_call(
        kernel,
        out_shape=outs,
        in_specs=[vmem] * len(args),
        out_specs=[vmem] * len(outs),
        compiler_params=pltpu.CompilerParams(vmem_limit_bytes=VMEM_LIMIT),
        name=stage.__name__,
    )(*args)


def exchange(values, axis):
    return lax.all_to_all(values, axis, split_axis=0, concat_axis=0, tiled=True)


def make_body(members):
    def body(grad_x, grad_y):
        n = grad_x.shape[0]
        t = {k: jnp.asarray(v) for k, v in build_tables(n, members).items()}
        sent, near = jax.ShapeDtypeStruct, pltpu.VMEM
        edges, u, kept = run_local(members, {**t, "x": grad_x, "y": grad_y})
        strip = exchange(edges, "col")
        share, keep = run_stage(
            stage_strip, members, [sent((members, 4, n + 128), f32), near((8, n), f32)],
            strip, kept["q1"], kept["q2"], *(kept[name] for name in WAVES["y"]),
        )
        share = exchange(share, "row")
        return run_field(
            members, share, keep, u, kept["q1"], kept["q2"], kept["r"], kept["vec"]
        )

    return body


def solution(mesh):
    members = mesh.shape["row"]
    placed = (P("row", "col"), P("row", "col"))
    return jax.shard_map(
        make_body(members), mesh=mesh, in_specs=placed, out_specs=P("row", "col"), check_vma=False
    )
```

```python
import math

import jax
import jax.numpy as jnp
import numpy as np
from jax import lax
from jax.experimental import pallas as pl
from jax.experimental.pallas import tpu as pltpu
from jax.sharding import PartitionSpec as P

VMEM_LIMIT = 32 * 1024 * 1024
DIRECT = False
f32 = jnp.float32
bf16 = jnp.bfloat16


def cosine_basis(n):
    k, i = np.arange(n)[:, None], np.arange(n)[None]
    return np.sqrt(np.where(k == 0, 1, 2) / n) * np.cos(np.pi * k * (2 * i + 1) / (2 * n))


def edge_tables(n, members, freq):
    s = 2 * np.sin(freq)
    half = np.arcsinh(s / 2)
    e = np.exp(-2 * n * half)
    safe = np.where(s == 0, 1, s)
    e1 = np.where(s == 0, 0.5, e)
    th = np.tanh(np.arcsinh(safe / 2))
    one = np.where(s == 0, 0, 1)
    lead = one * th * (1 - e1 * e1)
    couple = one * e1 / (th * (1 - e1 * e1))
    return lead, e, couple


def pieces_of(value, count):
    found = []
    for _ in range(count):
        found.append(np.asarray(value, jnp.bfloat16))
        value = value - found[-1].astype(np.float64)
    return found


def stack_pieces(value):
    a1, a2, a3 = pieces_of(value, 3)
    return np.concatenate([a1, a1, a2, a2, a1, a3], 1)


def build_tables(n, members):
    total = n * members
    half = n // 2
    k = np.concatenate([np.arange(0, n, 2), np.arange(1, n, 2)])
    q = cosine_basis(n)[k]
    s = 2 * np.sin(np.pi * k / (2 * n))
    q0, q1 = q[:, 0], q[:, -1]
    lead, e, couple = edge_tables(n, members, np.pi * k / (2 * n))
    vec = np.zeros((8, n))
    vec[0], vec[1], vec[2], vec[3], vec[4] = q0, q1, lead, e, couple
    lane = np.arange(half)
    other = np.where(lane == 0, half, lane)
    d = np.arange(members)
    kap = np.concatenate(
        [
            d[:, None] + 2 * members * lane[None],
            2 * members * other[None] - np.where(d == 0, members, d)[:, None],
        ]
    )
    glob = np.stack(edge_tables(n, members, np.pi * kap / (2 * total)))
    bend = 1 + glob[1] ** 2 - 2 * glob[1] * np.cos(np.pi * np.arange(1, members) / members)[:, None, None]
    size = np.full((2 * members, half), 1 / np.sqrt(members))
    size[1:members, 0] *= np.sqrt(2)
    dens = (glob[0] * size / bend).reshape(-1, half)
    j = 2 * np.arange(n) + 1
    sb = np.sqrt(2 / n) * np.sin(np.pi * other[:, None] * j[None] / n)
    turn = np.concatenate([q[:half].T, sb.T], 0)
    sp = np.sqrt(2 / n) * s[:, None] * np.sin(np.pi * k[:, None] * (np.arange(n)[None] + 1) / n)
    sp[:, n - 1] = 0
    sp[0] = 0
    den = s[:, None] ** 2 + s[None] ** 2
    den[0, 0] = 1
    r = 1 / den
    r[0, 0] = 0
    ang = np.pi * np.arange(members + 1)[:, None] * j[None] / (2 * total)
    ca, sa = np.cos(ang), np.sin(ang)
    swap = np.concatenate([sa[members:], ca[1:members]], 0)
    acs = np.concatenate([ca[:members], sa[:members], swap, np.repeat(ca[members:], members, 0)], 0)
    p = np.arange(members)
    wang = np.pi * np.arange(members + 1)[:, None] * p[None] / members
    wc, ws = np.cos(wang), np.sin(wang)
    wfwd = np.concatenate([wc[:members], wc[members:], ws[1:members]], 0)
    winv = np.concatenate([wc[:members], wc[members:], -ws[1:members]], 0).T
    M = members
    t = np.arange(1, M)
    st = np.sqrt(2 / M) * np.sin(np.pi * np.outer(t, t) / M)
    sa, stt, s2 = np.zeros((M, M)), np.zeros((M, M)), np.zeros((M, M))
    sa[: M - 1, : M - 1] = st
    sa[: M - 1, M - 1] = st[:, M - 2]
    stt[: M - 1, 1:] = -st
    s2[: M - 1, : M - 1] = st
    a0 = (q1[1:] ** 2 / s[1:] ** 2).sum()
    b0 = (q0[1:] * q1[1:] / s[1:] ** 2).sum()
    qq = 1 / np.sqrt(n)
    pp = np.arange(M)
    frac = (pp[:, None] + 1) / M
    t1 = frac - (pp[None] <= pp[:, None])
    h15 = np.zeros((M, M))
    h15[:, M - 1] = frac[:, 0]
    hmat = np.concatenate([h15, t1], 1)
    acc = (pp[None] < pp[:, None]).astype(float)
    acc[:, M - 1] = 0
    acc = (acc - acc.mean(0)) / qq
    up = np.zeros((M, M))
    up[:-1, 1:] = np.eye(M - 1)
    keep = np.eye(M)
    keep[M - 1, M - 1] = 0
    ka = acc @ keep
    kt = -acc @ (keep @ up)
    kh = acc @ (keep @ (-(1 + 2 * a0) * np.eye(M) + b0 * up + b0 * up.T))
    s2x = s2.copy()
    s2x[M - 1, M - 1] = 1
    per = min(M, 256 // (2 * M))
    wbd = np.kron(np.eye(per), winv)
    minv = np.zeros((M, M, n))
    lean = lead / (1 + e * e - 2 * e * np.cos(np.pi * t / M)[:, None])
    minv[: M - 1, : M - 1] = np.einsum("pm,mk,mq->pqk", st, lean, st)
    mats = np.zeros((8 * M, 128))
    mats[0:M, : 2 * M] = np.concatenate([sa, stt], 1)
    mats[M : 2 * M, :M] = t1.T
    mats[2 * M : 3 * M, :M] = ka.T * qq
    mats[3 * M : 4 * M, :M] = kt.T * qq
    mats[4 * M : 5 * M, :M] = (kh @ t1).T
    step = (pp[:, None] >= pp[None]).astype(float)
    blocks = (ka, kt, s2x @ step, kh @ step, s2x @ frac, kh @ frac, frac)
    for a, block in enumerate(blocks):
        mats[5 * M : 6 * M, a * M : a * M + block.shape[1]] = block
    kmats = np.zeros((8 * M, 384), jnp.bfloat16)
    row = 0
    for small in (hmat, np.concatenate([ka, kt, kh], 1), s2, s2x, wfwd):
        stacked = stack_pieces(small)
        kmats[row : row + small.shape[0], : stacked.shape[1]] = stacked
        row += small.shape[0]
    q1, q2, q3 = pieces_of(q, 3)
    s1, s2 = pieces_of(sp, 2)
    v1, v2 = pieces_of(vec, 2)
    out = dict(
        vec=vec, r=r, col=np.repeat(q0[:, None], min(n, 128), 1), mats=mats,
        thin=np.concatenate([dens, glob[2]], 0),
        long=np.concatenate([minv.reshape(-1, n), acs], 0),
    )
    out = {name: np.asarray(value, np.float32) for name, value in out.items()}
    out.update(
        q1=q1, q2=q2, s1=s1, s2=s2, v=np.concatenate([v1, v2], 0), kmats=kmats,
        w=np.concatenate(pieces_of(wbd, 3), 0), turn=np.concatenate(pieces_of(turn, 3), 0),
        wide=np.concatenate([q3] + pieces_of(r, 3) + pieces_of(sb, 2), 0),
    )
    return out


def split(a):
    high = a.astype(bf16)
    return high, (a - high.astype(f32)).astype(bf16)


def mm(a, b, ca, cb):
    return lax.dot_general(a, b, (((ca,), (cb,)), ((), ())), preferred_element_type=f32)


def dot3s(a, b, ca=1, cb=0):
    ah, al = a if isinstance(a, tuple) else split(a)
    bh, bl = b if isinstance(b, tuple) else split(b)
    return mm(ah, bh, ca, cb) + (mm(ah, bl, ca, cb) + mm(al, bh, ca, cb))


def dot3(a, b, ca=1, cb=0):
    ah, al = a if isinstance(a, tuple) else split(a)
    bh, bl = b if isinstance(b, tuple) else split(b)
    return mm(jnp.concatenate([ah, ah, al], ca), jnp.concatenate([bh, bl, bh], cb), ca, cb)


def split3(a):
    high, rest = a.astype(bf16), None
    rest = a - high.astype(f32)
    mid = rest.astype(bf16)
    return high, mid, (rest - mid.astype(f32)).astype(bf16)


def dot6(a, b, cb=0):
    m = a.shape[0]
    a1, a2, a3 = split3(a)
    b1, b2, b3 = b
    p = mm(jnp.concatenate([a1, a2, a3], 0), b1, 1, cb)
    q = mm(jnp.concatenate([a1, a2], 0), b2, 1, cb)
    small = (p[2 * m :] + q[m:]) + mm(a1, b3, 1, cb)
    return p[:m] + ((p[m : 2 * m] + q[:m]) + small)


def dotl(a, b):
    m = a[0].shape[0]
    b1, b2, b3 = split3(b)
    p = mm(jnp.concatenate(a, 0), b1, 1, 0)
    q = mm(jnp.concatenate(a[:2], 0), b2, 1, 0)
    small = (p[2 * m :] + q[m:]) + mm(a[0], b3, 1, 0)
    return p[:m] + ((p[m : 2 * m] + q[:m]) + small)


def doths(a, qs):
    value = dot3(a, qs, 1, 1)
    exact = jnp.sum(a, 1, keepdims=True) * (1.0 / math.sqrt(a.shape[1]))
    return jnp.where(lanes_of(value.shape) == 0, exact, value)


def doth(a, b, ca=1, cb=0):
    return lax.dot_general(
        a, b, (((ca,), (cb,)), ((), ())), precision=lax.Precision.HIGHEST, preferred_element_type=f32
    )


def rows_of(shape):
    return lax.broadcasted_iota(jnp.int32, shape, 0)


def lanes_of(shape):
    return lax.broadcasted_iota(jnp.int32, shape, 1)


def pick(values, index):
    return jnp.sum(jnp.where(rows_of(values.shape) == index, values, 0.0), 0, keepdims=True)


def below(values):
    return jnp.concatenate([jnp.zeros_like(values[:1]), values[:-1]], 0)


def stacked(b):
    b1, b2, b3 = (piece.astype(f32) for piece in split3(b))
    return jnp.concatenate([b1, b2, b1, b2, b3, b1], 0).astype(bf16)


def dotk(a, b):
    return mm(a[:, : 6 * b.shape[0]], stacked(b), 1, 0)


def edge_solve(al, t0, couple, minv, mats, kmats):
    M, n = al.shape
    L = min(n, 128)
    last = rows_of((M, n)) == M - 1
    w = al - jnp.concatenate([t0[1:], t0[:1]], 0)
    H = jnp.where(last, al, 0.0)
    tail = couple * al[M - 1 :]
    for p in range(M - 1):
        wp = w[p : p + 1] + tail if p == M - 2 else w[p : p + 1]
        H = H + minv[M * p : M * (p + 1), :] * wp
    Hz = mats[5 * M : 6 * M, 6 * M : 6 * M + 1] * al[M - 1 :, :L]
    mean = dotk(kmats[M : 2 * M, :], jnp.concatenate([al[:, :L], t0[:, :L], Hz], 0))
    lane = lanes_of((M, L))
    first = jnp.where(lane == 0, Hz, H[:, :L])
    H = first if n == L else jnp.concatenate([first, H[:, L:]], 1)
    return H, mean[:, :1]


def to_peers(rows, members):
    one = jnp.concatenate(rows, 0)
    return jnp.broadcast_to(one[None], (members,) + one.shape)


def stage_local(r, c, M, wait, get):
    wait("q1", "x0", "x1", "q2")
    m1 = dot3(
        jnp.concatenate([get("x0"), get("x1")], 0), (get("q1"), get("q2")), 1, 1
    )
    wait("y", "s1", "s2", "r", "v", "col")
    n = m1.shape[0]
    half = n // 2
    L = min(n, 128)
    n2 = dot3((get("q1"), get("q2")), get("y"))
    ss = (get("s1"), get("s2"))
    f = dot3(ss, m1) + dot3(n2, ss, 1, 1)
    gyl = n2[:, n - L :].T[L - 1 :]
    u = -f * get("r")
    uh, ul = split(u)
    v = get("v")
    p = mm(v, uh, 1, 1)
    tk = p[:8] + (p[8:] + mm(v, ul, 1, 1)[:8])
    col = get("col")
    groups = []
    for rows in (slice(0, half), slice(half, n)):
        groups.append(
            jnp.concatenate(
                [
                    jnp.sum(u[rows, a : a + L] * col[rows], 0, keepdims=True)
                    for a in range(0, n, L)
                ],
                1,
            )
        )
    low, high = groups[0] + groups[1], groups[0] - groups[1]
    alpha = gyl + jnp.where(c < M - 1, tk[1:2], 0.0)
    beta = m1[n - 1 :] + jnp.where(r < M - 1, high, 0.0)
    return to_peers([alpha, tk[0:1], beta, low], M), u


WAVES = {None: ("q1", "x0", "x1", "q2", "y", "s1", "s2", "r", "v", "col")}
WAVES["y"] = ("vec", "wide", "turn", "w", "thin", "long", "mats", "kmats")
NAMES = sum(WAVES.values(), ())
KEPT = ("q1", "q2", "r") + WAVES["y"]


def run_local(members, arrays):
    n = arrays["q1"].shape[1]
    arrays["x0"], arrays["x1"] = arrays["x"][: n // 2], arrays["x"][n // 2 :]
    shapes = {name: (arrays[name].shape, arrays[name].dtype) for name in NAMES}
    if DIRECT:
        edges, u = stage_local(
            lax.axis_index("row"), lax.axis_index("col"), members, lambda *names: None,
            arrays.__getitem__,
        )
        return edges, u, {name: arrays[name] for name in KEPT}

    def kernel(*refs):
        count = len(NAMES)
        edges, u = refs[count : count + 2]
        here = dict(zip(KEPT, refs[count + 2 :]))
        here.update(zip((k for k in NAMES if k not in KEPT), refs[count + 2 + len(KEPT) :]))
        sem = refs[-1]
        def part_of(name, source):
            pick_half = {"x0": pl.ds(0, n // 2), "x1": pl.ds(n // 2, n // 2)}
            return source.at[pick_half[name]] if name in pick_half else source

        copies = {
            name: pltpu.make_async_copy(part_of(name, source), here[name], sem.at[i])
            for i, (name, source) in enumerate(zip(NAMES, refs))
        }

        def release(wave):
            for name in WAVES.get(wave, ()):
                copies[name].start()

        def wait(*names):
            for name in names:
                copies[name].wait()
                release(name)

        def get(name):
            return here[name][...]

        release(None)
        edges[...], u[...] = stage_local(
            lax.axis_index("row"), lax.axis_index("col"), members, wait, get
        )
        wait(*WAVES["y"])

    operands = [name if name not in ("x0", "x1") else "x" for name in NAMES]
    far, vmem, near = pl.BlockSpec(memory_space=pltpu.HBM), pl.BlockSpec(memory_space=pltpu.VMEM), pltpu.VMEM
    shape = {name: near(*shapes[name]) for name in NAMES}
    edges, u, *tables = pl.pallas_call(
        kernel,
        out_shape=[jax.ShapeDtypeStruct((members, 4, n), f32), near((n, n), f32)]
        + [shape[name] for name in KEPT],
        in_specs=[far] * len(NAMES),
        out_specs=[vmem] * (2 + len(KEPT)),
        scratch_shapes=[shape[name] for name in NAMES if name not in KEPT]
        + [pltpu.SemaphoreType.DMA((len(NAMES),))],
        compiler_params=pltpu.CompilerParams(vmem_limit_bytes=VMEM_LIMIT),
        name="stage_local",
    )(*(pltpu.with_memory_space_constraint(arrays[name], pltpu.HBM) for name in operands))
    return edges, u, dict(zip(KEPT, tables))


def lane_pick(values, index):
    return jnp.sum(jnp.where(lanes_of(values.shape) == index, values, 0.0), 1, keepdims=True)


def stage_strip(r, c, M, ag, q1, q2, vec, wide, turn, w, thin, long, mats, kmats):
    n = q1.shape[0]
    half = n // 2
    r1, r2, r3 = (wide[a * n : (a + 1) * n, :] for a in range(1, 4))
    b1, b2 = wide[4 * n : 4 * n + half, :], wide[4 * n + half : 5 * n, :]
    acs = long[M * M : M * M + 4 * M, :]
    al, t0, be, ta0 = (ag[:, a, :] for a in range(4))
    vec, mats = vec[...], mats[...]
    v0, v1, couple = vec[0:1], vec[1:2], vec[4:5]
    L = min(n, 128)
    qq = 1.0 / math.sqrt(n)
    sa, stt = mats[:M, :M], mats[:M, M : 2 * M]

    H, mean = edge_solve(al, t0, couple, long, mats, kmats)
    rs = (r1, r2)
    Z = dot6(jnp.concatenate([H * v0, H * v1], 0), rs + (r3,))
    add0 = v0 * below(Z[:M]) - v1 * Z[:M]
    add1 = v0 * below(Z[M:]) - v1 * Z[M:]
    flat = jnp.where(lanes_of((M, n)) == 0, mean * qq, 0.0)
    tau0 = ta0 + add0 + flat
    tau1 = be + jnp.where(r < M - 1, add1 + flat, 0.0)

    qs = (q1[...], q2[...])
    y = dot6(jnp.concatenate([tau1, tau0], 0), qs + (wide[:n, :],))
    ca, sna, swap, c16 = (acs[a * M : (a + 1) * M, :] for a in range(4))
    c16 = c16[:1]
    g = dotk(kmats[4 * M : 6 * M, :], jnp.concatenate([y[:M], y[M:]], 1))
    xs, ys, extra = [], [], []
    for side in range(2):
        C, S = (g[k * M : (k + 1) * M, side * n : (side + 1) * n] for k in range(2))
        xs.append(C * ca - S * sna)
        ys.append(C * sna + S * swap)
        extra.append(S[:1] * c16)
    xs += extra + [jnp.zeros((M - 2, n), f32)]
    cosines = tuple(turn[2 * n * a : 2 * n * a + n, :] for a in range(3))
    sines = tuple(turn[2 * n * a + n : 2 * n * (a + 1), :] for a in range(3))
    xcos = dot6(jnp.concatenate(xs, 0), cosines)
    ysin = dot6(jnp.concatenate(ys, 0), sines)
    pair = (M, half)
    left_lane, top_row = lanes_of(pair) == 0, rows_of(pair) == 0
    shape = (2 * M, half)
    origin = (rows_of(shape) == 0) & (lanes_of(shape) == 0)
    root = 1.0 / math.sqrt(M)
    wider = (lanes_of(shape) == 0) & (rows_of(shape) > 0) & (rows_of(shape) < M)
    scale = jnp.where(wider, root * math.sqrt(2.0), root)
    ends = []
    for side in range(2):
        xc, yb = xcos[side * M : (side + 1) * M], ysin[side * M : (side + 1) * M]
        plus = xc - jnp.where(left_lane | top_row, 0.0, yb)
        alone = jnp.where(top_row, xcos[2 * M + side : 2 * M + side + 1], xc)
        minus = jnp.where(left_lane, 0.0, alone) + yb
        ends.append(jnp.concatenate([plus, minus], 0) * scale)
    T1, T0 = ends

    edge = mats[5 * M : 6 * M, :]
    src = al[M - 1 :, :1] * (1.0 / math.sqrt(M))
    a15 = jnp.where(r == M - 1, T1[:1, :1], 0.0)
    kac, ktc, gstep, hstep = (lane_pick(edge[:, a * M : (a + 1) * M], r) for a in range(4))
    gfrac, hfrac = edge[:, 4 * M : 4 * M + 1], edge[:, 5 * M : 5 * M + 1]
    lift = kac * T1[:1, :1] + ktc * T0[:1, :1] + hfrac * (a15 + src) - hstep * src
    g0 = gfrac * (a15 + src) - gstep * src
    up, down = lane_pick(sa, r), lane_pick(stt, r)
    T1c = jnp.where(r == M - 1, T1 * thin[2 * M * (M - 1) :, :], T1)
    modes = []
    for m in range(M - 1):
        value = (up[m : m + 1] * T1c + down[m : m + 1] * T0) * thin[2 * M * m : 2 * M * (m + 1), :]
        modes.append(jnp.where(origin, g0[m : m + 1, :1] * root, value))
    modes.append(jnp.where(r == M - 1, T1, 0.0) * scale)
    sums, gaps, single = [], [], []
    for value in modes:
        gp, gm = value[:M], value[M:]
        sums.append(gp + jnp.where(left_lane | top_row, 0.0, gm))
        gaps.append(jnp.where(top_row, gm, jnp.where(left_lane, 0.0, gp) - gm))
        single.append(jnp.where(left_lane[:1], 0.0, gm[:1]))
    XC = dot3(split(jnp.concatenate(sums + single, 0)), (qs[0][:half], qs[1][:half]))
    XS = dot3(split(jnp.concatenate(gaps, 0)), (b1, b2))
    third = w.shape[0] // 3
    ws = tuple(w[third * a : third * (a + 1), :] for a in range(3))
    group = w.shape[1] // (2 * M)
    lines = []
    top_line = rows_of((M, n)) == 0
    for first in range(0, M, group):
        rots = []
        for m in range(first, first + group):
            xc, xs = XC[M * m : M * (m + 1)], XS[M * m : M * (m + 1)]
            alone = jnp.where(top_line, c16 * XC[M * M + m : M * M + m + 1], 0.0)
            rots += [ca * xc - sna * xs, sna * xc + swap * xs + alone]
        lines.append(dotl(ws, jnp.concatenate(rots, 0)))
    hx = doths(jnp.concatenate(lines, 0), qs)
    Y0, Y1 = [], []
    for rows in (slice(0, M * M // 2), slice(M * M // 2, M * M)):
        Y = dot3(jnp.concatenate([hx[rows] * v0, hx[rows] * v1], 0), rs)
        Y0.append(Y[: M * M // 2])
        Y1.append(Y[M * M // 2 :])
    Y0, Y1 = jnp.concatenate(Y0, 0), jnp.concatenate(Y1, 0)

    first = lanes_of((1, n)) == 0
    cols = []
    for cc in (c, c - 1):
        k1 = long[pl.ds(pl.multiple_of(jnp.maximum(cc, 0) * M, M), M), :]
        k1 = jnp.where(cc < 0, 0.0, k1)
        cols.append((k1, -below(k1), lane_pick(mats[M : 2 * M, :M], cc) * (-1.0 / qq)))
    ka, kt = lane_pick(mats[2 * M : 3 * M, :M], c), lane_pick(mats[3 * M : 4 * M, :M], c)
    kth = lane_pick(mats[4 * M : 5 * M, :M], c)
    here, side_c, side_b, level = [], [], [], []
    for m in range(M):
        rows = slice(M * m, M * (m + 1))
        hm, y0, y1 = hx[rows], Y0[rows], Y1[rows]
        here.append(pick(hm, c))
        for (k1, k2, ksrc), sides in zip(cols, (side_c, side_b)):
            phi = jnp.sum(k1 * y1 + k2 * y0, 0, keepdims=True)
            z = jnp.sum(ksrc * hm, 0, keepdims=True)
            sides.append(jnp.where(first, z, phi))
        level.append(
            jnp.sum(kth * hm[:, :L] - ka * y1[:, :L] - kt * y0[:, :L], 0, keepdims=True)
        )
    rows = [jnp.concatenate(v, 0) for v in (here, side_c, side_b, level)]
    mixed = dotk(kmats[3 * M : 4 * M, :], jnp.concatenate(rows, 1))
    mixed = [mixed[:, a * n : (a + 1) * n] for a in range(4)]
    right, fc, fb, lv = mixed
    lv = (lv - below(lv) + lift * (1.0 / math.sqrt(M)))[:, :1]
    share = [
        below(right),
        right,
        v0 * below(fc) - v1 * fc,
        v0 * below(fb) - v1 * fb,
        lv,
    ]
    keep = [pick(H, c), pick(H, c - 1), jnp.broadcast_to(pick(mean, c), (1, n))]
    return share, jnp.concatenate(keep + [jnp.zeros((5, n), f32)], 0)


def stage_field(r, c, M, share, keep, u, qh, ql, rr, vec):
    keep, vec = keep[...], vec[...]
    n = vec.shape[1]
    q0, q1 = vec[0:1], vec[1:2]
    left, right, here, before, level = (
        jnp.sum(share[:, a, :n] if a < 4 else share[:, 0, n:], 0, keepdims=True) for a in range(5)
    )
    here = here + keep[0:1]
    before = before + keep[1:2]
    level = level[:, :1] + keep[2:3, :1]
    pad = jnp.zeros((4, n), f32)
    a1, a2, a3 = (
        piece.astype(f32) for piece in split3(jnp.concatenate([q1, -q0, here, -before, pad], 0))
    )
    lhs = jnp.concatenate([a1, a1, a2, a2, a1, a3], 0).astype(bf16)
    G = mm(lhs, stacked(jnp.concatenate([right, left, q1, q0, pad], 0)), 0, 0)
    un = u[...] - rr[...] * G
    un = jnp.where((rows_of(un.shape) == 0) & (lanes_of(un.shape) == 0), level, un)
    qs = (qh[...], ql[...])
    half = split(dot3(un, qs))
    step = n // 4
    for part in range(4):
        cols = slice(part * step, (part + 1) * step)
        yield dot3((qs[0][:, cols], qs[1][:, cols]), half, 0, 0)


def run_field(members, *args):
    n = args[-1].shape[1]
    place = lambda: (lax.axis_index("row"), lax.axis_index("col"))
    if DIRECT:
        return jnp.concatenate(list(stage_field(*place(), members, *args)), 0)

    def kernel(*refs):
        field, rows, sem = refs[len(args) :]
        copies = []
        for part, value in enumerate(stage_field(*place(), members, *refs[: len(args)])):
            step = value.shape[0]
            span = slice(part * step, (part + 1) * step)
            rows[span, :] = value
            copies.append(pltpu.make_async_copy(rows.at[span], field.at[span], sem.at[part]))
            copies[-1].start()
        for copy in copies:
            copy.wait()

    vmem = pl.BlockSpec(memory_space=pltpu.VMEM)
    return pl.pallas_call(
        kernel,
        out_shape=jax.ShapeDtypeStruct((n, n), f32),
        in_specs=[vmem] * len(args),
        out_specs=pl.BlockSpec(memory_space=pltpu.HBM),
        scratch_shapes=[pltpu.VMEM((n, n), f32), pltpu.SemaphoreType.DMA((4,))],
        compiler_params=pltpu.CompilerParams(vmem_limit_bytes=VMEM_LIMIT),
        name="stage_field",
    )(*args)


def packed(rows):
    tail = jnp.broadcast_to(rows[4][:, :, None], rows[4].shape[:1] + (4, 128))
    return jnp.concatenate([jnp.stack(rows[:4], 1), tail], 2)


def run_stage(stage, members, outs, *args):
    if DIRECT:
        results = stage(lax.axis_index("row"), lax.axis_index("col"), members, *args)
        return [packed(v) if isinstance(v, list) else v for v in results]

    def kernel(*refs):
        r, c = lax.axis_index("row"), lax.axis_index("col")
        n = args[0].shape[-1]
        results = stage(r, c, members, *refs[: len(args)])
        for ref, value in zip(refs[len(args) :], results):
            if isinstance(value, list):
                for a, row in enumerate(value[:4]):
                    ref[:, a, :n] = row
                ref[:, :, n:] = jnp.broadcast_to(value[4][:, :, None], (members, 4, 128))
            else:
                ref[...] = value

    vmem = pl.BlockSpec(memory_space=pltpu.VMEM)
    return pl.pallas_call(
        kernel,
        out_shape=outs,
        in_specs=[vmem] * len(args),
        out_specs=[vmem] * len(outs),
        compiler_params=pltpu.CompilerParams(vmem_limit_bytes=VMEM_LIMIT),
        name=stage.__name__,
    )(*args)


def exchange(values, axis):
    return lax.all_to_all(values, axis, split_axis=0, concat_axis=0, tiled=True)


def make_body(members):
    def body(grad_x, grad_y):
        n = grad_x.shape[0]
        t = {k: jnp.asarray(v) for k, v in build_tables(n, members).items()}
        sent, near = jax.ShapeDtypeStruct, pltpu.VMEM
        edges, u, kept = run_local(members, {**t, "x": grad_x, "y": grad_y})
        strip = exchange(edges, "col")
        share, keep = run_stage(
            stage_strip, members, [sent((members, 4, n + 128), f32), near((8, n), f32)],
            strip, kept["q1"], kept["q2"], *(kept[name] for name in WAVES["y"]),
        )
        share = exchange(share, "row")
        return run_field(
            members, share, keep, u, kept["q1"], kept["q2"], kept["r"], kept["vec"]
        )

    return body


def solution(mesh):
    members = mesh.shape["row"]
    placed = (P("row", "col"), P("row", "col"))
    return jax.shard_map(
        make_body(members), mesh=mesh, in_specs=placed, out_specs=P("row", "col"), check_vma=False
    )
```

```python
import math

import jax
import jax.numpy as jnp
import numpy as np
from jax import lax
from jax.experimental import pallas as pl
from jax.experimental.pallas import tpu as pltpu
from jax.sharding import PartitionSpec as P

VMEM_LIMIT = 32 * 1024 * 1024
DIRECT = False
f32 = jnp.float32
bf16 = jnp.bfloat16


def cosine_basis(n):
    k, i = np.arange(n)[:, None], np.arange(n)[None]
    return np.sqrt(np.where(k == 0, 1, 2) / n) * np.cos(np.pi * k * (2 * i + 1) / (2 * n))


def edge_tables(n, members, freq):
    s = 2 * np.sin(freq)
    half = np.arcsinh(s / 2)
    e = np.exp(-2 * n * half)
    safe = np.where(s == 0, 1, s)
    e1 = np.where(s == 0, 0.5, e)
    th = np.tanh(np.arcsinh(safe / 2))
    one = np.where(s == 0, 0, 1)
    lead = one * th * (1 - e1 * e1)
    couple = one * e1 / (th * (1 - e1 * e1))
    return lead, e, couple


def pieces_of(value, count):
    found = []
    for _ in range(count):
        found.append(np.asarray(value, jnp.bfloat16))
        value = value - found[-1].astype(np.float64)
    return found


def stack_pieces(value):
    a1, a2, a3 = pieces_of(value, 3)
    return np.concatenate([a1, a1, a2, a2, a1, a3], 1)


def build_tables(n, members):
    total = n * members
    half = n // 2
    k = np.concatenate([np.arange(0, n, 2), np.arange(1, n, 2)])
    q = cosine_basis(n)[k]
    s = 2 * np.sin(np.pi * k / (2 * n))
    q0, q1 = q[:, 0], q[:, -1]
    lead, e, couple = edge_tables(n, members, np.pi * k / (2 * n))
    vec = np.zeros((8, n))
    vec[0], vec[1], vec[2], vec[3], vec[4] = q0, q1, lead, e, couple
    lane = np.arange(half)
    other = np.where(lane == 0, half, lane)
    d = np.arange(members)
    kap = np.concatenate(
        [
            d[:, None] + 2 * members * lane[None],
            2 * members * other[None] - np.where(d == 0, members, d)[:, None],
        ]
    )
    glob = np.stack(edge_tables(n, members, np.pi * kap / (2 * total)))
    bend = 1 + glob[1] ** 2 - 2 * glob[1] * np.cos(np.pi * np.arange(1, members) / members)[:, None, None]
    size = np.full((2 * members, half), 1 / np.sqrt(members))
    size[1:members, 0] *= np.sqrt(2)
    dens = (glob[0] * size / bend).reshape(-1, half)
    j = 2 * np.arange(n) + 1
    sb = np.sqrt(2 / n) * np.sin(np.pi * other[:, None] * j[None] / n)
    turn = np.concatenate([q[:half].T, sb.T], 0)
    sp = np.sqrt(2 / n) * s[:, None] * np.sin(np.pi * k[:, None] * (np.arange(n)[None] + 1) / n)
    sp[:, n - 1] = 0
    sp[0] = 0
    den = s[:, None] ** 2 + s[None] ** 2
    den[0, 0] = 1
    r = 1 / den
    r[0, 0] = 0
    ang = np.pi * np.arange(members + 1)[:, None] * j[None] / (2 * total)
    ca, sa = np.cos(ang), np.sin(ang)
    swap = np.concatenate([sa[members:], ca[1:members]], 0)
    acs = np.concatenate([ca[:members], sa[:members], swap, np.repeat(ca[members:], members, 0)], 0)
    p = np.arange(members)
    wang = np.pi * np.arange(members + 1)[:, None] * p[None] / members
    wc, ws = np.cos(wang), np.sin(wang)
    wfwd = np.concatenate([wc[:members], wc[members:], ws[1:members]], 0)
    winv = np.concatenate([wc[:members], wc[members:], -ws[1:members]], 0).T
    M = members
    t = np.arange(1, M)
    st = np.sqrt(2 / M) * np.sin(np.pi * np.outer(t, t) / M)
    sa, stt, s2 = np.zeros((M, M)), np.zeros((M, M)), np.zeros((M, M))
    sa[: M - 1, : M - 1] = st
    sa[: M - 1, M - 1] = st[:, M - 2]
    stt[: M - 1, 1:] = -st
    s2[: M - 1, : M - 1] = st
    a0 = (q1[1:] ** 2 / s[1:] ** 2).sum()
    b0 = (q0[1:] * q1[1:] / s[1:] ** 2).sum()
    qq = 1 / np.sqrt(n)
    pp = np.arange(M)
    frac = (pp[:, None] + 1) / M
    t1 = frac - (pp[None] <= pp[:, None])
    h15 = np.zeros((M, M))
    h15[:, M - 1] = frac[:, 0]
    hmat = np.concatenate([h15, t1], 1)
    acc = (pp[None] < pp[:, None]).astype(float)
    acc[:, M - 1] = 0
    acc = (acc - acc.mean(0)) / qq
    up = np.zeros((M, M))
    up[:-1, 1:] = np.eye(M - 1)
    keep = np.eye(M)
    keep[M - 1, M - 1] = 0
    ka = acc @ keep
    kt = -acc @ (keep @ up)
    kh = acc @ (keep @ (-(1 + 2 * a0) * np.eye(M) + b0 * up + b0 * up.T))
    s2x = s2.copy()
    s2x[M - 1, M - 1] = 1
    per = min(M, 256 // (2 * M))
    wbd = np.kron(np.eye(per), winv)
    minv = np.zeros((M, M, n))
    lean = lead / (1 + e * e - 2 * e * np.cos(np.pi * t / M)[:, None])
    minv[: M - 1, : M - 1] = np.einsum("pm,mk,mq->pqk", st, lean, st)
    mats = np.zeros((8 * M, 128))
    mats[0:M, : 2 * M] = np.concatenate([sa, stt], 1)
    mats[M : 2 * M, :M] = t1.T
    mats[2 * M : 3 * M, :M] = ka.T * qq
    mats[3 * M : 4 * M, :M] = kt.T * qq
    mats[4 * M : 5 * M, :M] = (kh @ t1).T
    step = (pp[:, None] >= pp[None]).astype(float)
    blocks = (ka, kt, s2x @ step, kh @ step, s2x @ frac, kh @ frac, frac)
    for a, block in enumerate(blocks):
        mats[5 * M : 6 * M, a * M : a * M + block.shape[1]] = block
    kmats = np.zeros((8 * M, 384), jnp.bfloat16)
    row = 0
    for small in (hmat, np.concatenate([ka, kt, kh], 1), s2, s2x, wfwd):
        stacked = stack_pieces(small)
        kmats[row : row + small.shape[0], : stacked.shape[1]] = stacked
        row += small.shape[0]
    q1, q2, q3 = pieces_of(q, 3)
    s1, s2 = pieces_of(sp, 2)
    v1, v2 = pieces_of(vec, 2)
    out = dict(
        vec=vec, r=r, col=np.repeat(q0[:, None], min(n, 128), 1), mats=mats,
        thin=np.concatenate([dens, glob[2]], 0),
        long=np.concatenate([minv.reshape(-1, n), acs], 0),
    )
    out = {name: np.asarray(value, np.float32) for name, value in out.items()}
    out.update(
        q1=q1, q2=q2, s1=s1, s2=s2, v=np.concatenate([v1, v2], 0), kmats=kmats,
        w=np.concatenate(pieces_of(wbd, 3), 0), turn=np.concatenate(pieces_of(turn, 3), 0),
        wide=np.concatenate([q3] + pieces_of(r, 3) + pieces_of(sb, 2), 0),
    )
    return out


def split(a):
    high = a.astype(bf16)
    return high, (a - high.astype(f32)).astype(bf16)


def mm(a, b, ca, cb):
    return lax.dot_general(a, b, (((ca,), (cb,)), ((), ())), preferred_element_type=f32)


def dot3s(a, b, ca=1, cb=0):
    ah, al = a if isinstance(a, tuple) else split(a)
    bh, bl = b if isinstance(b, tuple) else split(b)
    return mm(ah, bh, ca, cb) + (mm(ah, bl, ca, cb) + mm(al, bh, ca, cb))


def dot3(a, b, ca=1, cb=0):
    ah, al = a if isinstance(a, tuple) else split(a)
    bh, bl = b if isinstance(b, tuple) else split(b)
    return mm(jnp.concatenate([ah, ah, al], ca), jnp.concatenate([bh, bl, bh], cb), ca, cb)


def split3(a):
    high, rest = a.astype(bf16), None
    rest = a - high.astype(f32)
    mid = rest.astype(bf16)
    return high, mid, (rest - mid.astype(f32)).astype(bf16)


def dot6(a, b, cb=0):
    m = a.shape[0]
    a1, a2, a3 = split3(a)
    b1, b2, b3 = b
    p = mm(jnp.concatenate([a1, a2, a3], 0), b1, 1, cb)
    q = mm(jnp.concatenate([a1, a2], 0), b2, 1, cb)
    small = (p[2 * m :] + q[m:]) + mm(a1, b3, 1, cb)
    return p[:m] + ((p[m : 2 * m] + q[:m]) + small)


def dotl(a, b):
    m = a[0].shape[0]
    b1, b2, b3 = split3(b)
    p = mm(jnp.concatenate(a, 0), b1, 1, 0)
    q = mm(jnp.concatenate(a[:2], 0), b2, 1, 0)
    small = (p[2 * m :] + q[m:]) + mm(a[0], b3, 1, 0)
    return p[:m] + ((p[m : 2 * m] + q[:m]) + small)


def doths(a, qs):
    value = dot3(a, qs, 1, 1)
    exact = jnp.sum(a, 1, keepdims=True) * (1.0 / math.sqrt(a.shape[1]))
    return jnp.where(lanes_of(value.shape) == 0, exact, value)


def doth(a, b, ca=1, cb=0):
    return lax.dot_general(
        a, b, (((ca,), (cb,)), ((), ())), precision=lax.Precision.HIGHEST, preferred_element_type=f32
    )


def rows_of(shape):
    return lax.broadcasted_iota(jnp.int32, shape, 0)


def lanes_of(shape):
    return lax.broadcasted_iota(jnp.int32, shape, 1)


def pick(values, index):
    return jnp.sum(jnp.where(rows_of(values.shape) == index, values, 0.0), 0, keepdims=True)


def below(values):
    return jnp.concatenate([jnp.zeros_like(values[:1]), values[:-1]], 0)


def stacked(b):
    b1, b2, b3 = (piece.astype(f32) for piece in split3(b))
    return jnp.concatenate([b1, b2, b1, b2, b3, b1], 0).astype(bf16)


def dotk(a, b):
    return mm(a[:, : 6 * b.shape[0]], stacked(b), 1, 0)


def edge_solve(al, t0, couple, minv, mats, kmats):
    M, n = al.shape
    L = min(n, 128)
    last = rows_of((M, n)) == M - 1
    w = al - jnp.concatenate([t0[1:], t0[:1]], 0)
    H = jnp.where(last, al, 0.0)
    tail = couple * al[M - 1 :]
    for p in range(M - 1):
        wp = w[p : p + 1] + tail if p == M - 2 else w[p : p + 1]
        H = H + minv[M * p : M * (p + 1), :] * wp
    Hz = mats[5 * M : 6 * M, 6 * M : 6 * M + 1] * al[M - 1 :, :L]
    mean = dotk(kmats[M : 2 * M, :], jnp.concatenate([al[:, :L], t0[:, :L], Hz], 0))
    lane = lanes_of((M, L))
    first = jnp.where(lane == 0, Hz, H[:, :L])
    H = first if n == L else jnp.concatenate([first, H[:, L:]], 1)
    return H, mean[:, :1]


def to_peers(rows, members):
    one = jnp.concatenate(rows, 0)
    return jnp.broadcast_to(one[None], (members,) + one.shape)


def stage_local(r, c, M, wait, get):
    wait("q1", "x0", "x1", "q2")
    m1 = dot3(
        jnp.concatenate([get("x0"), get("x1")], 0), (get("q1"), get("q2")), 1, 1
    )
    wait("y", "s1", "s2", "r", "v", "col")
    n = m1.shape[0]
    half = n // 2
    L = min(n, 128)
    n2 = dot3((get("q1"), get("q2")), get("y"))
    ss = (get("s1"), get("s2"))
    f = dot3(ss, m1) + dot3(n2, ss, 1, 1)
    gyl = n2[:, n - L :].T[L - 1 :]
    u = -f * get("r")
    uh, ul = split(u)
    v = get("v")
    p = mm(v, uh, 1, 1)
    tk = p[:8] + (p[8:] + mm(v, ul, 1, 1)[:8])
    col = get("col")
    groups = []
    for rows in (slice(0, half), slice(half, n)):
        groups.append(
            jnp.concatenate(
                [
                    jnp.sum(u[rows, a : a + L] * col[rows], 0, keepdims=True)
                    for a in range(0, n, L)
                ],
                1,
            )
        )
    low, high = groups[0] + groups[1], groups[0] - groups[1]
    alpha = gyl + jnp.where(c < M - 1, tk[1:2], 0.0)
    beta = m1[n - 1 :] + jnp.where(r < M - 1, high, 0.0)
    return to_peers([alpha, tk[0:1], beta, low], M), u


WAVES = {None: ("q1", "x0", "x1", "q2", "y", "s1", "s2", "r", "v", "col")}
WAVES["y"] = ("vec", "wide", "turn", "w", "thin", "long", "mats", "kmats")
NAMES = sum(WAVES.values(), ())
KEPT = ("q1", "q2", "r") + WAVES["y"]


def run_local(members, arrays):
    n = arrays["q1"].shape[1]
    arrays["x0"], arrays["x1"] = arrays["x"][: n // 2], arrays["x"][n // 2 :]
    shapes = {name: (arrays[name].shape, arrays[name].dtype) for name in NAMES}
    if DIRECT:
        edges, u = stage_local(
            lax.axis_index("row"), lax.axis_index("col"), members, lambda *names: None,
            arrays.__getitem__,
        )
        return edges, u, {name: arrays[name] for name in KEPT}

    def kernel(*refs):
        count = len(NAMES)
        edges, u = refs[count : count + 2]
        here = dict(zip(KEPT, refs[count + 2 :]))
        here.update(zip((k for k in NAMES if k not in KEPT), refs[count + 2 + len(KEPT) :]))
        sem = refs[-1]
        def part_of(name, source):
            pick_half = {"x0": pl.ds(0, n // 2), "x1": pl.ds(n // 2, n // 2)}
            return source.at[pick_half[name]] if name in pick_half else source

        copies = {
            name: pltpu.make_async_copy(part_of(name, source), here[name], sem.at[i])
            for i, (name, source) in enumerate(zip(NAMES, refs))
        }

        def release(wave):
            for name in WAVES.get(wave, ()):
                copies[name].start()

        def wait(*names):
            for name in names:
                copies[name].wait()
                release(name)

        def get(name):
            return here[name][...]

        release(None)
        edges[...], u[...] = stage_local(
            lax.axis_index("row"), lax.axis_index("col"), members, wait, get
        )
        wait(*WAVES["y"])

    operands = [name if name not in ("x0", "x1") else "x" for name in NAMES]
    far, vmem, near = pl.BlockSpec(memory_space=pltpu.HBM), pl.BlockSpec(memory_space=pltpu.VMEM), pltpu.VMEM
    shape = {name: near(*shapes[name]) for name in NAMES}
    edges, u, *tables = pl.pallas_call(
        kernel,
        out_shape=[jax.ShapeDtypeStruct((members, 4, n), f32), near((n, n), f32)]
        + [shape[name] for name in KEPT],
        in_specs=[far] * len(NAMES),
        out_specs=[vmem] * (2 + len(KEPT)),
        scratch_shapes=[shape[name] for name in NAMES if name not in KEPT]
        + [pltpu.SemaphoreType.DMA((len(NAMES),))],
        compiler_params=pltpu.CompilerParams(vmem_limit_bytes=VMEM_LIMIT),
        name="stage_local",
    )(*(pltpu.with_memory_space_constraint(arrays[name], pltpu.HBM) for name in operands))
    return edges, u, dict(zip(KEPT, tables))


def lane_pick(values, index):
    return jnp.sum(jnp.where(lanes_of(values.shape) == index, values, 0.0), 1, keepdims=True)


def stage_strip(r, c, M, ag, q1, q2, vec, wide, turn, w, thin, long, mats, kmats):
    n = q1.shape[0]
    half = n // 2
    r1, r2, r3 = (wide[a * n : (a + 1) * n, :] for a in range(1, 4))
    b1, b2 = wide[4 * n : 4 * n + half, :], wide[4 * n + half : 5 * n, :]
    acs = long[M * M : M * M + 4 * M, :]
    al, t0, be, ta0 = (ag[:, a, :] for a in range(4))
    vec, mats = vec[...], mats[...]
    v0, v1, couple = vec[0:1], vec[1:2], vec[4:5]
    L = min(n, 128)
    qq = 1.0 / math.sqrt(n)
    sa, stt = mats[:M, :M], mats[:M, M : 2 * M]

    H, mean = edge_solve(al, t0, couple, long, mats, kmats)
    rs = (r1, r2)
    Z = dot6(jnp.concatenate([H * v0, H * v1], 0), rs + (r3,))
    add0 = v0 * below(Z[:M]) - v1 * Z[:M]
    add1 = v0 * below(Z[M:]) - v1 * Z[M:]
    flat = jnp.where(lanes_of((M, n)) == 0, mean * qq, 0.0)
    tau0 = ta0 + add0 + flat
    tau1 = be + jnp.where(r < M - 1, add1 + flat, 0.0)

    qs = (q1[...], q2[...])
    y = dot6(jnp.concatenate([tau1, tau0], 0), qs + (wide[:n, :],))
    ca, sna, swap, c16 = (acs[a * M : (a + 1) * M, :] for a in range(4))
    c16 = c16[:1]
    g = dotk(kmats[4 * M : 6 * M, :], jnp.concatenate([y[:M], y[M:]], 1))
    xs, ys, extra = [], [], []
    for side in range(2):
        C, S = (g[k * M : (k + 1) * M, side * n : (side + 1) * n] for k in range(2))
        xs.append(C * ca - S * sna)
        ys.append(C * sna + S * swap)
        extra.append(S[:1] * c16)
    xs += extra + [jnp.zeros((M - 2, n), f32)]
    cosines = tuple(turn[2 * n * a : 2 * n * a + n, :] for a in range(3))
    sines = tuple(turn[2 * n * a + n : 2 * n * (a + 1), :] for a in range(3))
    xcos = dot6(jnp.concatenate(xs, 0), cosines)
    ysin = dot6(jnp.concatenate(ys, 0), sines)
    pair = (M, half)
    left_lane, top_row = lanes_of(pair) == 0, rows_of(pair) == 0
    shape = (2 * M, half)
    origin = (rows_of(shape) == 0) & (lanes_of(shape) == 0)
    root = 1.0 / math.sqrt(M)
    wider = (lanes_of(shape) == 0) & (rows_of(shape) > 0) & (rows_of(shape) < M)
    scale = jnp.where(wider, root * math.sqrt(2.0), root)
    ends = []
    for side in range(2):
        xc, yb = xcos[side * M : (side + 1) * M], ysin[side * M : (side + 1) * M]
        plus = xc - jnp.where(left_lane | top_row, 0.0, yb)
        alone = jnp.where(top_row, xcos[2 * M + side : 2 * M + side + 1], xc)
        minus = jnp.where(left_lane, 0.0, alone) + yb
        ends.append(jnp.concatenate([plus, minus], 0) * scale)
    T1, T0 = ends

    edge = mats[5 * M : 6 * M, :]
    src = al[M - 1 :, :1] * (1.0 / math.sqrt(M))
    a15 = jnp.where(r == M - 1, T1[:1, :1], 0.0)
    kac, ktc, gstep, hstep = (lane_pick(edge[:, a * M : (a + 1) * M], r) for a in range(4))
    gfrac, hfrac = edge[:, 4 * M : 4 * M + 1], edge[:, 5 * M : 5 * M + 1]
    lift = kac * T1[:1, :1] + ktc * T0[:1, :1] + hfrac * (a15 + src) - hstep * src
    g0 = gfrac * (a15 + src) - gstep * src
    up, down = lane_pick(sa, r), lane_pick(stt, r)
    T1c = jnp.where(r == M - 1, T1 * thin[2 * M * (M - 1) :, :], T1)
    modes = []
    for m in range(M - 1):
        value = (up[m : m + 1] * T1c + down[m : m + 1] * T0) * thin[2 * M * m : 2 * M * (m + 1), :]
        modes.append(jnp.where(origin, g0[m : m + 1, :1] * root, value))
    modes.append(jnp.where(r == M - 1, T1, 0.0) * scale)
    sums, gaps, single = [], [], []
    for value in modes:
        gp, gm = value[:M], value[M:]
        sums.append(gp + jnp.where(left_lane | top_row, 0.0, gm))
        gaps.append(jnp.where(top_row, gm, jnp.where(left_lane, 0.0, gp) - gm))
        single.append(jnp.where(left_lane[:1], 0.0, gm[:1]))
    XC = dot3(split(jnp.concatenate(sums + single, 0)), (qs[0][:half], qs[1][:half]))
    XS = dot3(split(jnp.concatenate(gaps, 0)), (b1, b2))
    third = w.shape[0] // 3
    ws = tuple(w[third * a : third * (a + 1), :] for a in range(3))
    group = w.shape[1] // (2 * M)
    lines = []
    top_line = rows_of((M, n)) == 0
    for first in range(0, M, group):
        rots = []
        for m in range(first, first + group):
            xc, xs = XC[M * m : M * (m + 1)], XS[M * m : M * (m + 1)]
            alone = jnp.where(top_line, c16 * XC[M * M + m : M * M + m + 1], 0.0)
            rots += [ca * xc - sna * xs, sna * xc + swap * xs + alone]
        lines.append(dotl(ws, jnp.concatenate(rots, 0)))
    hx = doths(jnp.concatenate(lines, 0), qs)
    Y0, Y1 = [], []
    for rows in (slice(0, M * M // 2), slice(M * M // 2, M * M)):
        Y = dot3(jnp.concatenate([hx[rows] * v0, hx[rows] * v1], 0), rs)
        Y0.append(Y[: M * M // 2])
        Y1.append(Y[M * M // 2 :])
    Y0, Y1 = jnp.concatenate(Y0, 0), jnp.concatenate(Y1, 0)

    first = lanes_of((1, n)) == 0
    cols = []
    for cc in (c, c - 1):
        k1 = long[pl.ds(pl.multiple_of(jnp.maximum(cc, 0) * M, M), M), :]
        k1 = jnp.where(cc < 0, 0.0, k1)
        cols.append((k1, -below(k1), lane_pick(mats[M : 2 * M, :M], cc) * (-1.0 / qq)))
    ka, kt = lane_pick(mats[2 * M : 3 * M, :M], c), lane_pick(mats[3 * M : 4 * M, :M], c)
    kth = lane_pick(mats[4 * M : 5 * M, :M], c)
    here, side_c, side_b, level = [], [], [], []
    for m in range(M):
        rows = slice(M * m, M * (m + 1))
        hm, y0, y1 = hx[rows], Y0[rows], Y1[rows]
        here.append(pick(hm, c))
        for (k1, k2, ksrc), sides in zip(cols, (side_c, side_b)):
            phi = jnp.sum(k1 * y1 + k2 * y0, 0, keepdims=True)
            z = jnp.sum(ksrc * hm, 0, keepdims=True)
            sides.append(jnp.where(first, z, phi))
        level.append(
            jnp.sum(kth * hm[:, :L] - ka * y1[:, :L] - kt * y0[:, :L], 0, keepdims=True)
        )
    rows = [jnp.concatenate(v, 0) for v in (here, side_c, side_b, level)]
    mixed = dotk(kmats[3 * M : 4 * M, :], jnp.concatenate(rows, 1))
    mixed = [mixed[:, a * n : (a + 1) * n] for a in range(4)]
    right, fc, fb, lv = mixed
    lv = (lv - below(lv) + lift * (1.0 / math.sqrt(M)))[:, :1]
    share = [
        below(right),
        right,
        v0 * below(fc) - v1 * fc,
        v0 * below(fb) - v1 * fb,
        lv,
    ]
    keep = [pick(H, c), pick(H, c - 1), jnp.broadcast_to(pick(mean, c), (1, n))]
    return share, jnp.concatenate(keep + [jnp.zeros((5, n), f32)], 0)


CUTS = (0, 6, 8)


def stage_field(r, c, M, share, keep, u, qh, ql, rr, vec):
    keep, vec = keep[...], vec[...]
    n = vec.shape[1]
    q0, q1 = vec[0:1], vec[1:2]
    left, right, here, before, level = (
        jnp.sum(share[:, a, :n] if a < 4 else share[:, 0, n:], 0, keepdims=True) for a in range(5)
    )
    here = here + keep[0:1]
    before = before + keep[1:2]
    level = level[:, :1] + keep[2:3, :1]
    pad = jnp.zeros((4, n), f32)
    a1, a2, a3 = (
        piece.astype(f32) for piece in split3(jnp.concatenate([q1, -q0, here, -before, pad], 0))
    )
    lhs = jnp.concatenate([a1, a1, a2, a2, a1, a3], 0).astype(bf16)
    G = mm(lhs, stacked(jnp.concatenate([right, left, q1, q0, pad], 0)), 0, 0)
    un = u[...] - rr[...] * G
    un = jnp.where((rows_of(un.shape) == 0) & (lanes_of(un.shape) == 0), level, un)
    qs = (qh[...], ql[...])
    half = split(dot3(un, qs))
    for first, last in zip(CUTS, CUTS[1:]):
        cols = slice(first * n // 8, last * n // 8)
        yield dot3((qs[0][:, cols], qs[1][:, cols]), half, 0, 0)


def run_field(members, *args):
    n = args[-1].shape[1]
    place = lambda: (lax.axis_index("row"), lax.axis_index("col"))
    if DIRECT:
        return jnp.concatenate(list(stage_field(*place(), members, *args)), 0)

    def kernel(*refs):
        field, rows, sem = refs[len(args) :]
        copies = []
        for part, value in enumerate(stage_field(*place(), members, *refs[: len(args)])):
            span = slice(CUTS[part] * n // 8, CUTS[part + 1] * n // 8)
            rows[span, :] = value
            copies.append(pltpu.make_async_copy(rows.at[span], field.at[span], sem.at[part]))
            copies[-1].start()
        for copy in copies:
            copy.wait()

    vmem = pl.BlockSpec(memory_space=pltpu.VMEM)
    return pl.pallas_call(
        kernel,
        out_shape=jax.ShapeDtypeStruct((n, n), f32),
        in_specs=[vmem] * len(args),
        out_specs=pl.BlockSpec(memory_space=pltpu.HBM),
        scratch_shapes=[pltpu.VMEM((n, n), f32), pltpu.SemaphoreType.DMA((len(CUTS) - 1,))],
        compiler_params=pltpu.CompilerParams(vmem_limit_bytes=VMEM_LIMIT),
        name="stage_field",
    )(*args)


def packed(rows):
    tail = jnp.broadcast_to(rows[4][:, :, None], rows[4].shape[:1] + (4, 128))
    return jnp.concatenate([jnp.stack(rows[:4], 1), tail], 2)


def run_stage(stage, members, outs, *args):
    if DIRECT:
        results = stage(lax.axis_index("row"), lax.axis_index("col"), members, *args)
        return [packed(v) if isinstance(v, list) else v for v in results]

    def kernel(*refs):
        r, c = lax.axis_index("row"), lax.axis_index("col")
        n = args[0].shape[-1]
        results = stage(r, c, members, *refs[: len(args)])
        for ref, value in zip(refs[len(args) :], results):
            if isinstance(value, list):
                for a, row in enumerate(value[:4]):
                    ref[:, a, :n] = row
                ref[:, :, n:] = jnp.broadcast_to(value[4][:, :, None], (members, 4, 128))
            else:
                ref[...] = value

    vmem = pl.BlockSpec(memory_space=pltpu.VMEM)
    return pl.pallas_call(
        kernel,
        out_shape=outs,
        in_specs=[vmem] * len(args),
        out_specs=[vmem] * len(outs),
        compiler_params=pltpu.CompilerParams(vmem_limit_bytes=VMEM_LIMIT),
        name=stage.__name__,
    )(*args)


def exchange(values, axis):
    return lax.all_to_all(values, axis, split_axis=0, concat_axis=0, tiled=True)


def make_body(members):
    def body(grad_x, grad_y):
        n = grad_x.shape[0]
        t = {k: jnp.asarray(v) for k, v in build_tables(n, members).items()}
        sent, near = jax.ShapeDtypeStruct, pltpu.VMEM
        edges, u, kept = run_local(members, {**t, "x": grad_x, "y": grad_y})
        strip = exchange(edges, "col")
        share, keep = run_stage(
            stage_strip, members, [sent((members, 4, n + 128), f32), near((8, n), f32)],
            strip, kept["q1"], kept["q2"], *(kept[name] for name in WAVES["y"]),
        )
        share = exchange(share, "row")
        return run_field(
            members, share, keep, u, kept["q1"], kept["q2"], kept["r"], kept["vec"]
        )

    return body


def solution(mesh):
    members = mesh.shape["row"]
    placed = (P("row", "col"), P("row", "col"))
    return jax.shard_map(
        make_body(members), mesh=mesh, in_specs=placed, out_specs=P("row", "col"), check_vma=False
    )
```

```python
import math

import jax
import jax.numpy as jnp
import numpy as np
from jax import lax
from jax.experimental import pallas as pl
from jax.experimental.pallas import tpu as pltpu
from jax.sharding import PartitionSpec as P

VMEM_LIMIT = 32 * 1024 * 1024
DIRECT = False
f32 = jnp.float32
bf16 = jnp.bfloat16


def cosine_basis(n):
    k, i = np.arange(n)[:, None], np.arange(n)[None]
    return np.sqrt(np.where(k == 0, 1, 2) / n) * np.cos(np.pi * k * (2 * i + 1) / (2 * n))


def edge_tables(n, members, freq):
    s = 2 * np.sin(freq)
    half = np.arcsinh(s / 2)
    e = np.exp(-2 * n * half)
    safe = np.where(s == 0, 1, s)
    e1 = np.where(s == 0, 0.5, e)
    th = np.tanh(np.arcsinh(safe / 2))
    one = np.where(s == 0, 0, 1)
    lead = one * th * (1 - e1 * e1)
    couple = one * e1 / (th * (1 - e1 * e1))
    return lead, e, couple


def pieces_of(value, count):
    found = []
    for _ in range(count):
        found.append(np.asarray(value, jnp.bfloat16))
        value = value - found[-1].astype(np.float64)
    return found


def stack_pieces(value):
    a1, a2, a3 = pieces_of(value, 3)
    return np.concatenate([a1, a1, a2, a2, a1, a3], 1)


def build_tables(n, members):
    total = n * members
    half = n // 2
    k = np.concatenate([np.arange(0, n, 2), np.arange(1, n, 2)])
    q = cosine_basis(n)[k]
    s = 2 * np.sin(np.pi * k / (2 * n))
    q0, q1 = q[:, 0], q[:, -1]
    lead, e, couple = edge_tables(n, members, np.pi * k / (2 * n))
    vec = np.zeros((8, n))
    vec[0], vec[1], vec[2], vec[3], vec[4] = q0, q1, lead, e, couple
    lane = np.arange(half)
    other = np.where(lane == 0, half, lane)
    d = np.arange(members)
    kap = np.concatenate(
        [
            d[:, None] + 2 * members * lane[None],
            2 * members * other[None] - np.where(d == 0, members, d)[:, None],
        ]
    )
    glob = np.stack(edge_tables(n, members, np.pi * kap / (2 * total)))
    bend = 1 + glob[1] ** 2 - 2 * glob[1] * np.cos(np.pi * np.arange(1, members) / members)[:, None, None]
    size = np.full((2 * members, half), 1 / np.sqrt(members))
    size[1:members, 0] *= np.sqrt(2)
    dens = (glob[0] * size / bend).reshape(-1, half)
    j = 2 * np.arange(n) + 1
    sb = np.sqrt(2 / n) * np.sin(np.pi * other[:, None] * j[None] / n)
    turn = np.concatenate([q[:half].T, sb.T], 0)
    sp = np.sqrt(2 / n) * s[:, None] * np.sin(np.pi * k[:, None] * (np.arange(n)[None] + 1) / n)
    sp[:, n - 1] = 0
    sp[0] = 0
    den = s[:, None] ** 2 + s[None] ** 2
    den[0, 0] = 1
    r = 1 / den
    r[0, 0] = 0
    ang = np.pi * np.arange(members + 1)[:, None] * j[None] / (2 * total)
    ca, sa = np.cos(ang), np.sin(ang)
    swap = np.concatenate([sa[members:], ca[1:members]], 0)
    acs = np.concatenate([ca[:members], sa[:members], swap, np.repeat(ca[members:], members, 0)], 0)
    p = np.arange(members)
    wang = np.pi * np.arange(members + 1)[:, None] * p[None] / members
    wc, ws = np.cos(wang), np.sin(wang)
    wfwd = np.concatenate([wc[:members], wc[members:], ws[1:members]], 0)
    winv = np.concatenate([wc[:members], wc[members:], -ws[1:members]], 0).T
    M = members
    t = np.arange(1, M)
    st = np.sqrt(2 / M) * np.sin(np.pi * np.outer(t, t) / M)
    sa, stt, s2 = np.zeros((M, M)), np.zeros((M, M)), np.zeros((M, M))
    sa[: M - 1, : M - 1] = st
    sa[: M - 1, M - 1] = st[:, M - 2]
    stt[: M - 1, 1:] = -st
    s2[: M - 1, : M - 1] = st
    a0 = (q1[1:] ** 2 / s[1:] ** 2).sum()
    b0 = (q0[1:] * q1[1:] / s[1:] ** 2).sum()
    qq = 1 / np.sqrt(n)
    pp = np.arange(M)
    frac = (pp[:, None] + 1) / M
    t1 = frac - (pp[None] <= pp[:, None])
    h15 = np.zeros((M, M))
    h15[:, M - 1] = frac[:, 0]
    hmat = np.concatenate([h15, t1], 1)
    acc = (pp[None] < pp[:, None]).astype(float)
    acc[:, M - 1] = 0
    acc = (acc - acc.mean(0)) / qq
    up = np.zeros((M, M))
    up[:-1, 1:] = np.eye(M - 1)
    keep = np.eye(M)
    keep[M - 1, M - 1] = 0
    ka = acc @ keep
    kt = -acc @ (keep @ up)
    kh = acc @ (keep @ (-(1 + 2 * a0) * np.eye(M) + b0 * up + b0 * up.T))
    s2x = s2.copy()
    s2x[M - 1, M - 1] = 1
    per = min(M, 256 // (2 * M))
    wbd = np.kron(np.eye(per), winv)
    minv = np.zeros((M, M, n))
    lean = lead / (1 + e * e - 2 * e * np.cos(np.pi * t / M)[:, None])
    minv[: M - 1, : M - 1] = np.einsum("pm,mk,mq->pqk", st, lean, st)
    mats = np.zeros((8 * M, 128))
    mats[0:M, : 2 * M] = np.concatenate([sa, stt], 1)
    mats[M : 2 * M, :M] = t1.T
    mats[2 * M : 3 * M, :M] = ka.T * qq
    mats[3 * M : 4 * M, :M] = kt.T * qq
    mats[4 * M : 5 * M, :M] = (kh @ t1).T
    step = (pp[:, None] >= pp[None]).astype(float)
    blocks = (ka, kt, s2x @ step, kh @ step, s2x @ frac, kh @ frac, frac)
    for a, block in enumerate(blocks):
        mats[5 * M : 6 * M, a * M : a * M + block.shape[1]] = block
    kmats = np.zeros((8 * M, 384), jnp.bfloat16)
    row = 0
    for small in (hmat, np.concatenate([ka, kt, kh], 1), s2, s2x, wfwd):
        stacked = stack_pieces(small)
        kmats[row : row + small.shape[0], : stacked.shape[1]] = stacked
        row += small.shape[0]
    q1, q2, q3 = pieces_of(q, 3)
    s1, s2 = pieces_of(sp, 2)
    v1, v2 = pieces_of(vec, 2)
    out = dict(
        vec=vec, r=r, col=np.repeat(q0[:, None], min(n, 128), 1), mats=mats,
        thin=np.concatenate([dens, glob[2]], 0),
        long=np.concatenate([minv.reshape(-1, n), acs], 0),
    )
    out = {name: np.asarray(value, np.float32) for name, value in out.items()}
    out.update(
        q1=q1, q2=q2, s1=s1, s2=s2, v=np.concatenate([v1, v2], 0), kmats=kmats,
        w=np.concatenate(pieces_of(wbd, 3), 0), turn=np.concatenate(pieces_of(turn, 3), 0),
        wide=np.concatenate([q3] + pieces_of(r, 3) + pieces_of(sb, 2), 0),
    )
    return out


def split(a):
    high = a.astype(bf16)
    return high, (a - high.astype(f32)).astype(bf16)


def mm(a, b, ca, cb):
    return lax.dot_general(a, b, (((ca,), (cb,)), ((), ())), preferred_element_type=f32)


def dot3s(a, b, ca=1, cb=0):
    ah, al = a if isinstance(a, tuple) else split(a)
    bh, bl = b if isinstance(b, tuple) else split(b)
    return mm(ah, bh, ca, cb) + (mm(ah, bl, ca, cb) + mm(al, bh, ca, cb))


def dot3(a, b, ca=1, cb=0):
    ah, al = a if isinstance(a, tuple) else split(a)
    bh, bl = b if isinstance(b, tuple) else split(b)
    return mm(jnp.concatenate([ah, ah, al], ca), jnp.concatenate([bh, bl, bh], cb), ca, cb)


def split3(a):
    high, rest = a.astype(bf16), None
    rest = a - high.astype(f32)
    mid = rest.astype(bf16)
    return high, mid, (rest - mid.astype(f32)).astype(bf16)


def dot6(a, b, cb=0):
    m = a.shape[0]
    a1, a2, a3 = split3(a)
    b1, b2, b3 = b
    p = mm(jnp.concatenate([a1, a2, a3], 0), b1, 1, cb)
    q = mm(jnp.concatenate([a1, a2], 0), b2, 1, cb)
    small = (p[2 * m :] + q[m:]) + mm(a1, b3, 1, cb)
    return p[:m] + ((p[m : 2 * m] + q[:m]) + small)


def dotl(a, b):
    m = a[0].shape[0]
    b1, b2, b3 = split3(b)
    p = mm(jnp.concatenate(a, 0), b1, 1, 0)
    q = mm(jnp.concatenate(a[:2], 0), b2, 1, 0)
    small = (p[2 * m :] + q[m:]) + mm(a[0], b3, 1, 0)
    return p[:m] + ((p[m : 2 * m] + q[:m]) + small)


def doths(a, qs):
    value = dot3(a, qs, 1, 1)
    exact = jnp.sum(a, 1, keepdims=True) * (1.0 / math.sqrt(a.shape[1]))
    return jnp.where(lanes_of(value.shape) == 0, exact, value)


def doth(a, b, ca=1, cb=0):
    return lax.dot_general(
        a, b, (((ca,), (cb,)), ((), ())), precision=lax.Precision.HIGHEST, preferred_element_type=f32
    )


def rows_of(shape):
    return lax.broadcasted_iota(jnp.int32, shape, 0)


def lanes_of(shape):
    return lax.broadcasted_iota(jnp.int32, shape, 1)


def pick(values, index):
    return jnp.sum(jnp.where(rows_of(values.shape) == index, values, 0.0), 0, keepdims=True)


def below(values):
    return jnp.concatenate([jnp.zeros_like(values[:1]), values[:-1]], 0)


def stacked(b):
    b1, b2, b3 = (piece.astype(f32) for piece in split3(b))
    return jnp.concatenate([b1, b2, b1, b2, b3, b1], 0).astype(bf16)


def dotk(a, b):
    return mm(a[:, : 6 * b.shape[0]], stacked(b), 1, 0)


def edge_solve(al, t0, couple, minv, mats, kmats):
    M, n = al.shape
    L = min(n, 128)
    last = rows_of((M, n)) == M - 1
    w = al - jnp.concatenate([t0[1:], t0[:1]], 0)
    H = jnp.where(last, al, 0.0)
    tail = couple * al[M - 1 :]
    for p in range(M - 1):
        wp = w[p : p + 1] + tail if p == M - 2 else w[p : p + 1]
        H = H + minv[M * p : M * (p + 1), :] * wp
    Hz = mats[5 * M : 6 * M, 6 * M : 6 * M + 1] * al[M - 1 :, :L]
    mean = dotk(kmats[M : 2 * M, :], jnp.concatenate([al[:, :L], t0[:, :L], Hz], 0))
    lane = lanes_of((M, L))
    first = jnp.where(lane == 0, Hz, H[:, :L])
    H = first if n == L else jnp.concatenate([first, H[:, L:]], 1)
    return H, mean[:, :1]


def to_peers(rows, members):
    one = jnp.concatenate(rows, 0)
    return jnp.broadcast_to(one[None], (members,) + one.shape)


def stage_local(r, c, M, wait, get):
    wait("q1", "x0", "x1", "q2")
    m1 = dot3(
        jnp.concatenate([get("x0"), get("x1")], 0), (get("q1"), get("q2")), 1, 1
    )
    wait("y", "s1", "s2", "r", "v", "col")
    n = m1.shape[0]
    half = n // 2
    L = min(n, 128)
    n2 = dot3((get("q1"), get("q2")), get("y"))
    ss = (get("s1"), get("s2"))
    m1s, n2s = split(m1), split(n2)
    st = tuple(piece.T for piece in ss)
    f = dot3(
        tuple(jnp.concatenate([a, b], 1) for a, b in zip(ss, n2s)),
        tuple(jnp.concatenate([a, b], 0) for a, b in zip(m1s, st)),
    )
    gyl = n2[:, n - L :].T[L - 1 :]
    u = -f * get("r")
    uh, ul = split(u)
    v = get("v")
    p = mm(v, uh, 1, 1)
    tk = p[:8] + (p[8:] + mm(v, ul, 1, 1)[:8])
    col = get("col")
    groups = []
    for rows in (slice(0, half), slice(half, n)):
        groups.append(
            jnp.concatenate(
                [
                    jnp.sum(u[rows, a : a + L] * col[rows], 0, keepdims=True)
                    for a in range(0, n, L)
                ],
                1,
            )
        )
    low, high = groups[0] + groups[1], groups[0] - groups[1]
    alpha = gyl + jnp.where(c < M - 1, tk[1:2], 0.0)
    beta = m1[n - 1 :] + jnp.where(r < M - 1, high, 0.0)
    return to_peers([alpha, tk[0:1], beta, low], M), u


WAVES = {None: ("q1", "x0", "x1", "q2", "y", "s1", "s2", "r", "v", "col")}
WAVES["y"] = ("vec", "wide", "turn", "w", "thin", "long", "mats", "kmats")
NAMES = sum(WAVES.values(), ())
KEPT = ("q1", "q2", "r") + WAVES["y"]


def run_local(members, arrays):
    n = arrays["q1"].shape[1]
    arrays["x0"], arrays["x1"] = arrays["x"][: n // 2], arrays["x"][n // 2 :]
    shapes = {name: (arrays[name].shape, arrays[name].dtype) for name in NAMES}
    if DIRECT:
        edges, u = stage_local(
            lax.axis_index("row"), lax.axis_index("col"), members, lambda *names: None,
            arrays.__getitem__,
        )
        return edges, u, {name: arrays[name] for name in KEPT}

    def kernel(*refs):
        count = len(NAMES)
        edges, u = refs[count : count + 2]
        here = dict(zip(KEPT, refs[count + 2 :]))
        here.update(zip((k for k in NAMES if k not in KEPT), refs[count + 2 + len(KEPT) :]))
        sem = refs[-1]
        def part_of(name, source):
            pick_half = {"x0": pl.ds(0, n // 2), "x1": pl.ds(n // 2, n // 2)}
            return source.at[pick_half[name]] if name in pick_half else source

        copies = {
            name: pltpu.make_async_copy(part_of(name, source), here[name], sem.at[i])
            for i, (name, source) in enumerate(zip(NAMES, refs))
        }

        def release(wave):
            for name in WAVES.get(wave, ()):
                copies[name].start()

        def wait(*names):
            for name in names:
                copies[name].wait()
                release(name)

        def get(name):
            return here[name][...]

        release(None)
        edges[...], u[...] = stage_local(
            lax.axis_index("row"), lax.axis_index("col"), members, wait, get
        )
        wait(*WAVES["y"])

    operands = [name if name not in ("x0", "x1") else "x" for name in NAMES]
    far, vmem, near = pl.BlockSpec(memory_space=pltpu.HBM), pl.BlockSpec(memory_space=pltpu.VMEM), pltpu.VMEM
    shape = {name: near(*shapes[name]) for name in NAMES}
    edges, u, *tables = pl.pallas_call(
        kernel,
        out_shape=[jax.ShapeDtypeStruct((members, 4, n), f32), near((n, n), f32)]
        + [shape[name] for name in KEPT],
        in_specs=[far] * len(NAMES),
        out_specs=[vmem] * (2 + len(KEPT)),
        scratch_shapes=[shape[name] for name in NAMES if name not in KEPT]
        + [pltpu.SemaphoreType.DMA((len(NAMES),))],
        compiler_params=pltpu.CompilerParams(vmem_limit_bytes=VMEM_LIMIT),
        name="stage_local",
    )(*(pltpu.with_memory_space_constraint(arrays[name], pltpu.HBM) for name in operands))
    return edges, u, dict(zip(KEPT, tables))


def lane_pick(values, index):
    return jnp.sum(jnp.where(lanes_of(values.shape) == index, values, 0.0), 1, keepdims=True)


def stage_strip(r, c, M, ag, q1, q2, vec, wide, turn, w, thin, long, mats, kmats):
    n = q1.shape[0]
    half = n // 2
    r1, r2, r3 = (wide[a * n : (a + 1) * n, :] for a in range(1, 4))
    b1, b2 = wide[4 * n : 4 * n + half, :], wide[4 * n + half : 5 * n, :]
    acs = long[M * M : M * M + 4 * M, :]
    al, t0, be, ta0 = (ag[:, a, :] for a in range(4))
    vec, mats = vec[...], mats[...]
    v0, v1, couple = vec[0:1], vec[1:2], vec[4:5]
    L = min(n, 128)
    qq = 1.0 / math.sqrt(n)
    sa, stt = mats[:M, :M], mats[:M, M : 2 * M]

    H, mean = edge_solve(al, t0, couple, long, mats, kmats)
    rs = (r1, r2)
    Z = dot6(jnp.concatenate([H * v0, H * v1], 0), rs + (r3,))
    add0 = v0 * below(Z[:M]) - v1 * Z[:M]
    add1 = v0 * below(Z[M:]) - v1 * Z[M:]
    flat = jnp.where(lanes_of((M, n)) == 0, mean * qq, 0.0)
    tau0 = ta0 + add0 + flat
    tau1 = be + jnp.where(r < M - 1, add1 + flat, 0.0)

    qs = (q1[...], q2[...])
    y = dot6(jnp.concatenate([tau1, tau0], 0), qs + (wide[:n, :],))
    ca, sna, swap, c16 = (acs[a * M : (a + 1) * M, :] for a in range(4))
    c16 = c16[:1]
    g = dotk(kmats[4 * M : 6 * M, :], jnp.concatenate([y[:M], y[M:]], 1))
    xs, ys, extra = [], [], []
    for side in range(2):
        C, S = (g[k * M : (k + 1) * M, side * n : (side + 1) * n] for k in range(2))
        xs.append(C * ca - S * sna)
        ys.append(C * sna + S * swap)
        extra.append(S[:1] * c16)
    xs += extra + [jnp.zeros((M - 2, n), f32)]
    cosines = tuple(turn[2 * n * a : 2 * n * a + n, :] for a in range(3))
    sines = tuple(turn[2 * n * a + n : 2 * n * (a + 1), :] for a in range(3))
    xcos = dot6(jnp.concatenate(xs, 0), cosines)
    ysin = dot6(jnp.concatenate(ys, 0), sines)
    pair = (M, half)
    left_lane, top_row = lanes_of(pair) == 0, rows_of(pair) == 0
    shape = (2 * M, half)
    origin = (rows_of(shape) == 0) & (lanes_of(shape) == 0)
    root = 1.0 / math.sqrt(M)
    wider = (lanes_of(shape) == 0) & (rows_of(shape) > 0) & (rows_of(shape) < M)
    scale = jnp.where(wider, root * math.sqrt(2.0), root)
    ends = []
    for side in range(2):
        xc, yb = xcos[side * M : (side + 1) * M], ysin[side * M : (side + 1) * M]
        plus = xc - jnp.where(left_lane | top_row, 0.0, yb)
        alone = jnp.where(top_row, xcos[2 * M + side : 2 * M + side + 1], xc)
        minus = jnp.where(left_lane, 0.0, alone) + yb
        ends.append(jnp.concatenate([plus, minus], 0) * scale)
    T1, T0 = ends

    edge = mats[5 * M : 6 * M, :]
    src = al[M - 1 :, :1] * (1.0 / math.sqrt(M))
    a15 = jnp.where(r == M - 1, T1[:1, :1], 0.0)
    kac, ktc, gstep, hstep = (lane_pick(edge[:, a * M : (a + 1) * M], r) for a in range(4))
    gfrac, hfrac = edge[:, 4 * M : 4 * M + 1], edge[:, 5 * M : 5 * M + 1]
    lift = kac * T1[:1, :1] + ktc * T0[:1, :1] + hfrac * (a15 + src) - hstep * src
    g0 = gfrac * (a15 + src) - gstep * src
    up, down = lane_pick(sa, r), lane_pick(stt, r)
    T1c = jnp.where(r == M - 1, T1 * thin[2 * M * (M - 1) :, :], T1)
    modes = []
    for m in range(M - 1):
        value = (up[m : m + 1] * T1c + down[m : m + 1] * T0) * thin[2 * M * m : 2 * M * (m + 1), :]
        modes.append(jnp.where(origin, g0[m : m + 1, :1] * root, value))
    modes.append(jnp.where(r == M - 1, T1, 0.0) * scale)
    sums, gaps, single = [], [], []
    for value in modes:
        gp, gm = value[:M], value[M:]
        sums.append(gp + jnp.where(left_lane | top_row, 0.0, gm))
        gaps.append(jnp.where(top_row, gm, jnp.where(left_lane, 0.0, gp) - gm))
        single.append(jnp.where(left_lane[:1], 0.0, gm[:1]))
    XC = dot3(split(jnp.concatenate(sums + single, 0)), (qs[0][:half], qs[1][:half]))
    XS = dot3(split(jnp.concatenate(gaps, 0)), (b1, b2))
    third = w.shape[0] // 3
    ws = tuple(w[third * a : third * (a + 1), :] for a in range(3))
    group = w.shape[1] // (2 * M)
    lines = []
    top_line = rows_of((M, n)) == 0
    for first in range(0, M, group):
        rots = []
        for m in range(first, first + group):
            xc, xs = XC[M * m : M * (m + 1)], XS[M * m : M * (m + 1)]
            alone = jnp.where(top_line, c16 * XC[M * M + m : M * M + m + 1], 0.0)
            rots += [ca * xc - sna * xs, sna * xc + swap * xs + alone]
        lines.append(dotl(ws, jnp.concatenate(rots, 0)))
    hx = doths(jnp.concatenate(lines, 0), qs)
    Y0, Y1 = [], []
    for rows in (slice(0, M * M // 2), slice(M * M // 2, M * M)):
        Y = dot3(jnp.concatenate([hx[rows] * v0, hx[rows] * v1], 0), rs)
        Y0.append(Y[: M * M // 2])
        Y1.append(Y[M * M // 2 :])
    Y0, Y1 = jnp.concatenate(Y0, 0), jnp.concatenate(Y1, 0)

    first = lanes_of((1, n)) == 0
    cols = []
    for cc in (c, c - 1):
        k1 = long[pl.ds(pl.multiple_of(jnp.maximum(cc, 0) * M, M), M), :]
        k1 = jnp.where(cc < 0, 0.0, k1)
        cols.append((k1, -below(k1), lane_pick(mats[M : 2 * M, :M], cc) * (-1.0 / qq)))
    ka, kt = lane_pick(mats[2 * M : 3 * M, :M], c), lane_pick(mats[3 * M : 4 * M, :M], c)
    kth = lane_pick(mats[4 * M : 5 * M, :M], c)
    here, side_c, side_b, level = [], [], [], []
    for m in range(M):
        rows = slice(M * m, M * (m + 1))
        hm, y0, y1 = hx[rows], Y0[rows], Y1[rows]
        here.append(pick(hm, c))
        for (k1, k2, ksrc), sides in zip(cols, (side_c, side_b)):
            phi = jnp.sum(k1 * y1 + k2 * y0, 0, keepdims=True)
            z = jnp.sum(ksrc * hm, 0, keepdims=True)
            sides.append(jnp.where(first, z, phi))
        level.append(
            jnp.sum(kth * hm[:, :L] - ka * y1[:, :L] - kt * y0[:, :L], 0, keepdims=True)
        )
    rows = [jnp.concatenate(v, 0) for v in (here, side_c, side_b, level)]
    mixed = dotk(kmats[3 * M : 4 * M, :], jnp.concatenate(rows, 1))
    mixed = [mixed[:, a * n : (a + 1) * n] for a in range(4)]
    right, fc, fb, lv = mixed
    lv = (lv - below(lv) + lift * (1.0 / math.sqrt(M)))[:, :1]
    share = [
        below(right),
        right,
        v0 * below(fc) - v1 * fc,
        v0 * below(fb) - v1 * fb,
        lv,
    ]
    keep = [pick(H, c), pick(H, c - 1), jnp.broadcast_to(pick(mean, c), (1, n))]
    return share, jnp.concatenate(keep + [jnp.zeros((5, n), f32)], 0)


CUTS = (0, 6, 8)


def stage_field(r, c, M, share, keep, u, qh, ql, rr, vec):
    keep, vec = keep[...], vec[...]
    n = vec.shape[1]
    q0, q1 = vec[0:1], vec[1:2]
    left, right, here, before, level = (
        jnp.sum(share[:, a, :n] if a < 4 else share[:, 0, n:], 0, keepdims=True) for a in range(5)
    )
    here = here + keep[0:1]
    before = before + keep[1:2]
    level = level[:, :1] + keep[2:3, :1]
    pad = jnp.zeros((4, n), f32)
    a1, a2, a3 = (
        piece.astype(f32) for piece in split3(jnp.concatenate([q1, -q0, here, -before, pad], 0))
    )
    lhs = jnp.concatenate([a1, a1, a2, a2, a1, a3], 0).astype(bf16)
    G = mm(lhs, stacked(jnp.concatenate([right, left, q1, q0, pad], 0)), 0, 0)
    un = u[...] - rr[...] * G
    un = jnp.where((rows_of(un.shape) == 0) & (lanes_of(un.shape) == 0), level, un)
    qs = (qh[...], ql[...])
    half = split(dot3(un, qs))
    for first, last in zip(CUTS, CUTS[1:]):
        cols = slice(first * n // 8, last * n // 8)
        yield dot3((qs[0][:, cols], qs[1][:, cols]), half, 0, 0)


def run_field(members, *args):
    n = args[-1].shape[1]
    place = lambda: (lax.axis_index("row"), lax.axis_index("col"))
    if DIRECT:
        return jnp.concatenate(list(stage_field(*place(), members, *args)), 0)

    def kernel(*refs):
        field, rows, sem = refs[len(args) :]
        copies = []
        for part, value in enumerate(stage_field(*place(), members, *refs[: len(args)])):
            span = slice(CUTS[part] * n // 8, CUTS[part + 1] * n // 8)
            rows[span, :] = value
            copies.append(pltpu.make_async_copy(rows.at[span], field.at[span], sem.at[part]))
            copies[-1].start()
        for copy in copies:
            copy.wait()

    vmem = pl.BlockSpec(memory_space=pltpu.VMEM)
    return pl.pallas_call(
        kernel,
        out_shape=jax.ShapeDtypeStruct((n, n), f32),
        in_specs=[vmem] * len(args),
        out_specs=pl.BlockSpec(memory_space=pltpu.HBM),
        scratch_shapes=[pltpu.VMEM((n, n), f32), pltpu.SemaphoreType.DMA((len(CUTS) - 1,))],
        compiler_params=pltpu.CompilerParams(vmem_limit_bytes=VMEM_LIMIT),
        name="stage_field",
    )(*args)


def packed(rows):
    tail = jnp.broadcast_to(rows[4][:, :, None], rows[4].shape[:1] + (4, 128))
    return jnp.concatenate([jnp.stack(rows[:4], 1), tail], 2)


def run_stage(stage, members, outs, *args):
    if DIRECT:
        results = stage(lax.axis_index("row"), lax.axis_index("col"), members, *args)
        return [packed(v) if isinstance(v, list) else v for v in results]

    def kernel(*refs):
        r, c = lax.axis_index("row"), lax.axis_index("col")
        n = args[0].shape[-1]
        results = stage(r, c, members, *refs[: len(args)])
        for ref, value in zip(refs[len(args) :], results):
            if isinstance(value, list):
                for a, row in enumerate(value[:4]):
                    ref[:, a, :n] = row
                ref[:, :, n:] = jnp.broadcast_to(value[4][:, :, None], (members, 4, 128))
            else:
                ref[...] = value

    vmem = pl.BlockSpec(memory_space=pltpu.VMEM)
    return pl.pallas_call(
        kernel,
        out_shape=outs,
        in_specs=[vmem] * len(args),
        out_specs=[vmem] * len(outs),
        compiler_params=pltpu.CompilerParams(vmem_limit_bytes=VMEM_LIMIT),
        name=stage.__name__,
    )(*args)


def exchange(values, axis):
    return lax.all_to_all(values, axis, split_axis=0, concat_axis=0, tiled=True)


def make_body(members):
    def body(grad_x, grad_y):
        n = grad_x.shape[0]
        t = {k: jnp.asarray(v) for k, v in build_tables(n, members).items()}
        sent, near = jax.ShapeDtypeStruct, pltpu.VMEM
        edges, u, kept = run_local(members, {**t, "x": grad_x, "y": grad_y})
        strip = exchange(edges, "col")
        share, keep = run_stage(
            stage_strip, members, [sent((members, 4, n + 128), f32), near((8, n), f32)],
            strip, kept["q1"], kept["q2"], *(kept[name] for name in WAVES["y"]),
        )
        share = exchange(share, "row")
        return run_field(
            members, share, keep, u, kept["q1"], kept["q2"], kept["r"], kept["vec"]
        )

    return body


def solution(mesh):
    members = mesh.shape["row"]
    placed = (P("row", "col"), P("row", "col"))
    return jax.shard_map(
        make_body(members), mesh=mesh, in_specs=placed, out_specs=P("row", "col"), check_vma=False
    )
```
